32 devices in a mesh: row: 4 (over z), col: 8 (over y, x, core).
Axes of the slice: x: 2, y: 2, z: 4, core: 2. Of those that a mesh axis runs over, the one named last changes fastest.
Arguments:
- velocity: float32 [3, 64, 64, 256], P(None, 'row', 'col'), may hold values from -6 to 6
- positions: bfloat16 [1024, 3, 128], P(('row', 'col')), may hold values from -4 to 4
- weights: bfloat16 [1024, 3, 8, 128], P(('row', 'col')), may hold values from 0 to 0.5
- stiffness: bfloat16 [1024], P(('row', 'col')), may hold values from 0.099609375 to 1
- rest_sq: bfloat16 [1024], P(('row', 'col')), may hold values from 1 to 8
- owner_column: int32 [1024, 1], P(('row', 'col')), may hold values from 0 to 7; in each aligned block of 32 rows (0 to 31, 32 to 63, ...) at most 12 rows name the same one
- brick_index: int32 [1024], P(('row', 'col')), may hold values from 0 to 63
Outputs:
- new_velocity: float32 [3, 64, 64, 256], P(None, 'row', 'col')
- marker_velocity: float32 [1024, 3, 128], P(('row', 'col'))
The draws below stay inside these ranges and needn't reach their ends.
Inputs may be any that keep to these rules, and one draw needn't show every extreme that they name: `owner_column`: A block's brick lies on the device in the block's own device row and in this column; no device's 32 blocks name one column more than 12 times, and that many is reached.
All inputs are finite; a program needn't handle non-finite values.
Results may differ from the reference program's by a relative error of at most 0.0003.
Values may be sent and summed in bfloat16 or wider, within the bound.
A program may use at most 64 MiB of HBM per device.

```python
import math
import jax
import jax.numpy as jnp
import numpy as np
from jax import lax

CX = 16
CY = 8
NZ = 256
BRICK = 8
MARK = 128
BLK_DEV = 32
NX = 64
NY = 64
BLOCKS = 1024
CAP = 12
BRK_DEV = 64
N_ROW = 4
N_COL = 8


def set_ends(array, rng, smallest, high):
    place = [jax.random.randint(jax.random.fold_in(rng, axis), (), 0, length) for axis, length in enumerate(array.shape)]
    longest = array.shape.index(max(array.shape))
    beside = place[:longest] + [(place[longest] + 1) % array.shape[longest]] + place[longest + 1:]
    return array.at[tuple(place)].set(smallest).at[tuple(beside)].set(high)


def levels(key, dims, pieces, least, top_value):
    level, own = 1.0, jax.random.fold_in(key, 6)
    for axis_at, parts in pieces:
        heights = jnp.exp(jax.random.uniform(jax.random.fold_in(own, axis_at), (parts,), jnp.float32, least / len(pieces), top_value / len(pieces)))
        level = level * jnp.repeat(heights, dims[axis_at] // parts).reshape([-1 if axis == axis_at else 1 for axis in range(len(dims))])
    return level


def deal_out(stream_key, own, number, rows, amount, top, most, skew):
    sequence = jax.random.permutation(stream_key, amount)
    crowded, usual = load_shares(amount, rows * top, most, skew, True), load_shares(amount, rows * top, most, skew, False)
    places = jnp.arange(amount)

    def named(lengths, rotation):
        used = int((lengths > 0).sum())
        fixed = max(1, used // 4)
        moved = fixed + (places - fixed + rotation * (used - fixed)) % max(1, amount - fixed)
        return jnp.zeros((amount,), jnp.int32).at[sequence[jnp.where(places < fixed, places, moved)]].set(jnp.asarray(lengths, jnp.int32))

    lengths = jnp.where(number % 4 == 0, named(crowded, number // 4), named(usual, number - number // 4 - 1))
    mixed = jax.random.permutation(jax.random.fold_in(own, 3), amount)
    giver, sink = mixed[0:amount // 2 * 2:2], mixed[1:amount // 2 * 2:2]
    room = jnp.minimum(lengths[giver] - 1, most - lengths[sink]) // 2
    room = jnp.where((giver == sequence[0]) | (sink == sequence[0]) | (lengths[sink] == 0), 0, jnp.maximum(room, 0))
    moved = jax.random.randint(jax.random.fold_in(own, 4), (amount // 2,), 0, 1 << 20) % (room + 1)
    lengths = lengths.at[giver].add(-moved).at[sink].add(moved)
    labels = jnp.searchsorted(jnp.cumsum(lengths), jnp.arange(rows * top), side="right").astype(jnp.int32)
    table = labels.reshape(top, rows).T
    table = table[jax.random.permutation(jax.random.fold_in(own, 1), rows)]
    rotation = jax.random.randint(jax.random.fold_in(own, 2), (rows, 1), 0, top)
    return jnp.take_along_axis(table, (jnp.arange(top)[None, :] + rotation) % top, axis=1)


def load_shares(count, total, limit, lean, full):
    loads = [(1 << 20) // math.isqrt(grade ** lean) + 1 for grade in range(1, count + 1)]
    largest = limit if full else min(limit, max(-(-total // count), total * loads[0] // sum(loads)))
    least = 1 if total - largest >= count - 1 else 0
    counts, spare = [largest] + [least] * (count - 1), total - largest - least * (count - 1)
    while spare > 0:
        movable = [i for i in range(1, count) if counts[i] < largest] or [i for i in range(1, count) if counts[i] < limit]
        mass, budget = sum([loads[i] for i in movable]), spare
        for i in movable:
            addition = min(limit - counts[i], max(1, budget * loads[i] // mass), spare)
            counts[i] = counts[i] + addition
            spare = spare - addition
    return np.array(counts)


def normal_values(rng, extent, scale, most, pieces=(), held_as=jnp.bfloat16):
    factor_of = levels(rng, extent, pieces, -0.22, 0.18) if pieces else 1.0
    drawn = jax.random.normal(rng, extent, jnp.float32) * scale * factor_of
    return jnp.minimum(jnp.maximum(drawn, -most), most).astype(held_as)


def setup_inputs(seed: int = 0) -> dict:
    seeds = jax.random.split(jax.random.key(seed), 8)
    velocity = normal_values(seeds[0], (3, NX, NY, NZ), 1.0, 6.0, ((1, 4), (2, 8)), jnp.float32)
    positions = normal_values(seeds[1], (BLOCKS, 3, MARK), 1.0, 4.0, ((0, 32),))
    weights = jnp.clip(0.5 * jax.random.uniform(seeds[2], (BLOCKS, 3, BRICK, MARK), jnp.float32) ** levels(seeds[2], (BLOCKS, 3, BRICK, MARK), ((0, 32),), -0.2, 0.2), 0.0, 0.5).astype(jnp.bfloat16)
    stiffness = jnp.clip(jnp.exp(math.log(1.0) - 2.306499 * jax.random.uniform(seeds[3], (BLOCKS,), jnp.float32) ** levels(seeds[3], (BLOCKS,), ((0, 32),), -0.2, 0.2)), 0.099609375, 1.0).astype(jnp.bfloat16)
    rest_sq = jnp.clip(jnp.exp(math.log(8.0) - 2.0794415 * jax.random.uniform(seeds[4], (BLOCKS,), jnp.float32) ** levels(seeds[4], (BLOCKS,), ((0, 32),), -0.2, 0.2)), 1.0, 8.0).astype(jnp.bfloat16)
    owner_column_keys = jax.random.split(jax.random.fold_in(seeds[5], 1), BLOCKS // BLK_DEV)
    owner_column_turns = jax.random.permutation(jax.random.fold_in(seeds[5], 3), BLOCKS // BLK_DEV)
    owner_column = jax.vmap(lambda own, number: deal_out(jax.random.fold_in(seeds[5], 2), own, number, BLK_DEV, N_COL, 1, CAP, 2))(owner_column_keys, owner_column_turns).reshape((BLOCKS, 1))
    brick_index = set_ends(jax.random.randint(seeds[6], (BLOCKS,), 0, BRK_DEV), jax.random.fold_in(seeds[6], 1), 0, BRK_DEV - 1).astype(jnp.int32)
    return dict(velocity=velocity, positions=positions, weights=weights, stiffness=stiffness, rest_sq=rest_sq, owner_column=owner_column, brick_index=brick_index)


DT_STEP = 0.5
VISCOSITY = 0.1
PRECISE = lax.Precision.HIGHEST


def to_bricks(values):
    components, size_x, size_y, size_z = values.shape
    blocks_view = values.reshape(components, size_x // BRICK, BRICK, size_y // BRICK, BRICK, size_z // BRICK, BRICK)
    blocks_view = blocks_view.transpose(1, 3, 5, 0, 2, 4, 6)
    return blocks_view.reshape(-1, components * BRICK * BRICK * BRICK)


def from_bricks(bricks, size_x, size_y, size_z):
    blocks_view = bricks.reshape(size_x // BRICK, size_y // BRICK, size_z // BRICK, 3, BRICK, BRICK, BRICK)
    blocks_view = blocks_view.transpose(3, 0, 4, 1, 5, 2, 6)
    return blocks_view.reshape(3, size_x, size_y, size_z)


def chain_force(positions_f, stiffness_f, rest_f):
    segment = jnp.roll(positions_f, -1, axis=2) - positions_f
    stretch = jnp.sum(segment * segment, axis=1, keepdims=True) / rest_f[:, None, None]
    tension = 0.5 * stiffness_f[:, None, None] * (stretch - 1.0) * segment
    return tension - jnp.roll(tension, 1, axis=2)


def interpolate(bricks_in, weights_f):
    cubes = bricks_in.reshape(-1, 3, BRICK, BRICK, BRICK)
    reduced = jnp.einsum('ncijk,nkm->ncijm', cubes, weights_f[:, 2], precision=PRECISE)
    reduced = jnp.einsum('ncijm,njm->ncim', reduced, weights_f[:, 1], precision=PRECISE)
    return jnp.einsum('ncim,nim->ncm', reduced, weights_f[:, 0], precision=PRECISE)


def spread(forces, weights_f):
    partial_sum = jnp.einsum('ncm,nim->ncim', forces, weights_f[:, 0], precision=PRECISE)
    partial_sum = jnp.einsum('ncim,njm->ncijm', partial_sum, weights_f[:, 1], precision=PRECISE)
    cubes = jnp.einsum('ncijm,nkm->ncijk', partial_sum, weights_f[:, 2], precision=PRECISE)
    return cubes.reshape(cubes.shape[0], -1)


def advect(values):
    transport = jnp.zeros_like(values)
    for direction in range(3):
        gradient = (jnp.roll(values, -1, axis=direction + 1) - jnp.roll(values, 1, axis=direction + 1)) * 0.5
        transport = transport + values[direction] * gradient
    return transport


def signed_modes(indices, length):
    return jnp.where(indices <= (length - 1) // 2, indices, indices - length)


def direction_modes(indices, length):
    return jnp.where(2 * indices == length, 0, signed_modes(indices, length))


def reference(velocity, positions, weights, stiffness, rest_sq, owner_column, brick_index):
    brick_table = to_bricks(velocity)
    local_x = CX // BRICK
    local_y = CY // BRICK
    local_z = NZ // BRICK
    total_y = NY // BRICK
    block_ids = jnp.arange(BLOCKS, dtype=jnp.int32)
    row_index = block_ids // (BLK_DEV * N_COL)
    column = owner_column[:, 0]
    brick_x = brick_index // (local_y * local_z)
    brick_y = (brick_index // local_z) % local_y
    brick_z = brick_index % local_z
    global_ids = ((row_index * local_x + brick_x) * total_y + column * local_y + brick_y) * local_z + brick_z
    device_count = N_ROW * N_COL

    def visit_group(forcing, member):
        brick_ids, positions_g, weights_g, stiffness_g, rest_g = member
        weights_f = weights_g.astype(jnp.float32)
        marker_vel = interpolate(brick_table[brick_ids], weights_f)
        forces = chain_force(positions_g.astype(jnp.float32), stiffness_g.astype(jnp.float32), rest_g.astype(jnp.float32))
        forcing = forcing.at[brick_ids].add(spread(forces, weights_f))
        return forcing, marker_vel

    members = (global_ids.reshape(device_count, BLK_DEV),
               positions.reshape(device_count, BLK_DEV, 3, MARK),
               weights.reshape(device_count, BLK_DEV, 3, BRICK, MARK),
               stiffness.reshape(device_count, BLK_DEV),
               rest_sq.reshape(device_count, BLK_DEV))
    forcing, gathered = lax.scan(visit_group, jnp.zeros_like(brick_table), members)
    marker_velocity = gathered.reshape(BLOCKS, 3, MARK)
    force_field = from_bricks(forcing, NX, NY, NZ)
    star = velocity + DT_STEP * (force_field - advect(velocity))
    spectrum = jnp.fft.fftn(star, axes=(1, 2, 3))
    index_x = jnp.arange(NX, dtype=jnp.int32)
    index_y = jnp.arange(NY, dtype=jnp.int32)
    index_z = jnp.arange(NZ, dtype=jnp.int32)
    full_x = (2.0 * jnp.pi / NX) * signed_modes(index_x, NX).astype(jnp.float32)[:, None, None]
    full_y = (2.0 * jnp.pi / NY) * signed_modes(index_y, NY).astype(jnp.float32)[None, :, None]
    full_z = (2.0 * jnp.pi / NZ) * signed_modes(index_z, NZ).astype(jnp.float32)[None, None, :]
    dir_x = direction_modes(index_x, NX)[:, None, None]
    dir_y = direction_modes(index_y, NY)[None, :, None]
    dir_z = direction_modes(index_z, NZ)[None, None, :]
    no_direction = (dir_x == 0) & (dir_y == 0) & (dir_z == 0)
    wave_x = (2.0 * jnp.pi / NX) * dir_x.astype(jnp.float32)
    wave_y = (2.0 * jnp.pi / NY) * dir_y.astype(jnp.float32)
    wave_z = (2.0 * jnp.pi / NZ) * dir_z.astype(jnp.float32)
    wave_sq = wave_x * wave_x + wave_y * wave_y + wave_z * wave_z
    inverse_sq = jnp.where(no_direction, 0.0, 1.0 / jnp.where(no_direction, 1.0, wave_sq))
    damping = 1.0 / (1.0 + DT_STEP * VISCOSITY * (full_x * full_x + full_y * full_y + full_z * full_z))
    normal_part = (wave_x * spectrum[0] + wave_y * spectrum[1] + wave_z * spectrum[2]) * inverse_sq
    projected = jnp.stack([(spectrum[0] - wave_x * normal_part) * damping,
                           (spectrum[1] - wave_y * normal_part) * damping,
                           (spectrum[2] - wave_z * normal_part) * damping])
    new_velocity = jnp.real(jnp.fft.ifftn(projected, axes=(1, 2, 3))).astype(jnp.float32)
    return new_velocity, marker_velocity
```

```python
from functools import partial

import numpy as np

import jax
import jax.numpy as jnp
from jax import lax
from jax.experimental import pallas as pl
from jax.experimental.pallas import tpu as pltpu
from jax.sharding import PartitionSpec as P

BRICK = 8


DT_STEP = 0.5
VISCOSITY = 0.1
PRECISE = lax.Precision.HIGHEST


def with_halo(block, sides, width):
    for axis, dim in sides:
        count = lax.axis_size(axis)
        forward = [(i, i + 1) for i in range(count - 1)]
        forward.append((count - 1, 0))
        backward = [(target, source) for source, target in forward]
        low = lax.ppermute(
            lax.slice_in_dim(block, block.shape[dim] - width, None, axis=dim), axis, forward
        )
        high = lax.ppermute(lax.slice_in_dim(block, 0, width, axis=dim), axis, backward)
        block = jnp.concatenate([low, block, high], axis=dim)
    return block


def to_bricks(values):
    components, size_x, size_y, size_z = values.shape
    blocks_view = values.reshape(
        components, size_x // BRICK, BRICK, size_y // BRICK, BRICK, size_z // BRICK, BRICK
    )
    blocks_view = blocks_view.transpose(1, 3, 5, 0, 2, 4, 6)
    return blocks_view.reshape(-1, components * BRICK * BRICK * BRICK)


def from_bricks(bricks, size_x, size_y, size_z):
    blocks_view = bricks.reshape(
        size_x // BRICK, size_y // BRICK, size_z // BRICK, 3, BRICK, BRICK, BRICK
    )
    blocks_view = blocks_view.transpose(3, 0, 4, 1, 5, 2, 6)
    return blocks_view.reshape(3, size_x, size_y, size_z)


def chain_force(positions_f, stiffness_f, rest_f):
    segment = jnp.roll(positions_f, -1, axis=2) - positions_f
    stretch = jnp.sum(segment * segment, axis=1, keepdims=True) / rest_f[:, None, None]
    tension = 0.5 * stiffness_f[:, None, None] * (stretch - 1.0) * segment
    return tension - jnp.roll(tension, 1, axis=2)


def interpolate(bricks_in, weights_f):
    cubes = bricks_in.reshape(-1, 3, BRICK, BRICK, BRICK)
    reduced = jnp.einsum("ncijk,nkm->ncijm", cubes, weights_f[:, 2], precision=PRECISE)
    reduced = jnp.einsum("ncijm,njm->ncim", reduced, weights_f[:, 1], precision=PRECISE)
    return jnp.einsum("ncim,nim->ncm", reduced, weights_f[:, 0], precision=PRECISE)


def spread(forces, weights_f):
    partial_sum = jnp.einsum("ncm,nim->ncim", forces, weights_f[:, 0], precision=PRECISE)
    partial_sum = jnp.einsum("ncim,njm->ncijm", partial_sum, weights_f[:, 1], precision=PRECISE)
    cubes = jnp.einsum("ncijm,nkm->ncijk", partial_sum, weights_f[:, 2], precision=PRECISE)
    return cubes.reshape(cubes.shape[0], -1)


def signed_modes(indices, length):
    return jnp.where(indices <= (length - 1) // 2, indices, indices - length)


def direction_modes(indices, length):
    return jnp.where(2 * indices == length, 0, signed_modes(indices, length))


def tables(length):
    indices = jnp.arange(length, dtype=jnp.int32)
    phases = indices[:, None] * indices[None, :] % length
    angles = 2.0 * jnp.pi / length * phases.astype(jnp.float32)
    return (jnp.cos(angles), jnp.sin(angles))


def forward(form, real_part, imag_part, length):
    cosine, sine = tables(length)
    product = partial(jnp.einsum, precision=PRECISE)
    out_real = product(form, real_part, cosine) + product(form, imag_part, sine)
    out_imag = product(form, imag_part, cosine) - product(form, real_part, sine)
    return (out_real, out_imag)


def backward(form, real_part, imag_part, length):
    cosine, sine = tables(length)
    product = partial(jnp.einsum, precision=PRECISE)
    out_real = product(form, real_part, cosine) - product(form, imag_part, sine)
    out_imag = product(form, imag_part, cosine) + product(form, real_part, sine)
    return (out_real / length, out_imag / length)


def col_transpose(values):
    return lax.all_to_all(values, "col", split_axis=4, concat_axis=3, tiled=True)


def row_transpose(values):
    return lax.all_to_all(values, "row", split_axis=4, concat_axis=2, tiled=True)


def wave_parts(indices, length):
    scale = 2.0 * jnp.pi / length
    direct = direction_modes(indices, length)
    signed = signed_modes(indices, length)
    return (scale * direct.astype(jnp.float32), scale * signed.astype(jnp.float32), direct == 0)


def general(velocity, positions, weights, stiffness, rest_sq, owner_column, brick_index):
    row_count = lax.axis_size("row")
    col_count = lax.axis_size("col")
    size_x = velocity.shape[1]
    size_y = velocity.shape[2]
    size_z = velocity.shape[3]
    block_count = positions.shape[0]
    capacity = max(2, 3 * block_count // col_count)
    total_slots = col_count * capacity
    owner_col = owner_column[:, 0]
    order_ids = jnp.arange(block_count, dtype=jnp.int32)
    earlier_same = (owner_col[None, :] == owner_col[:, None]) & (
        order_ids[None, :] < order_ids[:, None]
    )
    slot_index = owner_col * capacity + jnp.sum(earlier_same.astype(jnp.int32), axis=1)
    stored = to_bricks(velocity)
    brick_count = stored.shape[0]

    def place(values, fill):
        buffer = jnp.full((total_slots,) + values.shape[1:], fill, values.dtype)
        return buffer.at[slot_index].set(values).reshape((col_count, capacity) + values.shape[1:])

    weights_f = weights.astype(jnp.float32)
    forces = chain_force(
        positions.astype(jnp.float32), stiffness.astype(jnp.float32), rest_sq.astype(jnp.float32)
    )
    pushed = spread(forces, weights_f)
    send_force = place(pushed, 0.0)
    send_index = place(brick_index.astype(jnp.float32), 0.0)
    wanted = lax.all_to_all(send_index, "col", split_axis=0, concat_axis=0, tiled=True)
    pushes = lax.all_to_all(send_force, "col", split_axis=0, concat_axis=0, tiled=True)
    wanted_ids = wanted.astype(jnp.int32)
    reply = stored[wanted_ids]
    returned = lax.all_to_all(reply, "col", split_axis=0, concat_axis=0, tiled=True)
    returned, arrived_ids, arrived = (returned, wanted_ids, pushes)
    fetched = returned.reshape(total_slots, -1)[slot_index]
    marker_velocity = interpolate(fetched, weights_f)
    forcing = jax.ops.segment_sum(
        arrived.reshape(total_slots, -1), arrived_ids.reshape(-1), num_segments=brick_count
    )
    force_field = from_bricks(forcing, size_x, size_y, size_z)
    padded = with_halo(velocity, (("row", 1), ("col", 2)), 1)
    grad_x = (padded[:, 2:, 1:-1] - padded[:, :-2, 1:-1]) * 0.5
    grad_y = (padded[:, 1:-1, 2:] - padded[:, 1:-1, :-2]) * 0.5
    grad_z = (jnp.roll(velocity, -1, axis=3) - jnp.roll(velocity, 1, axis=3)) * 0.5
    transport = velocity[0] * grad_x + velocity[1] * grad_y + velocity[2] * grad_z
    star = velocity + DT_STEP * (force_field - transport)
    cos_z, sin_z = tables(size_z)
    half_z = size_z // 2
    col_here = lax.axis_index("col")
    cos_fore = cos_z[:, :half_z]
    sin_fore = sin_z[:, :half_z].at[:, 0].set(-cos_z[:, half_z])
    z_real = jnp.einsum("cxyz,zk->cxyk", star, cos_fore, precision=PRECISE)
    z_imag = -jnp.einsum("cxyz,zk->cxyk", star, sin_fore, precision=PRECISE)
    shuffled = col_transpose(jnp.stack([z_real, z_imag]))
    slab = shuffled.shape[4]
    first_slot = (col_here == 0) & (jnp.arange(slab, dtype=jnp.int32) == 0)
    highest = shuffled[1][..., 0:1] * (col_here == 0).astype(jnp.float32)
    lower_imag = jnp.where(first_slot, 0.0, shuffled[1])
    y_in_real = jnp.concatenate([shuffled[0], highest], axis=3)
    y_in_imag = jnp.concatenate([lower_imag, jnp.zeros_like(highest)], axis=3)
    z_index = jnp.concatenate(
        [col_here * slab + jnp.arange(slab, dtype=jnp.int32), jnp.full((1,), half_z, jnp.int32)]
    )
    y_real, y_imag = forward("cxyz,yk->cxzk", y_in_real, y_in_imag, y_in_real.shape[2])
    shuffled = row_transpose(jnp.stack([y_real, y_imag]))
    x_real, x_imag = forward("cxzy,xk->czyk", shuffled[0], shuffled[1], shuffled.shape[2])
    slab_y = x_real.shape[2]
    full_x = x_real.shape[3]
    full_y = slab_y * row_count
    y_index = lax.axis_index("row") * slab_y + jnp.arange(slab_y, dtype=jnp.int32)
    x_index = jnp.arange(full_x, dtype=jnp.int32)
    dir_z, sig_z, zero_z = wave_parts(z_index, size_z)
    dir_y, sig_y, zero_y = wave_parts(y_index, full_y)
    dir_x, sig_x, zero_x = wave_parts(x_index, full_x)
    wave_z = dir_z[:, None, None]
    wave_y = dir_y[None, :, None]
    wave_x = dir_x[None, None, :]
    no_direction = zero_z[:, None, None] & zero_y[None, :, None] & zero_x[None, None, :]
    wave_sq = wave_x * wave_x + wave_y * wave_y + wave_z * wave_z
    full_sq = sig_z[:, None, None] ** 2 + sig_y[None, :, None] ** 2 + sig_x[None, None, :] ** 2
    inverse_sq = jnp.where(no_direction, 0.0, 1.0 / jnp.where(no_direction, 1.0, wave_sq))
    damping = 1.0 / (1.0 + DT_STEP * VISCOSITY * full_sq)
    waves = jnp.stack(
        [
            jnp.broadcast_to(wave_x, wave_sq.shape),
            jnp.broadcast_to(wave_y, wave_sq.shape),
            jnp.broadcast_to(wave_z, wave_sq.shape),
        ]
    )
    normal_real = jnp.sum(waves * x_real, axis=0) * inverse_sq
    normal_imag = jnp.sum(waves * x_imag, axis=0) * inverse_sq
    p_real = (x_real - waves * normal_real) * damping
    p_imag = (x_imag - waves * normal_imag) * damping
    b_real, b_imag = backward("czyk,kx->cyzx", p_real, p_imag, full_x)
    shuffled = row_transpose(jnp.stack([b_real, b_imag]))
    b_real, b_imag = backward("cyzx,yk->cxzk", shuffled[0], shuffled[1], shuffled.shape[2])
    slab = b_real.shape[2] - 1
    first_slot = (col_here == 0) & (jnp.arange(slab, dtype=jnp.int32) == 0)
    highest = b_real[:, :, slab:, :]
    packed_imag = jnp.where(first_slot[None, None, :, None], highest, b_imag[:, :, :slab, :])
    shuffled = col_transpose(jnp.stack([b_real[:, :, :slab, :], packed_imag]))
    doubling = jnp.where(jnp.arange(half_z, dtype=jnp.int32) == 0, 1.0, 2.0)[:, None]
    cos_back = cos_z[:half_z] * doubling
    sin_back = (sin_z[:half_z] * doubling).at[0].set(-cos_z[half_z])
    new_velocity = (
        jnp.einsum("cxky,kz->cxyz", shuffled[0], cos_back, precision=PRECISE)
        - jnp.einsum("cxky,kz->cxyz", shuffled[1], sin_back, precision=PRECISE)
    ) / size_z
    return (new_velocity, marker_velocity)


VMEM = pltpu.VMEM
MESH = pl.DeviceIdType.MESH
F32 = jnp.float32
BF16 = jnp.bfloat16
I32 = jnp.int32
TOP = 32700.0
NT = ((1,), (1,))


def two_parts(table):
    table = np.asarray(table, np.float64)
    high = table.astype(jnp.bfloat16)
    low = (table - high.astype(np.float64)).astype(jnp.bfloat16)
    return np.stack([high, low])


def angle_of(length, left, right):
    return 2.0 * np.pi / length * (np.outer(left, right) % length)


def build_tables(size_x, size_y, size_z, rows):
    half_z = size_z // 2
    turn = angle_of(size_z, np.arange(size_z), np.arange(half_z))
    fore = np.concatenate([np.cos(turn), -np.sin(turn)], axis=1)
    back = np.concatenate([2.0 * np.cos(turn), -2.0 * np.sin(turn)], axis=1)
    alternate = np.where(np.arange(size_z) % 2 == 0, 1.0, -1.0)
    fore[:, half_z] = alternate
    back[:, 0], back[:, half_z] = 1.0, alternate
    back = back.T / (size_x * size_y * size_z)
    turn_y = angle_of(size_y, np.arange(size_y), np.arange(size_y))
    line = np.concatenate([np.cos(turn_y), np.sin(turn_y)], axis=0)
    lane = np.arange(size_x)
    place = (lane % rows) * (size_x // rows) + lane // rows
    turn_x = angle_of(size_x, place, np.arange(size_x))
    cosine, sine = np.cos(turn_x), np.sin(turn_x)
    wide = np.concatenate(
        [np.concatenate([cosine, -sine], axis=1), np.concatenate([sine, cosine], axis=1)], axis=0
    )
    return tuple(two_parts(t) for t in (fore, back, line, wide, wide.T))


def parts(values):
    high = values.astype(BF16)
    return high, (values - high.astype(F32)).astype(BF16)


def mul(left, right, dims=((1,), (0,))):
    return lax.dot_general(left, right, (dims, ((), ())), preferred_element_type=F32)


def mul3(left, right, dims=((1,), (0,))):
    return (
        mul(left[0], right[0], dims) + mul(left[1], right[0], dims) + mul(left[0], right[1], dims)
    )


def roll(values, shift):
    return pltpu.roll(values, shift % 128, values.ndim - 1)


def lanes_of(shape):
    return lax.broadcasted_iota(I32, shape, len(shape) - 1)


def code_of(peak):
    return jnp.floor(jnp.log2(jnp.maximum(peak, 1e-30)) * 65536.0).astype(I32) + 2


def unit_of(code):
    return jnp.exp2(code.astype(F32) * (1.0 / 65536.0)) * (1.0 / TOP)


def whole(values):
    return jnp.round(values).astype(I32)


def join(first, second):
    return (first << 16) + second


def split(word):
    second = (word << 16) >> 16
    return (word - second) >> 16, second


def swap_bits(tiles, steps):
    tiles = list(tiles)
    keep = {s: (lanes_of(tiles[0].shape) & s) == 0 for s in steps}
    for bit, step in enumerate(steps):
        for one in range(len(tiles)):
            if one >> bit & 1:
                continue
            two = one | 1 << bit
            a, b = tiles[one], tiles[two]
            tiles[one] = jnp.where(keep[step], a, roll(b, step))
            tiles[two] = jnp.where(keep[step], roll(a, -step), b)
    return tiles


def compress(tiles, lane):
    out = []
    for t in range(9):
        out.append(jnp.where(lane < 96, tiles[t], roll(tiles[9 + t // 3], 96 - 32 * (t % 3))))
    return out


def expand(tiles, lane):
    out = list(tiles)
    for u in range(3):
        a, b, c = (roll(tiles[3 * u + p], 32 + 32 * p) for p in range(3))
        out.append(jnp.where(lane < 32, a, jnp.where(lane < 64, b, c)))
    return out


def pack_cubes(wide, lane):
    tiles = [wide[t * 8 : t * 8 + 8].astype(I32) for t in range(24)]
    words = []
    for c in range(3):
        for i in range(4):
            words.append(join(tiles[c * 8 + i], tiles[c * 8 + i + 4]))
    return compress(words, lane)


def open_cubes(tiles, lane):
    out = [None] * 24
    for t, word in enumerate(expand(tiles, lane)):
        at = t // 4 * 8 + t % 4
        out[at], out[at + 4] = split(word)
    return jnp.concatenate([t.astype(F32) for t in out], axis=0)


def peak_of(values):
    while values.ndim > 2:
        values = jnp.max(values, axis=0)
    return jnp.max(jnp.max(values, axis=0, keepdims=True), axis=1, keepdims=True)


def column(row):
    shape = (row.shape[1], row.shape[1])
    diagonal = lax.broadcasted_iota(I32, shape, 0) == lax.broadcasted_iota(I32, shape, 1)
    return jnp.sum(jnp.where(diagonal, row, 0.0), axis=1, keepdims=True)


def mix(step, cols):
    ring, pair = step // cols, step % cols
    return ((6, 2, 4, 7, 3, 5, 1, 0).index(pair % 8), (2, 1, 3, 0).index(ring % 4), step)


def main_kernel(
    rows, columns, capacity,
    owner_ref, brick_ref, stiff_ref, rest_ref, pos_ref, weight_ref, velocity_ref,
    fore_ref, line_ref, wide_ref, unwide_ref,
    last_ref, mark_ref,
    force, deep, cube, place, face_x, face_y, near_x, near_y, push, pushed, star, select,
    held, modes, arrived, reply, replied, ready,
    face_sems, push_sems, mode_sems, reply_sems, last_sems,
):
    row, col = lax.axis_index("row"), lax.axis_index("col")
    devices = rows * columns
    blocks = pos_ref.shape[1]
    size_x, size_y, size_z = velocity_ref.shape[1:]
    bricks_x = size_x // 8
    barrier = pltpu.get_barrier_semaphore()

    def flip(step):
        at, bit = 0, 1
        while bit < columns:
            own = lax.rem(col // bit, 2)
            at = at + bit * (1 - own if step & bit else own)
            bit *= 2
        return at

    def peer(step):
        to_row, to_col = lax.rem(row + step // columns, rows), flip(step % columns)
        return (to_row, to_col), to_row * columns + to_col

    for step in range(1, devices):
        pl.semaphore_signal(barrier, inc=1, device_id=peer(step)[0], device_id_type=MESH)

    def remote(source, target, sems, step, device):
        return pltpu.make_async_remote_copy(
            source, target, sems.at[0, step], sems.at[1, step],
            device_id=device, device_id_type=MESH,
        )

    def send_all(source, target, sems, around):
        waits = []
        count = devices if around else columns
        me = row * columns + col if around else col
        for step in sorted(range(1, count), key=lambda n: mix(n, columns)):
            device, at = peer(step)
            at = at if around else device[1]
            copy = remote(source.at[at], target.at[me], sems, step, device)
            copy.start()
            opposite = (rows - step // columns) % rows * columns + step % columns
            origin_device, origin = peer(opposite)
            origin = origin if around else origin_device[1]
            waits.append((copy, remote(source.at[at], target.at[origin], sems, step, device)))
        own = pltpu.make_async_copy(source.at[me], target.at[me], sems.at[0, 0])
        own.start()
        return waits, own

    def receive(sent):
        for _, arrival in sent[0]:
            arrival.wait_recv()
        sent[1].wait()

    def finish(sent):
        for copy, _ in sent[0]:
            copy.wait_send()

    lane8 = lanes_of((8, 128))

    owner_row = owner_ref[...].astype(F32)
    owner = column(owner_row)
    shape = (blocks, blocks)
    earlier = lax.broadcasted_iota(I32, shape, 1) < lax.broadcasted_iota(I32, shape, 0)
    rank = jnp.sum(
        jnp.where((owner == owner_row) & earlier, 1.0, 0.0), axis=1, keepdims=True
    )
    slot = jnp.broadcast_to(owner * 128.0 + rank * 8.0, (blocks, 128))
    brick = jnp.broadcast_to(column(brick_ref[...].astype(F32)) + 1.0, (blocks, 128))
    deep_shape = (blocks, 8, 128)
    inner = lax.broadcasted_iota(I32, deep_shape, 1).astype(F32)
    slot = (slot[:, None, :] + inner).reshape(blocks * 8, 128)
    brick = jnp.broadcast_to(brick[:, None, :], deep_shape).reshape(blocks * 8, 128)
    lane_f = lanes_of((blocks * 8, 128)).astype(F32)
    marks = []
    for at in range(columns):
        hit = slot == lane_f + 128.0 * at
        place[:, at * 128 : (at + 1) * 128] = jnp.where(hit, 1.0, 0.0).astype(BF16)
        marks.append(jnp.sum(jnp.where(hit, brick, 0.0), axis=0, keepdims=True).astype(I32))

    stiff = column(stiff_ref[...].astype(F32))
    rest = column(rest_ref[...].astype(F32))
    points = [pos_ref[c].astype(F32) for c in range(3)]
    segment = [pltpu.roll(p, 127, 1) - p for p in points]
    stretch = sum(part * part for part in segment) / rest
    pull = 0.5 * stiff * (stretch - 1.0)
    for c in range(3):
        tension = pull * segment[c]
        force[c] = tension - pltpu.roll(tension, 1, 1)

    def spread(index, carry):
        first = weight_ref[index, 0].astype(F32)
        second = weight_ref[index, 1].astype(F32)
        third = weight_ref[index, 2].astype(F32)
        high, low = parts((first[:, None, :] * third[None]).reshape(64, 128))
        both = jnp.concatenate([high, low], axis=0)
        deep[index] = both
        pushes = jnp.concatenate([force[c, pl.ds(index, 1), :] * second for c in range(3)], axis=0)
        upper = pushes.astype(BF16).astype(F32)
        left = jnp.concatenate([upper, pushes - upper], axis=0).astype(BF16)
        result = mul(left, both, NT)
        total = result[0:24] + result[24:48]
        total = total + pltpu.roll(total, 64, 1)
        cube[index] = total.reshape(3, 8, 128)
        return carry

    lax.fori_loop(0, blocks, spread, 0, unroll=8)

    low_half = lane8 < 64
    outs = [[None] * 2 for _ in range(24)]
    for c in range(3):
        for g in range(2):
            tiles = [
                jnp.where(low_half, cube[g * 16 + b, c], cube[g * 16 + 8 + b, c]) for b in range(8)
            ]
            for i, tile in enumerate(swap_bits(tiles, (8, 16, 32))):
                outs[c * 8 + i][g] = tile
    spreads = jnp.concatenate([jnp.concatenate(pair, axis=1) for pair in outs], axis=0)
    push_code = code_of(peak_of(jnp.abs(spreads)))
    high, low = parts(jnp.round(spreads * (1.0 / unit_of(push_code))))
    for at in range(columns):
        window = place[:, at * 128 : (at + 1) * 128]
        tiles = pack_cubes(mul(high, window) + mul(low, window), lane8)
        for t in range(9):
            push[at, t * 8 : t * 8 + 8] = tiles[t]
        push[at, 72:80] = jnp.where(lane8 < 96, marks[at], push_code)

    face_x[0] = velocity_ref[:, size_x - 1]
    face_x[1] = velocity_ref[:, 0]
    face_y[0] = velocity_ref[:, :, size_y - 1, :]
    face_y[1] = velocity_ref[:, :, 0, :]

    pl.semaphore_wait(barrier, devices - 1)
    faces = []
    for source, target, base, axis in ((face_x, near_x, 0, 0), (face_y, near_y, 2, 1)):
        for side in range(2):
            extent = (rows, columns)[axis]
            step = 1 if side == 0 else extent - 1
            if axis == 0:
                device = (lax.rem(row + step, rows), col)
            else:
                device = (row, lax.rem(col + step, columns))
            copy = remote(source.at[side], target.at[side], face_sems, base + side, device)
            copy.start()
            faces.append(copy)
    pushes = send_all(push, pushed, push_sems, False)

    for copy in faces:
        copy.wait()
    value = velocity_ref[...]
    ahead = jnp.concatenate([value[:, 1:], near_x[1][:, None]], axis=1)
    behind = jnp.concatenate([near_x[0][:, None], value[:, :-1]], axis=1)
    transport = value[0:1] * ((ahead - behind) * 0.5)
    flat = value.reshape(3 * size_x, size_y, size_z)
    sub = lax.broadcasted_iota(I32, flat.shape, 1)
    face_low = near_y[0].reshape(3 * size_x, 1, size_z)
    face_high = near_y[1].reshape(3 * size_x, 1, size_z)
    ahead = jnp.where(sub == size_y - 1, face_high, pltpu.roll(flat, size_y - 1, 1))
    behind = jnp.where(sub == 0, face_low, pltpu.roll(flat, 1, 1))
    transport += value[1:2] * ((ahead - behind) * 0.5).reshape(value.shape)
    ahead = pltpu.roll(flat, size_z - 1, 2)
    behind = pltpu.roll(flat, 1, 2)
    transport += value[2:3] * ((ahead - behind) * 0.5).reshape(value.shape)
    star[...] = value - DT_STEP * transport

    receive(pushes)
    spot = lax.broadcasted_iota(I32, (bricks_x * size_z, 128), 0)
    inner = lanes_of((1, 128)) & 7
    for at in range(columns):
        tiles = [pushed[at, t * 8 : t * 8 + 8] for t in range(9)]
        meta = pushed[at, 72:80]
        unit = unit_of(meta)[:, 127:128]
        wide = open_cubes(tiles, lane8).reshape(24, 8, 128) * unit[None]
        high, low = parts(wide.reshape(192, 128))
        held[0, :, at * 128 : (at + 1) * 128] = high
        held[1, :, at * 128 : (at + 1) * 128] = low
        mark = meta[0:1]
        mark = jnp.where((lanes_of((1, 128)) < 96) & (mark > 0), (mark - 1) * 8 + inner, -1)
        select[:, at * 128 : (at + 1) * 128] = jnp.where(spot == mark, 1.0, 0.0).astype(BF16)
    for brick_x in range(bricks_x):
        chosen = select[brick_x * size_z : (brick_x + 1) * size_z]
        field = mul(held[0], chosen, NT) + mul(held[1], chosen, NT)
        star[:, brick_x * 8 : (brick_x + 1) * 8] += DT_STEP * field.reshape(3, 8, 8, size_z)

    spectrum = mul3(parts(star[...].reshape(-1, size_z)), (fore_ref[0], fore_ref[1]))
    real = spectrum[:, 0:128].reshape(3 * size_x, 8, 128)
    imag = spectrum[:, 128:256].reshape(3 * size_x, 8, 128)
    peak = jnp.maximum(jnp.max(jnp.abs(real), axis=0), jnp.max(jnp.abs(imag), axis=0))
    mode_code = jnp.broadcast_to(code_of(jnp.max(peak, axis=0, keepdims=True)), (8, 128))
    scale = (1.0 / unit_of(mode_code))[None]
    words = join(whole(real * scale), whole(imag * scale))
    steps = (4, 8, 16, 32, 64)
    tiles = swap_bits([words[t] for t in range(32)], steps)
    for t in range(devices):
        modes[t, 0:8] = tiles[t]
    tiles = swap_bits([words[32 + t] for t in range(16)] + [mode_code] * 16, steps)
    for t in range(devices):
        modes[t, 8:16] = tiles[t]
    moved = send_all(modes, arrived, mode_sems, True)

    reply_code = code_of(peak_of(jnp.abs(velocity_ref[...].reshape(-1, 8, size_z))))
    scale = 1.0 / unit_of(reply_code)
    cells = []
    for brick_x in range(bricks_x):
        piece = velocity_ref[:, brick_x * 8 : (brick_x + 1) * 8].reshape(192, size_z)
        cells.append(parts(jnp.round(piece * scale)))
    for at in range(columns):
        wide = None
        for brick_x in range(bricks_x):
            chosen = select[
                brick_x * size_z : (brick_x + 1) * size_z, at * 128 : (at + 1) * 128
            ]
            piece = mul(cells[brick_x][0], chosen) + mul(cells[brick_x][1], chosen)
            wide = piece if wide is None else wide + piece
        tiles = pack_cubes(wide, lane8)
        for t in range(9):
            reply[at, t * 8 : t * 8 + 8] = tiles[t]
        reply[at, 72:80] = jnp.broadcast_to(reply_code, (8, 128))
    replies = send_all(reply, replied, reply_sems, False)

    receive(moved)
    here = row * columns + col
    first = here == 0
    upper = jnp.logical_not(low_half)
    lines = [[[] for _ in range(3)] for _ in range(4)]
    for at in range(columns):
        zero = swap_bits([arrived[r * columns + at, 0:8] for r in range(rows)], (1, 2))
        rest_tiles = swap_bits([arrived[r * columns + at, 8:16] for r in range(rows)], (1, 2))
        for mode in range(4):
            code = jnp.where(low_half, roll(rest_tiles[mode], 64), rest_tiles[mode])
            unit = unit_of(code)
            real0, imag0 = (p.astype(F32) * unit for p in split(zero[mode]))
            real1, imag1 = (p.astype(F32) * unit for p in split(rest_tiles[mode]))
            lines[mode][0].append(jnp.where(low_half, real0, roll(imag0, 64)))
            lines[mode][1].append(jnp.where(low_half, roll(real0, 64), imag0))
            lines[mode][2].append(jnp.where(low_half, real1, roll(imag1, 64)))
    lines = [[jnp.concatenate(lines[mode][c], axis=0) for c in range(3)] for mode in range(4)]
    wide_y = columns * 8
    low_line = lanes_of((wide_y, 128)) < 64
    lines.append([jnp.where(low_line, roll(v, 64), 0.0) for v in lines[0]])
    lines[0] = [jnp.where(jnp.logical_and(first, jnp.logical_not(low_line)), 0.0, v) for v in lines[0]]
    line_table = (line_ref[0], line_ref[1])
    sign = jnp.where(low_line, 1.0, -1.0)
    lined = []
    for slot_at in range(5):
        both = mul3(line_table, parts(jnp.concatenate(lines[slot_at], axis=1)))
        for c in range(3):
            a = both[0:wide_y, c * 128 : (c + 1) * 128]
            b = both[wide_y:, c * 128 : (c + 1) * 128]
            lined.append(a + sign * roll(b, 64))
    full_x = rows * size_x
    index = lanes_of((wide_y, 128)) & (full_x - 1)
    line = lax.broadcasted_iota(I32, (wide_y, 128), 0)
    scale_x, scale_y, scale_z = (2.0 * np.pi / n for n in (full_x, wide_y, size_z))
    sig_x = jnp.where(index < full_x // 2, index, index - full_x).astype(F32) * scale_x
    sig_y = jnp.where(line < wide_y // 2, line, line - wide_y).astype(F32) * scale_y
    wave_x = jnp.where(index == full_x // 2, 0.0, sig_x)
    wave_y = jnp.where(line == wide_y // 2, 0.0, sig_y)
    backs = []
    for slot_at in range(5):
        spot_lines = jnp.concatenate(lined[slot_at * 3 : slot_at * 3 + 3], axis=0)
        values = mul3(parts(spot_lines), (wide_ref[0], wide_ref[1]))
        x, y, z = (values[c * wide_y : (c + 1) * wide_y] for c in range(3))
        if slot_at < 4:
            sig_z = (here * 4 + slot_at).astype(F32) * scale_z
            wave_z = sig_z
        else:
            sig_z, wave_z = F32(np.pi), F32(0.0)
        square = wave_x * wave_x + wave_y * wave_y + wave_z * wave_z
        full = sig_x * sig_x + sig_y * sig_y + sig_z * sig_z
        none = square == 0.0
        inverse_sq = jnp.where(none, 0.0, 1.0 / jnp.where(none, 1.0, square))
        damping = 1.0 / (1.0 + DT_STEP * VISCOSITY * full)
        normal = (wave_x * x + wave_y * y + wave_z * z) * inverse_sq
        result = jnp.concatenate(
            [
                (x - wave_x * normal) * damping,
                (y - wave_y * normal) * damping,
                (z - wave_z * normal) * damping,
            ],
            axis=0,
        )
        turned = mul3(parts(result), (unwide_ref[0], unwide_ref[1]))
        stacked = jnp.concatenate(
            [turned[c * wide_y : (c + 1) * wide_y] for c in range(3)], axis=1
        )
        both = mul3(line_table, parts(stacked))
        back = []
        for c in range(3):
            a = both[0:wide_y, c * 128 : (c + 1) * 128]
            b = both[wide_y:, c * 128 : (c + 1) * 128]
            back.append(a - sign * roll(b, 64))
        backs.append(back)
    top = jnp.logical_and(first, jnp.logical_not(low_line))
    backs[0] = [jnp.where(top, roll(backs[4][c], 64), backs[0][c]) for c in range(3)]
    zero_words, rest_words = [], []
    for mode in range(4):
        e = backs[mode]
        peak = jnp.maximum(jnp.maximum(jnp.abs(e[0]), jnp.abs(e[1])), jnp.abs(e[2]))
        code = code_of(peak_of(peak))
        scale = 1.0 / unit_of(code)
        e = [v * scale for v in e]
        real0 = whole(jnp.where(low_line, e[0], roll(e[1], 64)))
        imag0 = whole(jnp.where(low_line, roll(e[0], 64), e[1]))
        zero_words.append(join(real0, imag0))
        rest_words.append(jnp.where(low_line, join(whole(e[2]), whole(roll(e[2], 64))), code))
    for at in range(columns):
        span = slice(at * 8, at * 8 + 8)
        tiles = swap_bits([w[span] for w in zero_words], (1, 2))
        for r in range(rows):
            ready[r * columns + at, 0:8] = tiles[r]
        tiles = swap_bits([w[span] for w in rest_words], (1, 2))
        for r in range(rows):
            ready[r * columns + at, 8:16] = tiles[r]
    lasts = send_all(ready, last_ref, last_sems, True)

    receive(replies)
    for at in range(columns):
        tiles = [replied[at, t * 8 : t * 8 + 8] for t in range(9)]
        unit = unit_of(replied[at, 72:80])
        wide = open_cubes(tiles, lane8).reshape(24, 8, 128) * unit[None]
        high, low = parts(wide.reshape(192, 128))
        held[0, :, at * 128 : (at + 1) * 128] = high
        held[1, :, at * 128 : (at + 1) * 128] = low
    fetched = mul(held[0], place[...], NT) + mul(held[1], place[...], NT)
    for c in range(3):
        for g in range(2):
            tiles = [
                fetched[c * 64 + i * 8 : c * 64 + i * 8 + 8, g * 128 : (g + 1) * 128]
                for i in range(8)
            ]
            for b, tile in enumerate(swap_bits(tiles, (8, 16, 32))):
                cube[g * 8 + b, c] = tile

    low_rows = lanes_of((24, 128)) < 64

    def interpolate_pair(index, carry):
        block = index // 8 * 16 + lax.rem(index, 8)
        cells = cube[index].reshape(24, 128)
        apart = jnp.concatenate(
            [jnp.where(low_rows, cells, 0.0), jnp.where(low_rows, 0.0, cells)], axis=0
        )
        high, low = parts(apart)
        one, two = deep[block], deep[block + 8]
        upper = jnp.concatenate([one[0:64], two[0:64]], axis=0)
        lower = jnp.concatenate([one[64:128], two[64:128]], axis=0)
        summed = mul(high, upper) + mul(low, upper) + mul(high, lower)
        for half, at in ((0, block), (1, block + 8)):
            second = weight_ref[at, 1].astype(F32)
            piece = summed[half * 24 : half * 24 + 24].reshape(3, 8, 128) * second[None]
            piece = jnp.sum(piece, axis=1)
            for c in range(3):
                mark_ref[c, pl.ds(at, 1), :] = piece[c : c + 1]
        return carry

    lax.fori_loop(0, blocks // 2, interpolate_pair, 0, unroll=4)
    receive(lasts)
    for sent in (pushes, moved, replies, lasts):
        finish(sent)


def final_kernel(last_ref, back_ref, mark_ref, new_ref, out_ref):
    devices = last_ref.shape[0]
    steps = (4, 8, 16, 32, 64)
    words = swap_bits([last_ref[t, 0:8] for t in range(devices)], steps)
    rest = swap_bits([last_ref[t, 8:16] for t in range(devices)], steps)
    unit = unit_of(rest[16])
    words += rest[0:16]
    rows = []
    for word in words:
        real, imag = split(word)
        rows.append(jnp.concatenate([real.astype(F32) * unit, imag.astype(F32) * unit], axis=1))
    result = mul3(parts(jnp.concatenate(rows, axis=0)), (back_ref[0], back_ref[1]))
    new_ref[...] = result.reshape(new_ref.shape)
    out_ref[...] = mark_ref[...]


def local(velocity, positions, weights, stiffness, rest_sq, owner_column, brick_index):
    rows = lax.axis_size("row")
    columns = lax.axis_size("col")
    devices = rows * columns
    _, local_x, local_y, size_z = velocity.shape
    blocks = positions.shape[0]
    capacity = max(2, 3 * blocks // columns)
    fits = (
        local_x == 16 and local_y == 8 and size_z == 8 * devices and positions.shape[2] == 128
        and capacity == 12 and blocks == 32 and columns == 8 and rows == 4
    )
    if not fits:
        return general(
            velocity, positions, weights, stiffness, rest_sq, owner_column, brick_index
        )
    return fast(velocity, positions, weights, stiffness, rest_sq, owner_column, brick_index)


def fast(velocity, positions, weights, stiffness, rest_sq, owner_column, brick_index):
    rows = lax.axis_size("row")
    columns = lax.axis_size("col")
    devices = rows * columns
    _, local_x, local_y, size_z = velocity.shape
    blocks = positions.shape[0]
    capacity = max(2, 3 * blocks // columns)
    size_x, size_y = rows * local_x, columns * local_y
    fore, back, line, wide, unwide = build_tables(size_x, size_y, size_z, rows)
    vm = pl.BlockSpec(memory_space=VMEM)
    shape = jax.ShapeDtypeStruct
    cells = local_x // BRICK * size_z
    dma = pltpu.SemaphoreType.DMA
    last, marks = pl.pallas_call(
        partial(main_kernel, rows, columns, capacity),
        out_shape=[shape((devices, 16, 128), I32), shape((3, blocks, 128), F32)],
        in_specs=[vm] * 11,
        out_specs=[vm, vm],
        scratch_shapes=[
            VMEM((3, blocks, 128), F32),
            VMEM((blocks, 128, 128), BF16),
            VMEM((blocks, 3, 8, 128), F32),
            VMEM((blocks * 8, columns * 128), BF16),
            VMEM((2, 3, local_y, size_z), F32),
            VMEM((2, 3, local_x, size_z), F32),
            VMEM((2, 3, local_y, size_z), F32),
            VMEM((2, 3, local_x, size_z), F32),
            VMEM((columns, 80, 128), I32),
            VMEM((columns, 80, 128), I32),
            VMEM((3, local_x, local_y, size_z), F32),
            VMEM((cells, columns * 128), BF16),
            VMEM((2, 192, columns * 128), BF16),
            VMEM((devices, 16, 128), I32),
            VMEM((devices, 16, 128), I32),
            VMEM((columns, 80, 128), I32),
            VMEM((columns, 80, 128), I32),
            VMEM((devices, 16, 128), I32),
            dma((2, 4)),
            dma((2, columns)),
            dma((2, devices)),
            dma((2, columns)),
            dma((2, devices)),
        ],
        compiler_params=pltpu.CompilerParams(collective_id=1, has_side_effects=True),
        name="step",
    )(
        owner_column.reshape(1, blocks), brick_index.reshape(1, blocks),
        stiffness.reshape(1, blocks), rest_sq.reshape(1, blocks),
        positions.transpose(1, 0, 2), weights, velocity, fore, line, wide, unwide,
    )
    new_velocity, marks = pl.pallas_call(
        final_kernel,
        out_shape=[shape(velocity.shape, F32), shape((3, blocks, 128), F32)],
        in_specs=[vm, vm, vm],
        out_specs=[vm, vm],
        name="final",
    )(last, back, marks)
    return new_velocity, marks.transpose(1, 0, 2)


def solution(mesh):
    return jax.shard_map(
        local,
        mesh=mesh,
        in_specs=(
            P(None, "row", "col", None),
            P(("row", "col"), None, None),
            P(("row", "col"), None, None, None),
            P(("row", "col")),
            P(("row", "col")),
            P(("row", "col"), None),
            P(("row", "col")),
        ),
        out_specs=(P(None, "row", "col", None), P(("row", "col"), None, None)),
        check_vma=False,
    )
```

```python
from functools import partial

import numpy as np

import jax
import jax.numpy as jnp
from jax import lax
from jax.experimental import pallas as pl
from jax.experimental.pallas import tpu as pltpu
from jax.sharding import PartitionSpec as P

BRICK = 8


DT_STEP = 0.5
VISCOSITY = 0.1
PRECISE = lax.Precision.HIGHEST


def with_halo(block, sides, width):
    for axis, dim in sides:
        count = lax.axis_size(axis)
        forward = [(i, i + 1) for i in range(count - 1)]
        forward.append((count - 1, 0))
        backward = [(target, source) for source, target in forward]
        low = lax.ppermute(
            lax.slice_in_dim(block, block.shape[dim] - width, None, axis=dim), axis, forward
        )
        high = lax.ppermute(lax.slice_in_dim(block, 0, width, axis=dim), axis, backward)
        block = jnp.concatenate([low, block, high], axis=dim)
    return block


def to_bricks(values):
    components, size_x, size_y, size_z = values.shape
    blocks_view = values.reshape(
        components, size_x // BRICK, BRICK, size_y // BRICK, BRICK, size_z // BRICK, BRICK
    )
    blocks_view = blocks_view.transpose(1, 3, 5, 0, 2, 4, 6)
    return blocks_view.reshape(-1, components * BRICK * BRICK * BRICK)


def from_bricks(bricks, size_x, size_y, size_z):
    blocks_view = bricks.reshape(
        size_x // BRICK, size_y // BRICK, size_z // BRICK, 3, BRICK, BRICK, BRICK
    )
    blocks_view = blocks_view.transpose(3, 0, 4, 1, 5, 2, 6)
    return blocks_view.reshape(3, size_x, size_y, size_z)


def chain_force(positions_f, stiffness_f, rest_f):
    segment = jnp.roll(positions_f, -1, axis=2) - positions_f
    stretch = jnp.sum(segment * segment, axis=1, keepdims=True) / rest_f[:, None, None]
    tension = 0.5 * stiffness_f[:, None, None] * (stretch - 1.0) * segment
    return tension - jnp.roll(tension, 1, axis=2)


def interpolate(bricks_in, weights_f):
    cubes = bricks_in.reshape(-1, 3, BRICK, BRICK, BRICK)
    reduced = jnp.einsum("ncijk,nkm->ncijm", cubes, weights_f[:, 2], precision=PRECISE)
    reduced = jnp.einsum("ncijm,njm->ncim", reduced, weights_f[:, 1], precision=PRECISE)
    return jnp.einsum("ncim,nim->ncm", reduced, weights_f[:, 0], precision=PRECISE)


def spread(forces, weights_f):
    partial_sum = jnp.einsum("ncm,nim->ncim", forces, weights_f[:, 0], precision=PRECISE)
    partial_sum = jnp.einsum("ncim,njm->ncijm", partial_sum, weights_f[:, 1], precision=PRECISE)
    cubes = jnp.einsum("ncijm,nkm->ncijk", partial_sum, weights_f[:, 2], precision=PRECISE)
    return cubes.reshape(cubes.shape[0], -1)


def signed_modes(indices, length):
    return jnp.where(indices <= (length - 1) // 2, indices, indices - length)


def direction_modes(indices, length):
    return jnp.where(2 * indices == length, 0, signed_modes(indices, length))


def tables(length):
    indices = jnp.arange(length, dtype=jnp.int32)
    phases = indices[:, None] * indices[None, :] % length
    angles = 2.0 * jnp.pi / length * phases.astype(jnp.float32)
    return (jnp.cos(angles), jnp.sin(angles))


def forward(form, real_part, imag_part, length):
    cosine, sine = tables(length)
    product = partial(jnp.einsum, precision=PRECISE)
    out_real = product(form, real_part, cosine) + product(form, imag_part, sine)
    out_imag = product(form, imag_part, cosine) - product(form, real_part, sine)
    return (out_real, out_imag)


def backward(form, real_part, imag_part, length):
    cosine, sine = tables(length)
    product = partial(jnp.einsum, precision=PRECISE)
    out_real = product(form, real_part, cosine) - product(form, imag_part, sine)
    out_imag = product(form, imag_part, cosine) + product(form, real_part, sine)
    return (out_real / length, out_imag / length)


def col_transpose(values):
    return lax.all_to_all(values, "col", split_axis=4, concat_axis=3, tiled=True)


def row_transpose(values):
    return lax.all_to_all(values, "row", split_axis=4, concat_axis=2, tiled=True)


def wave_parts(indices, length):
    scale = 2.0 * jnp.pi / length
    direct = direction_modes(indices, length)
    signed = signed_modes(indices, length)
    return (scale * direct.astype(jnp.float32), scale * signed.astype(jnp.float32), direct == 0)


def general(velocity, positions, weights, stiffness, rest_sq, owner_column, brick_index):
    row_count = lax.axis_size("row")
    col_count = lax.axis_size("col")
    size_x = velocity.shape[1]
    size_y = velocity.shape[2]
    size_z = velocity.shape[3]
    block_count = positions.shape[0]
    capacity = max(2, 3 * block_count // col_count)
    total_slots = col_count * capacity
    owner_col = owner_column[:, 0]
    order_ids = jnp.arange(block_count, dtype=jnp.int32)
    earlier_same = (owner_col[None, :] == owner_col[:, None]) & (
        order_ids[None, :] < order_ids[:, None]
    )
    slot_index = owner_col * capacity + jnp.sum(earlier_same.astype(jnp.int32), axis=1)
    stored = to_bricks(velocity)
    brick_count = stored.shape[0]

    def place(values, fill):
        buffer = jnp.full((total_slots,) + values.shape[1:], fill, values.dtype)
        return buffer.at[slot_index].set(values).reshape((col_count, capacity) + values.shape[1:])

    weights_f = weights.astype(jnp.float32)
    forces = chain_force(
        positions.astype(jnp.float32), stiffness.astype(jnp.float32), rest_sq.astype(jnp.float32)
    )
    pushed = spread(forces, weights_f)
    send_force = place(pushed, 0.0)
    send_index = place(brick_index.astype(jnp.float32), 0.0)
    wanted = lax.all_to_all(send_index, "col", split_axis=0, concat_axis=0, tiled=True)
    pushes = lax.all_to_all(send_force, "col", split_axis=0, concat_axis=0, tiled=True)
    wanted_ids = wanted.astype(jnp.int32)
    reply = stored[wanted_ids]
    returned = lax.all_to_all(reply, "col", split_axis=0, concat_axis=0, tiled=True)
    returned, arrived_ids, arrived = (returned, wanted_ids, pushes)
    fetched = returned.reshape(total_slots, -1)[slot_index]
    marker_velocity = interpolate(fetched, weights_f)
    forcing = jax.ops.segment_sum(
        arrived.reshape(total_slots, -1), arrived_ids.reshape(-1), num_segments=brick_count
    )
    force_field = from_bricks(forcing, size_x, size_y, size_z)
    padded = with_halo(velocity, (("row", 1), ("col", 2)), 1)
    grad_x = (padded[:, 2:, 1:-1] - padded[:, :-2, 1:-1]) * 0.5
    grad_y = (padded[:, 1:-1, 2:] - padded[:, 1:-1, :-2]) * 0.5
    grad_z = (jnp.roll(velocity, -1, axis=3) - jnp.roll(velocity, 1, axis=3)) * 0.5
    transport = velocity[0] * grad_x + velocity[1] * grad_y + velocity[2] * grad_z
    star = velocity + DT_STEP * (force_field - transport)
    cos_z, sin_z = tables(size_z)
    half_z = size_z // 2
    col_here = lax.axis_index("col")
    cos_fore = cos_z[:, :half_z]
    sin_fore = sin_z[:, :half_z].at[:, 0].set(-cos_z[:, half_z])
    z_real = jnp.einsum("cxyz,zk->cxyk", star, cos_fore, precision=PRECISE)
    z_imag = -jnp.einsum("cxyz,zk->cxyk", star, sin_fore, precision=PRECISE)
    shuffled = col_transpose(jnp.stack([z_real, z_imag]))
    slab = shuffled.shape[4]
    first_slot = (col_here == 0) & (jnp.arange(slab, dtype=jnp.int32) == 0)
    highest = shuffled[1][..., 0:1] * (col_here == 0).astype(jnp.float32)
    lower_imag = jnp.where(first_slot, 0.0, shuffled[1])
    y_in_real = jnp.concatenate([shuffled[0], highest], axis=3)
    y_in_imag = jnp.concatenate([lower_imag, jnp.zeros_like(highest)], axis=3)
    z_index = jnp.concatenate(
        [col_here * slab + jnp.arange(slab, dtype=jnp.int32), jnp.full((1,), half_z, jnp.int32)]
    )
    y_real, y_imag = forward("cxyz,yk->cxzk", y_in_real, y_in_imag, y_in_real.shape[2])
    shuffled = row_transpose(jnp.stack([y_real, y_imag]))
    x_real, x_imag = forward("cxzy,xk->czyk", shuffled[0], shuffled[1], shuffled.shape[2])
    slab_y = x_real.shape[2]
    full_x = x_real.shape[3]
    full_y = slab_y * row_count
    y_index = lax.axis_index("row") * slab_y + jnp.arange(slab_y, dtype=jnp.int32)
    x_index = jnp.arange(full_x, dtype=jnp.int32)
    dir_z, sig_z, zero_z = wave_parts(z_index, size_z)
    dir_y, sig_y, zero_y = wave_parts(y_index, full_y)
    dir_x, sig_x, zero_x = wave_parts(x_index, full_x)
    wave_z = dir_z[:, None, None]
    wave_y = dir_y[None, :, None]
    wave_x = dir_x[None, None, :]
    no_direction = zero_z[:, None, None] & zero_y[None, :, None] & zero_x[None, None, :]
    wave_sq = wave_x * wave_x + wave_y * wave_y + wave_z * wave_z
    full_sq = sig_z[:, None, None] ** 2 + sig_y[None, :, None] ** 2 + sig_x[None, None, :] ** 2
    inverse_sq = jnp.where(no_direction, 0.0, 1.0 / jnp.where(no_direction, 1.0, wave_sq))
    damping = 1.0 / (1.0 + DT_STEP * VISCOSITY * full_sq)
    waves = jnp.stack(
        [
            jnp.broadcast_to(wave_x, wave_sq.shape),
            jnp.broadcast_to(wave_y, wave_sq.shape),
            jnp.broadcast_to(wave_z, wave_sq.shape),
        ]
    )
    normal_real = jnp.sum(waves * x_real, axis=0) * inverse_sq
    normal_imag = jnp.sum(waves * x_imag, axis=0) * inverse_sq
    p_real = (x_real - waves * normal_real) * damping
    p_imag = (x_imag - waves * normal_imag) * damping
    b_real, b_imag = backward("czyk,kx->cyzx", p_real, p_imag, full_x)
    shuffled = row_transpose(jnp.stack([b_real, b_imag]))
    b_real, b_imag = backward("cyzx,yk->cxzk", shuffled[0], shuffled[1], shuffled.shape[2])
    slab = b_real.shape[2] - 1
    first_slot = (col_here == 0) & (jnp.arange(slab, dtype=jnp.int32) == 0)
    highest = b_real[:, :, slab:, :]
    packed_imag = jnp.where(first_slot[None, None, :, None], highest, b_imag[:, :, :slab, :])
    shuffled = col_transpose(jnp.stack([b_real[:, :, :slab, :], packed_imag]))
    doubling = jnp.where(jnp.arange(half_z, dtype=jnp.int32) == 0, 1.0, 2.0)[:, None]
    cos_back = cos_z[:half_z] * doubling
    sin_back = (sin_z[:half_z] * doubling).at[0].set(-cos_z[half_z])
    new_velocity = (
        jnp.einsum("cxky,kz->cxyz", shuffled[0], cos_back, precision=PRECISE)
        - jnp.einsum("cxky,kz->cxyz", shuffled[1], sin_back, precision=PRECISE)
    ) / size_z
    return (new_velocity, marker_velocity)


VMEM = pltpu.VMEM
MESH = pl.DeviceIdType.MESH
F32 = jnp.float32
BF16 = jnp.bfloat16
I32 = jnp.int32
TOP = 32700.0
NT = ((1,), (1,))


def two_parts(table):
    table = np.asarray(table, np.float64)
    high = table.astype(jnp.bfloat16)
    low = (table - high.astype(np.float64)).astype(jnp.bfloat16)
    return np.stack([high, low])


def angle_of(length, left, right):
    return 2.0 * np.pi / length * (np.outer(left, right) % length)


def build_tables(size_x, size_y, size_z, rows):
    half_z = size_z // 2
    turn = angle_of(size_z, np.arange(size_z), np.arange(half_z))
    fore = np.concatenate([np.cos(turn), -np.sin(turn)], axis=1)
    back = np.concatenate([2.0 * np.cos(turn), -2.0 * np.sin(turn)], axis=1)
    alternate = np.where(np.arange(size_z) % 2 == 0, 1.0, -1.0)
    fore[:, half_z] = alternate
    back[:, 0], back[:, half_z] = 1.0, alternate
    back = back.T / (size_x * size_y * size_z)
    turn_y = angle_of(size_y, np.arange(size_y), np.arange(size_y))
    line = np.concatenate([np.cos(turn_y), np.sin(turn_y)], axis=0)
    lane = np.arange(size_x)
    place = (lane % rows) * (size_x // rows) + lane // rows
    turn_x = angle_of(size_x, place, np.arange(size_x))
    cosine, sine = np.cos(turn_x), np.sin(turn_x)
    wide = np.concatenate(
        [np.concatenate([cosine, -sine], axis=1), np.concatenate([sine, cosine], axis=1)], axis=0
    )
    return tuple(two_parts(t) for t in (fore, back, line, wide, wide.T))


def parts(values):
    high = values.astype(BF16)
    return high, (values - high.astype(F32)).astype(BF16)


def mul(left, right, dims=((1,), (0,))):
    return lax.dot_general(left, right, (dims, ((), ())), preferred_element_type=F32)


def mul3(left, right, dims=((1,), (0,))):
    return (
        mul(left[0], right[0], dims) + mul(left[1], right[0], dims) + mul(left[0], right[1], dims)
    )


def roll(values, shift):
    return pltpu.roll(values, shift % 128, values.ndim - 1)


def lanes_of(shape):
    return lax.broadcasted_iota(I32, shape, len(shape) - 1)


def code_of(peak):
    return jnp.floor(jnp.log2(jnp.maximum(peak, 1e-30)) * 65536.0).astype(I32) + 2


def unit_of(code):
    return jnp.exp2(code.astype(F32) * (1.0 / 65536.0)) * (1.0 / TOP)


def whole(values):
    return jnp.round(values).astype(I32)


def join(first, second):
    return (first << 16) + second


def split(word):
    second = (word << 16) >> 16
    return (word - second) >> 16, second


def swap_bits(tiles, steps):
    tiles = list(tiles)
    keep = {s: (lanes_of(tiles[0].shape) & s) == 0 for s in steps}
    for bit, step in enumerate(steps):
        for one in range(len(tiles)):
            if one >> bit & 1:
                continue
            two = one | 1 << bit
            a, b = tiles[one], tiles[two]
            tiles[one] = jnp.where(keep[step], a, roll(b, step))
            tiles[two] = jnp.where(keep[step], roll(a, -step), b)
    return tiles


def compress(tiles, lane):
    out = []
    for t in range(9):
        out.append(jnp.where(lane < 96, tiles[t], roll(tiles[9 + t // 3], 96 - 32 * (t % 3))))
    return out


def expand(tiles, lane):
    out = list(tiles)
    for u in range(3):
        a, b, c = (roll(tiles[3 * u + p], 32 + 32 * p) for p in range(3))
        out.append(jnp.where(lane < 32, a, jnp.where(lane < 64, b, c)))
    return out


def pack_cubes(wide, lane):
    tiles = [wide[t * 8 : t * 8 + 8].astype(I32) for t in range(24)]
    words = []
    for c in range(3):
        for i in range(4):
            words.append(join(tiles[c * 8 + i], tiles[c * 8 + i + 4]))
    return compress(words, lane)


def open_cubes(tiles, lane):
    out = [None] * 24
    for t, word in enumerate(expand(tiles, lane)):
        at = t // 4 * 8 + t % 4
        out[at], out[at + 4] = split(word)
    return jnp.concatenate([t.astype(F32) for t in out], axis=0)


def pad(tile):
    return jnp.concatenate([tile, jnp.zeros((3, 128), I32)], axis=0)


def fold(tile, low, near):
    other = pltpu.roll(roll(tile, 64), 4, 0)
    return jnp.where(jnp.logical_or(low, jnp.logical_not(near)), tile, other)


def unfold(tile, near):
    return jnp.where(near, tile, pltpu.roll(roll(tile, 64), 4, 0))


def peak_of(values):
    while values.ndim > 2:
        values = jnp.max(values, axis=0)
    return jnp.max(jnp.max(values, axis=0, keepdims=True), axis=1, keepdims=True)


def column(row):
    shape = (row.shape[1], row.shape[1])
    diagonal = lax.broadcasted_iota(I32, shape, 0) == lax.broadcasted_iota(I32, shape, 1)
    return jnp.sum(jnp.where(diagonal, row, 0.0), axis=1, keepdims=True)


def mix(step, cols):
    ring, pair = step // cols, step % cols
    return ((6, 2, 4, 7, 3, 5, 1, 0).index(pair % 8), (2, 1, 3, 0).index(ring % 4), step)


def main_kernel(
    rows, columns, capacity,
    owner_hbm, brick_hbm, stiff_hbm, rest_hbm, pos_hbm, weight_hbm, velocity_hbm,
    fore_hbm, line_hbm, wide_hbm, unwide_hbm,
    last_ref, mark_ref,
    owner_ref, brick_ref, stiff_ref, rest_ref, pos_ref, weight_ref, velocity_ref,
    fore_ref, line_ref, wide_ref, unwide_ref, noted,
    force, deep, cube, place, face_x, face_y, near_x, near_y, push, pushed, star, select,
    held, modes, arrived, reply, replied, ready,
    load_sems, face_sems, push_sems, mode_sems, reply_sems, last_sems,
):
    sources = (
        owner_hbm, brick_hbm, stiff_hbm, rest_hbm, pos_hbm, weight_hbm, velocity_hbm,
        fore_hbm, line_hbm, wide_hbm, unwide_hbm,
    )
    targets = (
        owner_ref, brick_ref, stiff_ref, rest_ref, pos_ref, weight_ref, velocity_ref,
        fore_ref, line_ref, wide_ref, unwide_ref,
    )
    loads = []
    for number, (source, target) in enumerate(zip(sources, targets)):
        loads.append(pltpu.make_async_copy(source, target, load_sems.at[number]))
        loads[-1].start()
    row, col = lax.axis_index("row"), lax.axis_index("col")
    devices = rows * columns
    blocks = pos_ref.shape[1]
    size_x, size_y, size_z = velocity_ref.shape[1:]
    bricks_x = size_x // 8
    barrier = pltpu.get_barrier_semaphore()

    def flip(step):
        at, bit = 0, 1
        while bit < columns:
            own = lax.rem(col // bit, 2)
            at = at + bit * (1 - own if step & bit else own)
            bit *= 2
        return at

    def peer(step):
        to_row, to_col = lax.rem(row + step // columns, rows), flip(step % columns)
        return (to_row, to_col), to_row * columns + to_col

    greet = list(range(1, columns)) + list(range(columns, devices, columns))
    for step in greet:
        pl.semaphore_signal(barrier, inc=1, device_id=peer(step)[0], device_id_type=MESH)

    def remote(source, target, sems, step, device):
        return pltpu.make_async_remote_copy(
            source, target, sems.at[0, step], sems.at[1, step],
            device_id=device, device_id_type=MESH,
        )

    def send_all(source, target, sems, around):
        waits = []
        count = devices if around else columns
        me = row * columns + col if around else col
        for step in sorted(range(1, count), key=lambda n: mix(n, columns)):
            device, at = peer(step)
            at = at if around else device[1]
            copy = remote(source.at[at], target.at[me], sems, step, device)
            copy.start()
            opposite = (rows - step // columns) % rows * columns + step % columns
            origin_device, origin = peer(opposite)
            origin = origin if around else origin_device[1]
            arrival = remote(source.at[at], target.at[origin], sems, step, device)
            waits.append((copy, arrival))
        own = pltpu.make_async_copy(source.at[me], target.at[me], sems.at[0, 0])
        own.start()
        return waits, own

    def receive(sent):
        for _, arrival in sent[0]:
            arrival.wait_recv()
        sent[1].wait()

    def finish(sent):
        for copy, _ in sent[0]:
            copy.wait_send()

    lane8 = lanes_of((8, 128))
    near = lax.broadcasted_iota(I32, (8, 128), 0) < 4

    for load in loads[:4]:
        load.wait()
    owner_row = owner_ref[...].astype(F32)
    owner = column(owner_row)
    shape = (blocks, blocks)
    earlier = lax.broadcasted_iota(I32, shape, 1) < lax.broadcasted_iota(I32, shape, 0)
    rank = jnp.sum(
        jnp.where((owner == owner_row) & earlier, 1.0, 0.0), axis=1, keepdims=True
    )
    slot = jnp.broadcast_to(owner * 128.0 + rank * 8.0, (blocks, 128))
    brick = jnp.broadcast_to(column(brick_ref[...].astype(F32)) + 1.0, (blocks, 128))
    deep_shape = (blocks, 8, 128)
    inner = lax.broadcasted_iota(I32, deep_shape, 1).astype(F32)
    slot = (slot[:, None, :] + inner).reshape(blocks * 8, 128)
    brick = jnp.broadcast_to(brick[:, None, :], deep_shape).reshape(blocks * 8, 128)
    lane_f = lanes_of((blocks * 8, 128)).astype(F32)
    for at in range(columns):
        hit = slot == lane_f + 128.0 * at
        place[:, at * 128 : (at + 1) * 128] = jnp.where(hit, 1.0, 0.0).astype(BF16)
        named = jnp.sum(jnp.where(hit, brick, 0.0), axis=0, keepdims=True).astype(I32)
        noted[at] = jnp.broadcast_to(named, (8, 128))

    for load in loads[4:6]:
        load.wait()
    stiff = column(stiff_ref[...].astype(F32))
    rest = column(rest_ref[...].astype(F32))
    points = [pos_ref[c].astype(F32) for c in range(3)]
    segment = [pltpu.roll(p, 127, 1) - p for p in points]
    stretch = sum(part * part for part in segment) / rest
    pull = 0.5 * stiff * (stretch - 1.0)
    for c in range(3):
        tension = pull * segment[c]
        force[c] = tension - pltpu.roll(tension, 1, 1)

    def spread(index, carry):
        first = weight_ref[index, 0].astype(F32)
        second = weight_ref[index, 1].astype(F32)
        third = weight_ref[index, 2].astype(F32)
        high, low = parts((first[:, None, :] * third[None]).reshape(64, 128))
        both = jnp.concatenate([high, low], axis=0)
        deep[index] = both
        pushes = jnp.concatenate([force[c, pl.ds(index, 1), :] * second for c in range(3)], axis=0)
        upper = pushes.astype(BF16).astype(F32)
        left = jnp.concatenate([upper, pushes - upper], axis=0).astype(BF16)
        result = mul(left, both, NT)
        total = result[0:24] + result[24:48]
        total = total + pltpu.roll(total, 64, 1)
        cube[index] = total.reshape(3, 8, 128)
        return carry

    lax.fori_loop(0, blocks, spread, 0, unroll=8)

    low_half = lane8 < 64
    outs = [[None] * 2 for _ in range(24)]
    for c in range(3):
        for g in range(2):
            tiles = [
                jnp.where(low_half, cube[g * 16 + b, c], cube[g * 16 + 8 + b, c]) for b in range(8)
            ]
            for i, tile in enumerate(swap_bits(tiles, (8, 16, 32))):
                outs[c * 8 + i][g] = tile
    spreads = jnp.concatenate([jnp.concatenate(pair, axis=1) for pair in outs], axis=0)
    push_code = code_of(peak_of(jnp.abs(spreads)))
    high, low = parts(jnp.round(spreads * (1.0 / unit_of(push_code))))

    for load in loads[6:]:
        load.wait()
    value_code = code_of(peak_of(jnp.abs(velocity_ref[...].reshape(-1, 8, size_z))))
    scale = 1.0 / unit_of(value_code)
    half = size_x // 2
    for side, at in ((0, size_x - 1), (1, 0)):
        cells = whole(velocity_ref[:, at] * scale[None])
        face_x[side, 0:24] = join(cells[:, :, 0:128], cells[:, :, 128:256]).reshape(24, 128)
        face_x[side, 24:25] = jnp.broadcast_to(value_code, (1, 128))
    for side, at in ((0, size_y - 1), (1, 0)):
        cells = whole(velocity_ref[:, :, at, :] * scale[None])
        face_y[side, 0:24] = join(cells[:, 0:half], cells[:, half:]).reshape(24, size_z)
        face_y[side, 24:25] = jnp.broadcast_to(value_code, (1, size_z))

    pl.semaphore_wait(barrier, len(greet))
    faces = []
    for source, target, base, axis in ((face_x, near_x, 0, 0), (face_y, near_y, 2, 1)):
        for side in range(2):
            extent = (rows, columns)[axis]
            step = 1 if side == 0 else extent - 1
            if axis == 0:
                device = (lax.rem(row + step, rows), col)
            else:
                device = (row, lax.rem(col + step, columns))
            copy = remote(source.at[side], target.at[side], face_sems, base + side, device)
            copy.start()
            faces.append(copy)

    near_order = sorted(range(1, columns), key=lambda n: mix(n, columns))
    pushes, waiting = [], None
    for step in near_order + [0]:
        device, _ = peer(step)
        at = device[1]
        window = place[:, pl.ds(pl.multiple_of(at * 128, 128), 128)]
        tiles = pack_cubes(mul(high, window) + mul(low, window), lane8)
        target = push if step else pushed
        for t in range(9):
            target[at, t * 8 : t * 8 + 8] = tiles[t]
        target[at, 72:73] = jnp.where(lane8[0:1] < 96, noted[at, 0:1], push_code)
        if waiting is not None:
            waiting.start()
        if step:
            waiting = remote(push.at[at], pushed.at[col], push_sems, step, device)
            arrival = remote(push.at[at], pushed.at[at], push_sems, step, device)
            pushes.append((waiting, arrival))

    for copy in faces:
        copy.wait()
    value = velocity_ref[...]
    sides_x, sides_y = [], []
    for side in range(2):
        unit = unit_of(near_x[side, 24:25])[:, 0:1]
        one, two = split(near_x[side, 0:24])
        wide = jnp.concatenate([one.astype(F32), two.astype(F32)], axis=1) * unit
        sides_x.append(wide.reshape(3, 1, size_y, size_z))
        unit = unit_of(near_y[side, 24:25])[:, 0:1]
        one, two = (part.astype(F32) * unit for part in split(near_y[side, 0:24]))
        wide = [part.reshape(3, half, size_z) for part in (one, two)]
        sides_y.append(jnp.concatenate(wide, axis=1).reshape(3 * size_x, 1, size_z))
    ahead = jnp.concatenate([value[:, 1:], sides_x[1]], axis=1)
    behind = jnp.concatenate([sides_x[0], value[:, :-1]], axis=1)
    transport = value[0:1] * ((ahead - behind) * 0.5)
    flat = value.reshape(3 * size_x, size_y, size_z)
    sub = lax.broadcasted_iota(I32, flat.shape, 1)
    face_low, face_high = sides_y
    ahead = jnp.where(sub == size_y - 1, face_high, pltpu.roll(flat, size_y - 1, 1))
    behind = jnp.where(sub == 0, face_low, pltpu.roll(flat, 1, 1))
    transport += value[1:2] * ((ahead - behind) * 0.5).reshape(value.shape)
    ahead = pltpu.roll(flat, size_z - 1, 2)
    behind = pltpu.roll(flat, 1, 2)
    transport += value[2:3] * ((ahead - behind) * 0.5).reshape(value.shape)
    star[...] = value - DT_STEP * transport

    spot = lax.broadcasted_iota(I32, (bricks_x * size_z, 128), 0)
    inner = lanes_of((1, 128)) & 7
    origins = [0] + near_order
    for k, step in enumerate(origins):
        if step:
            pushes[k - 1][1].wait_recv()
        at = peer(step)[0][1]
        tiles = [pushed[at, t * 8 : t * 8 + 8] for t in range(9)]
        meta = pushed[at, 72:73]
        unit = unit_of(meta)[:, 127:128]
        wide = open_cubes(tiles, lane8).reshape(24, 8, 128) * unit[None]
        high, low = parts(wide.reshape(192, 128))
        held[0, :, k * 128 : (k + 1) * 128] = high
        held[1, :, k * 128 : (k + 1) * 128] = low
        mark = jnp.where((lanes_of((1, 128)) < 96) & (meta > 0), (meta - 1) * 8 + inner, -1)
        select[:, k * 128 : (k + 1) * 128] = jnp.where(spot == mark, 1.0, 0.0).astype(BF16)
    for brick_x in range(bricks_x):
        chosen = select[brick_x * size_z : (brick_x + 1) * size_z]
        field = mul(held[0], chosen, NT) + mul(held[1], chosen, NT)
        star[:, brick_x * 8 : (brick_x + 1) * 8] += DT_STEP * field.reshape(3, 8, 8, size_z)

    spectrum = mul3(parts(star[...].reshape(-1, size_z)), (fore_ref[0], fore_ref[1]))
    real = spectrum[:, 0:128].reshape(3 * size_x, 8, 128)
    imag = spectrum[:, 128:256].reshape(3 * size_x, 8, 128)
    peak = jnp.maximum(jnp.max(jnp.abs(real), axis=0), jnp.max(jnp.abs(imag), axis=0))
    mode_code = jnp.broadcast_to(code_of(jnp.max(peak, axis=0, keepdims=True)), (8, 128))
    scale = (1.0 / unit_of(mode_code))[None]
    words = join(whole(real * scale), whole(imag * scale))
    steps = (4, 8, 16, 32, 64)
    tiles = swap_bits([words[t] for t in range(32)], steps)
    for t in range(devices):
        modes[t, 0:8] = tiles[t]
    tiles = swap_bits([words[32 + t] for t in range(16)] + [mode_code] * 16, steps)
    for t in range(devices):
        modes[t, 8:13] = fold(tiles[t], low_half, near)[0:5]
    moved = send_all(modes, arrived, mode_sems, True)

    scale = 1.0 / unit_of(value_code)
    cells = []
    for brick_x in range(bricks_x):
        piece = velocity_ref[:, brick_x * 8 : (brick_x + 1) * 8].reshape(192, size_z)
        cells.append(parts(jnp.round(piece * scale)))
    for k, step in enumerate(origins):
        at = peer(step)[0][1]
        wide = None
        for brick_x in range(bricks_x):
            chosen = select[
                brick_x * size_z : (brick_x + 1) * size_z, k * 128 : (k + 1) * 128
            ]
            piece = mul(cells[brick_x][0], chosen) + mul(cells[brick_x][1], chosen)
            wide = piece if wide is None else wide + piece
        tiles = pack_cubes(wide, lane8)
        for t in range(9):
            reply[at, t * 8 : t * 8 + 8] = tiles[t]
        reply[at, 72:73] = jnp.broadcast_to(value_code, (1, 128))

    receive(moved)
    replies = send_all(reply, replied, reply_sems, False)
    here = row * columns + col
    first = here == 0
    upper = jnp.logical_not(low_half)
    lines = [[[] for _ in range(3)] for _ in range(4)]
    for at in range(columns):
        zero = swap_bits([arrived[r * columns + at, 0:8] for r in range(rows)], (1, 2))
        rest_tiles = swap_bits([pad(arrived[r * columns + at, 8:13]) for r in range(rows)], (1, 2))
        for mode in range(4):
            code = jnp.broadcast_to(rest_tiles[mode][4:5], (8, 128))
            unit = unit_of(jnp.where(low_half, roll(code, 64), code))
            real0, imag0 = (p.astype(F32) * unit for p in split(zero[mode]))
            real1, imag1 = (p.astype(F32) * unit for p in split(unfold(rest_tiles[mode], near)))
            lines[mode][0].append(jnp.where(low_half, real0, roll(imag0, 64)))
            lines[mode][1].append(jnp.where(low_half, roll(real0, 64), imag0))
            lines[mode][2].append(jnp.where(low_half, real1, roll(imag1, 64)))
    lines = [[jnp.concatenate(lines[mode][c], axis=0) for c in range(3)] for mode in range(4)]
    wide_y = columns * 8
    low_line = lanes_of((wide_y, 128)) < 64
    lines.append([jnp.where(low_line, roll(v, 64), 0.0) for v in lines[0]])
    lines[0] = [jnp.where(jnp.logical_and(first, jnp.logical_not(low_line)), 0.0, v) for v in lines[0]]
    line_table = (line_ref[0], line_ref[1])
    sign = jnp.where(low_line, 1.0, -1.0)
    lined = []
    for slot_at in range(5):
        both = mul3(line_table, parts(jnp.concatenate(lines[slot_at], axis=1)))
        for c in range(3):
            a = both[0:wide_y, c * 128 : (c + 1) * 128]
            b = both[wide_y:, c * 128 : (c + 1) * 128]
            lined.append(a + sign * roll(b, 64))
    full_x = rows * size_x
    index = lanes_of((wide_y, 128)) & (full_x - 1)
    line = lax.broadcasted_iota(I32, (wide_y, 128), 0)
    scale_x, scale_y, scale_z = (2.0 * np.pi / n for n in (full_x, wide_y, size_z))
    sig_x = jnp.where(index < full_x // 2, index, index - full_x).astype(F32) * scale_x
    sig_y = jnp.where(line < wide_y // 2, line, line - wide_y).astype(F32) * scale_y
    wave_x = jnp.where(index == full_x // 2, 0.0, sig_x)
    wave_y = jnp.where(line == wide_y // 2, 0.0, sig_y)
    backs = []
    for slot_at in range(5):
        spot_lines = jnp.concatenate(lined[slot_at * 3 : slot_at * 3 + 3], axis=0)
        values = mul3(parts(spot_lines), (wide_ref[0], wide_ref[1]))
        x, y, z = (values[c * wide_y : (c + 1) * wide_y] for c in range(3))
        if slot_at < 4:
            sig_z = (here * 4 + slot_at).astype(F32) * scale_z
            wave_z = sig_z
        else:
            sig_z, wave_z = F32(np.pi), F32(0.0)
        square = wave_x * wave_x + wave_y * wave_y + wave_z * wave_z
        full = sig_x * sig_x + sig_y * sig_y + sig_z * sig_z
        none = square == 0.0
        inverse_sq = jnp.where(none, 0.0, 1.0 / jnp.where(none, 1.0, square))
        damping = 1.0 / (1.0 + DT_STEP * VISCOSITY * full)
        normal = (wave_x * x + wave_y * y + wave_z * z) * inverse_sq
        result = jnp.concatenate(
            [
                (x - wave_x * normal) * damping,
                (y - wave_y * normal) * damping,
                (z - wave_z * normal) * damping,
            ],
            axis=0,
        )
        turned = mul3(parts(result), (unwide_ref[0], unwide_ref[1]))
        stacked = jnp.concatenate(
            [turned[c * wide_y : (c + 1) * wide_y] for c in range(3)], axis=1
        )
        both = mul3(line_table, parts(stacked))
        back = []
        for c in range(3):
            a = both[0:wide_y, c * 128 : (c + 1) * 128]
            b = both[wide_y:, c * 128 : (c + 1) * 128]
            back.append(a - sign * roll(b, 64))
        backs.append(back)
    top = jnp.logical_and(first, jnp.logical_not(low_line))
    backs[0] = [jnp.where(top, roll(backs[4][c], 64), backs[0][c]) for c in range(3)]
    zero_words, rest_words = [], []
    for mode in range(4):
        e = backs[mode]
        peak = jnp.maximum(jnp.maximum(jnp.abs(e[0]), jnp.abs(e[1])), jnp.abs(e[2]))
        code = code_of(peak_of(peak))
        scale = 1.0 / unit_of(code)
        e = [v * scale for v in e]
        real0 = whole(jnp.where(low_line, e[0], roll(e[1], 64)))
        imag0 = whole(jnp.where(low_line, roll(e[0], 64), e[1]))
        zero_words.append(join(real0, imag0))
        rest_words.append(jnp.where(low_line, join(whole(e[2]), whole(roll(e[2], 64))), code))
    for at in range(columns):
        span = slice(at * 8, at * 8 + 8)
        tiles = swap_bits([w[span] for w in zero_words], (1, 2))
        for r in range(rows):
            ready[r * columns + at, 0:8] = tiles[r]
        tiles = swap_bits([w[span] for w in rest_words], (1, 2))
        for r in range(rows):
            ready[r * columns + at, 8:13] = fold(tiles[r], low_half, near)[0:5]
    lasts = send_all(ready, last_ref, last_sems, True)

    receive(replies)
    for at in range(columns):
        tiles = [replied[at, t * 8 : t * 8 + 8] for t in range(9)]
        unit = unit_of(replied[at, 72:73])
        wide = open_cubes(tiles, lane8).reshape(24, 8, 128) * unit[None]
        high, low = parts(wide.reshape(192, 128))
        held[0, :, at * 128 : (at + 1) * 128] = high
        held[1, :, at * 128 : (at + 1) * 128] = low
    fetched = mul(held[0], place[...], NT) + mul(held[1], place[...], NT)
    for c in range(3):
        for g in range(2):
            tiles = [
                fetched[c * 64 + i * 8 : c * 64 + i * 8 + 8, g * 128 : (g + 1) * 128]
                for i in range(8)
            ]
            for b, tile in enumerate(swap_bits(tiles, (8, 16, 32))):
                cube[g * 8 + b, c] = tile

    low_rows = lanes_of((24, 128)) < 64

    def interpolate_pair(index, carry):
        block = index // 8 * 16 + lax.rem(index, 8)
        cells = cube[index].reshape(24, 128)
        apart = jnp.concatenate(
            [jnp.where(low_rows, cells, 0.0), jnp.where(low_rows, 0.0, cells)], axis=0
        )
        high, low = parts(apart)
        one, two = deep[block], deep[block + 8]
        upper = jnp.concatenate([one[0:64], two[0:64]], axis=0)
        lower = jnp.concatenate([one[64:128], two[64:128]], axis=0)
        summed = mul(high, upper) + mul(low, upper) + mul(high, lower)
        for half, at in ((0, block), (1, block + 8)):
            second = weight_ref[at, 1].astype(F32)
            piece = summed[half * 24 : half * 24 + 24].reshape(3, 8, 128) * second[None]
            piece = jnp.sum(piece, axis=1)
            for c in range(3):
                mark_ref[c, pl.ds(at, 1), :] = piece[c : c + 1]
        return carry

    lax.fori_loop(0, blocks // 2, interpolate_pair, 0, unroll=4)
    receive(lasts)
    for copy, _ in pushes:
        copy.wait_send()
    for sent in (moved, replies, lasts):
        finish(sent)


def final_kernel(last_ref, back_ref, mark_ref, new_ref, out_ref):
    devices = last_ref.shape[0]
    steps = (4, 8, 16, 32, 64)
    words = swap_bits([last_ref[t, 0:8] for t in range(devices)], steps)
    low = lanes_of((8, 128)) < 64
    near = lax.broadcasted_iota(I32, (8, 128), 0) < 4
    rest = []
    for t in range(devices):
        tile = pad(last_ref[t, 8:13])
        code = jnp.broadcast_to(tile[4:5], (8, 128))
        rest.append(jnp.where(low, unfold(tile, near), code))
    rest = swap_bits(rest, steps)
    unit = unit_of(rest[16])
    words += rest[0:16]
    rows = []
    for word in words:
        real, imag = split(word)
        rows.append(jnp.concatenate([real.astype(F32) * unit, imag.astype(F32) * unit], axis=1))
    result = mul3(parts(jnp.concatenate(rows, axis=0)), (back_ref[0], back_ref[1]))
    new_ref[...] = result.reshape(new_ref.shape)
    out_ref[...] = mark_ref[...]


def local(velocity, positions, weights, stiffness, rest_sq, owner_column, brick_index):
    rows = lax.axis_size("row")
    columns = lax.axis_size("col")
    devices = rows * columns
    _, local_x, local_y, size_z = velocity.shape
    blocks = positions.shape[0]
    capacity = max(2, 3 * blocks // columns)
    fits = (
        local_x == 16 and local_y == 8 and size_z == 8 * devices and positions.shape[2] == 128
        and capacity == 12 and blocks == 32 and columns == 8 and rows == 4
    )
    if not fits:
        return general(
            velocity, positions, weights, stiffness, rest_sq, owner_column, brick_index
        )
    return fast(velocity, positions, weights, stiffness, rest_sq, owner_column, brick_index)


def fast(velocity, positions, weights, stiffness, rest_sq, owner_column, brick_index):
    rows = lax.axis_size("row")
    columns = lax.axis_size("col")
    devices = rows * columns
    _, local_x, local_y, size_z = velocity.shape
    blocks = positions.shape[0]
    capacity = max(2, 3 * blocks // columns)
    size_x, size_y = rows * local_x, columns * local_y
    fore, back, line, wide, unwide = build_tables(size_x, size_y, size_z, rows)
    vm = pl.BlockSpec(memory_space=VMEM)
    shape = jax.ShapeDtypeStruct
    cells = local_x // BRICK * size_z
    dma = pltpu.SemaphoreType.DMA
    operands = (
        owner_column.reshape(1, blocks), brick_index.reshape(1, blocks),
        stiffness.reshape(1, blocks), rest_sq.reshape(1, blocks),
        positions.transpose(1, 0, 2), weights, velocity, fore, line, wide, unwide,
    )
    last, marks = pl.pallas_call(
        partial(main_kernel, rows, columns, capacity),
        out_shape=[shape((devices, 13, 128), I32), shape((3, blocks, 128), F32)],
        in_specs=[pl.BlockSpec(memory_space=pl.ANY)] * 11,
        out_specs=[vm, vm],
        scratch_shapes=[VMEM(a.shape, a.dtype) for a in operands] + [
            VMEM((columns, 8, 128), I32),
            VMEM((3, blocks, 128), F32),
            VMEM((blocks, 128, 128), BF16),
            VMEM((blocks, 3, 8, 128), F32),
            VMEM((blocks * 8, columns * 128), BF16),
            VMEM((2, 25, 128), I32),
            VMEM((2, 25, size_z), I32),
            VMEM((2, 25, 128), I32),
            VMEM((2, 25, size_z), I32),
            VMEM((columns, 73, 128), I32),
            VMEM((columns, 73, 128), I32),
            VMEM((3, local_x, local_y, size_z), F32),
            VMEM((cells, columns * 128), BF16),
            VMEM((2, 192, columns * 128), BF16),
            VMEM((devices, 13, 128), I32),
            VMEM((devices, 13, 128), I32),
            VMEM((columns, 73, 128), I32),
            VMEM((columns, 73, 128), I32),
            VMEM((devices, 13, 128), I32),
            dma((11,)),
            dma((2, 4)),
            dma((2, columns)),
            dma((2, devices)),
            dma((2, columns)),
            dma((2, devices)),
        ],
        compiler_params=pltpu.CompilerParams(collective_id=1, has_side_effects=True),
        name="step",
    )(*operands)
    new_velocity, marks = pl.pallas_call(
        final_kernel,
        out_shape=[shape(velocity.shape, F32), shape((3, blocks, 128), F32)],
        in_specs=[vm, vm, vm],
        out_specs=[vm, vm],
        name="final",
    )(last, back, marks)
    return new_velocity, marks.transpose(1, 0, 2)


def solution(mesh):
    return jax.shard_map(
        local,
        mesh=mesh,
        in_specs=(
            P(None, "row", "col", None),
            P(("row", "col"), None, None),
            P(("row", "col"), None, None, None),
            P(("row", "col")),
            P(("row", "col")),
            P(("row", "col"), None),
            P(("row", "col")),
        ),
        out_specs=(P(None, "row", "col", None), P(("row", "col"), None, None)),
        check_vma=False,
    )
```

```python
from functools import partial

import numpy as np

import jax
import jax.numpy as jnp
from jax import lax
from jax.experimental import pallas as pl
from jax.experimental.pallas import tpu as pltpu
from jax.sharding import PartitionSpec as P

BRICK = 8


DT_STEP = 0.5
VISCOSITY = 0.1
PRECISE = lax.Precision.HIGHEST


def with_halo(block, sides, width):
    for axis, dim in sides:
        count = lax.axis_size(axis)
        forward = [(i, i + 1) for i in range(count - 1)]
        forward.append((count - 1, 0))
        backward = [(target, source) for source, target in forward]
        low = lax.ppermute(
            lax.slice_in_dim(block, block.shape[dim] - width, None, axis=dim), axis, forward
        )
        high = lax.ppermute(lax.slice_in_dim(block, 0, width, axis=dim), axis, backward)
        block = jnp.concatenate([low, block, high], axis=dim)
    return block


def to_bricks(values):
    components, size_x, size_y, size_z = values.shape
    blocks_view = values.reshape(
        components, size_x // BRICK, BRICK, size_y // BRICK, BRICK, size_z // BRICK, BRICK
    )
    blocks_view = blocks_view.transpose(1, 3, 5, 0, 2, 4, 6)
    return blocks_view.reshape(-1, components * BRICK * BRICK * BRICK)


def from_bricks(bricks, size_x, size_y, size_z):
    blocks_view = bricks.reshape(
        size_x // BRICK, size_y // BRICK, size_z // BRICK, 3, BRICK, BRICK, BRICK
    )
    blocks_view = blocks_view.transpose(3, 0, 4, 1, 5, 2, 6)
    return blocks_view.reshape(3, size_x, size_y, size_z)


def chain_force(positions_f, stiffness_f, rest_f):
    segment = jnp.roll(positions_f, -1, axis=2) - positions_f
    stretch = jnp.sum(segment * segment, axis=1, keepdims=True) / rest_f[:, None, None]
    tension = 0.5 * stiffness_f[:, None, None] * (stretch - 1.0) * segment
    return tension - jnp.roll(tension, 1, axis=2)


def interpolate(bricks_in, weights_f):
    cubes = bricks_in.reshape(-1, 3, BRICK, BRICK, BRICK)
    reduced = jnp.einsum("ncijk,nkm->ncijm", cubes, weights_f[:, 2], precision=PRECISE)
    reduced = jnp.einsum("ncijm,njm->ncim", reduced, weights_f[:, 1], precision=PRECISE)
    return jnp.einsum("ncim,nim->ncm", reduced, weights_f[:, 0], precision=PRECISE)


def spread(forces, weights_f):
    partial_sum = jnp.einsum("ncm,nim->ncim", forces, weights_f[:, 0], precision=PRECISE)
    partial_sum = jnp.einsum("ncim,njm->ncijm", partial_sum, weights_f[:, 1], precision=PRECISE)
    cubes = jnp.einsum("ncijm,nkm->ncijk", partial_sum, weights_f[:, 2], precision=PRECISE)
    return cubes.reshape(cubes.shape[0], -1)


def signed_modes(indices, length):
    return jnp.where(indices <= (length - 1) // 2, indices, indices - length)


def direction_modes(indices, length):
    return jnp.where(2 * indices == length, 0, signed_modes(indices, length))


def tables(length):
    indices = jnp.arange(length, dtype=jnp.int32)
    phases = indices[:, None] * indices[None, :] % length
    angles = 2.0 * jnp.pi / length * phases.astype(jnp.float32)
    return (jnp.cos(angles), jnp.sin(angles))


def forward(form, real_part, imag_part, length):
    cosine, sine = tables(length)
    product = partial(jnp.einsum, precision=PRECISE)
    out_real = product(form, real_part, cosine) + product(form, imag_part, sine)
    out_imag = product(form, imag_part, cosine) - product(form, real_part, sine)
    return (out_real, out_imag)


def backward(form, real_part, imag_part, length):
    cosine, sine = tables(length)
    product = partial(jnp.einsum, precision=PRECISE)
    out_real = product(form, real_part, cosine) - product(form, imag_part, sine)
    out_imag = product(form, imag_part, cosine) + product(form, real_part, sine)
    return (out_real / length, out_imag / length)


def col_transpose(values):
    return lax.all_to_all(values, "col", split_axis=4, concat_axis=3, tiled=True)


def row_transpose(values):
    return lax.all_to_all(values, "row", split_axis=4, concat_axis=2, tiled=True)


def wave_parts(indices, length):
    scale = 2.0 * jnp.pi / length
    direct = direction_modes(indices, length)
    signed = signed_modes(indices, length)
    return (scale * direct.astype(jnp.float32), scale * signed.astype(jnp.float32), direct == 0)


def general(velocity, positions, weights, stiffness, rest_sq, owner_column, brick_index):
    row_count = lax.axis_size("row")
    col_count = lax.axis_size("col")
    size_x = velocity.shape[1]
    size_y = velocity.shape[2]
    size_z = velocity.shape[3]
    block_count = positions.shape[0]
    capacity = max(2, 3 * block_count // col_count)
    total_slots = col_count * capacity
    owner_col = owner_column[:, 0]
    order_ids = jnp.arange(block_count, dtype=jnp.int32)
    earlier_same = (owner_col[None, :] == owner_col[:, None]) & (
        order_ids[None, :] < order_ids[:, None]
    )
    slot_index = owner_col * capacity + jnp.sum(earlier_same.astype(jnp.int32), axis=1)
    stored = to_bricks(velocity)
    brick_count = stored.shape[0]

    def place(values, fill):
        buffer = jnp.full((total_slots,) + values.shape[1:], fill, values.dtype)
        return buffer.at[slot_index].set(values).reshape((col_count, capacity) + values.shape[1:])

    weights_f = weights.astype(jnp.float32)
    forces = chain_force(
        positions.astype(jnp.float32), stiffness.astype(jnp.float32), rest_sq.astype(jnp.float32)
    )
    pushed = spread(forces, weights_f)
    send_force = place(pushed, 0.0)
    send_index = place(brick_index.astype(jnp.float32), 0.0)
    wanted = lax.all_to_all(send_index, "col", split_axis=0, concat_axis=0, tiled=True)
    pushes = lax.all_to_all(send_force, "col", split_axis=0, concat_axis=0, tiled=True)
    wanted_ids = wanted.astype(jnp.int32)
    reply = stored[wanted_ids]
    returned = lax.all_to_all(reply, "col", split_axis=0, concat_axis=0, tiled=True)
    returned, arrived_ids, arrived = (returned, wanted_ids, pushes)
    fetched = returned.reshape(total_slots, -1)[slot_index]
    marker_velocity = interpolate(fetched, weights_f)
    forcing = jax.ops.segment_sum(
        arrived.reshape(total_slots, -1), arrived_ids.reshape(-1), num_segments=brick_count
    )
    force_field = from_bricks(forcing, size_x, size_y, size_z)
    padded = with_halo(velocity, (("row", 1), ("col", 2)), 1)
    grad_x = (padded[:, 2:, 1:-1] - padded[:, :-2, 1:-1]) * 0.5
    grad_y = (padded[:, 1:-1, 2:] - padded[:, 1:-1, :-2]) * 0.5
    grad_z = (jnp.roll(velocity, -1, axis=3) - jnp.roll(velocity, 1, axis=3)) * 0.5
    transport = velocity[0] * grad_x + velocity[1] * grad_y + velocity[2] * grad_z
    star = velocity + DT_STEP * (force_field - transport)
    cos_z, sin_z = tables(size_z)
    half_z = size_z // 2
    col_here = lax.axis_index("col")
    cos_fore = cos_z[:, :half_z]
    sin_fore = sin_z[:, :half_z].at[:, 0].set(-cos_z[:, half_z])
    z_real = jnp.einsum("cxyz,zk->cxyk", star, cos_fore, precision=PRECISE)
    z_imag = -jnp.einsum("cxyz,zk->cxyk", star, sin_fore, precision=PRECISE)
    shuffled = col_transpose(jnp.stack([z_real, z_imag]))
    slab = shuffled.shape[4]
    first_slot = (col_here == 0) & (jnp.arange(slab, dtype=jnp.int32) == 0)
    highest = shuffled[1][..., 0:1] * (col_here == 0).astype(jnp.float32)
    lower_imag = jnp.where(first_slot, 0.0, shuffled[1])
    y_in_real = jnp.concatenate([shuffled[0], highest], axis=3)
    y_in_imag = jnp.concatenate([lower_imag, jnp.zeros_like(highest)], axis=3)
    z_index = jnp.concatenate(
        [col_here * slab + jnp.arange(slab, dtype=jnp.int32), jnp.full((1,), half_z, jnp.int32)]
    )
    y_real, y_imag = forward("cxyz,yk->cxzk", y_in_real, y_in_imag, y_in_real.shape[2])
    shuffled = row_transpose(jnp.stack([y_real, y_imag]))
    x_real, x_imag = forward("cxzy,xk->czyk", shuffled[0], shuffled[1], shuffled.shape[2])
    slab_y = x_real.shape[2]
    full_x = x_real.shape[3]
    full_y = slab_y * row_count
    y_index = lax.axis_index("row") * slab_y + jnp.arange(slab_y, dtype=jnp.int32)
    x_index = jnp.arange(full_x, dtype=jnp.int32)
    dir_z, sig_z, zero_z = wave_parts(z_index, size_z)
    dir_y, sig_y, zero_y = wave_parts(y_index, full_y)
    dir_x, sig_x, zero_x = wave_parts(x_index, full_x)
    wave_z = dir_z[:, None, None]
    wave_y = dir_y[None, :, None]
    wave_x = dir_x[None, None, :]
    no_direction = zero_z[:, None, None] & zero_y[None, :, None] & zero_x[None, None, :]
    wave_sq = wave_x * wave_x + wave_y * wave_y + wave_z * wave_z
    full_sq = sig_z[:, None, None] ** 2 + sig_y[None, :, None] ** 2 + sig_x[None, None, :] ** 2
    inverse_sq = jnp.where(no_direction, 0.0, 1.0 / jnp.where(no_direction, 1.0, wave_sq))
    damping = 1.0 / (1.0 + DT_STEP * VISCOSITY * full_sq)
    waves = jnp.stack(
        [
            jnp.broadcast_to(wave_x, wave_sq.shape),
            jnp.broadcast_to(wave_y, wave_sq.shape),
            jnp.broadcast_to(wave_z, wave_sq.shape),
        ]
    )
    normal_real = jnp.sum(waves * x_real, axis=0) * inverse_sq
    normal_imag = jnp.sum(waves * x_imag, axis=0) * inverse_sq
    p_real = (x_real - waves * normal_real) * damping
    p_imag = (x_imag - waves * normal_imag) * damping
    b_real, b_imag = backward("czyk,kx->cyzx", p_real, p_imag, full_x)
    shuffled = row_transpose(jnp.stack([b_real, b_imag]))
    b_real, b_imag = backward("cyzx,yk->cxzk", shuffled[0], shuffled[1], shuffled.shape[2])
    slab = b_real.shape[2] - 1
    first_slot = (col_here == 0) & (jnp.arange(slab, dtype=jnp.int32) == 0)
    highest = b_real[:, :, slab:, :]
    packed_imag = jnp.where(first_slot[None, None, :, None], highest, b_imag[:, :, :slab, :])
    shuffled = col_transpose(jnp.stack([b_real[:, :, :slab, :], packed_imag]))
    doubling = jnp.where(jnp.arange(half_z, dtype=jnp.int32) == 0, 1.0, 2.0)[:, None]
    cos_back = cos_z[:half_z] * doubling
    sin_back = (sin_z[:half_z] * doubling).at[0].set(-cos_z[half_z])
    new_velocity = (
        jnp.einsum("cxky,kz->cxyz", shuffled[0], cos_back, precision=PRECISE)
        - jnp.einsum("cxky,kz->cxyz", shuffled[1], sin_back, precision=PRECISE)
    ) / size_z
    return (new_velocity, marker_velocity)


VMEM = pltpu.VMEM
MESH = pl.DeviceIdType.MESH
F32 = jnp.float32
BF16 = jnp.bfloat16
I32 = jnp.int32
TOP = 32700.0
NT = ((1,), (1,))


def two_parts(table):
    table = np.asarray(table, np.float64)
    high = table.astype(jnp.bfloat16)
    low = (table - high.astype(np.float64)).astype(jnp.bfloat16)
    return np.stack([high, low])


def angle_of(length, left, right):
    return 2.0 * np.pi / length * (np.outer(left, right) % length)


def build_tables(size_x, size_y, size_z, rows):
    half_z = size_z // 2
    turn = angle_of(size_z, np.arange(size_z), np.arange(half_z))
    fore = np.concatenate([np.cos(turn), -np.sin(turn)], axis=1)
    back = np.concatenate([2.0 * np.cos(turn), -2.0 * np.sin(turn)], axis=1)
    alternate = np.where(np.arange(size_z) % 2 == 0, 1.0, -1.0)
    fore[:, half_z] = alternate
    back[:, 0], back[:, half_z] = 1.0, alternate
    back = back.T / (size_x * size_y * size_z)
    turn_y = angle_of(size_y, np.arange(size_y), np.arange(size_y))
    line = np.concatenate([np.cos(turn_y), np.sin(turn_y)], axis=0)
    lane = np.arange(size_x)
    place = (lane % rows) * (size_x // rows) + lane // rows
    turn_x = angle_of(size_x, place, np.arange(size_x))
    cosine, sine = np.cos(turn_x), np.sin(turn_x)
    wide = np.concatenate(
        [np.concatenate([cosine, -sine], axis=1), np.concatenate([sine, cosine], axis=1)], axis=0
    )
    return tuple(two_parts(t) for t in (fore, back, line, wide, wide.T))


def parts(values):
    high = values.astype(BF16)
    return high, (values - high.astype(F32)).astype(BF16)


def mul(left, right, dims=((1,), (0,))):
    return lax.dot_general(left, right, (dims, ((), ())), preferred_element_type=F32)


def mul3(left, right, dims=((1,), (0,))):
    return (
        mul(left[0], right[0], dims) + mul(left[1], right[0], dims) + mul(left[0], right[1], dims)
    )


def roll(values, shift):
    return pltpu.roll(values, shift % 128, values.ndim - 1)


def lanes_of(shape):
    return lax.broadcasted_iota(I32, shape, len(shape) - 1)


def code_of(peak):
    return jnp.floor(jnp.log2(jnp.maximum(peak, 1e-30)) * 65536.0).astype(I32) + 2


def unit_of(code):
    return jnp.exp2(code.astype(F32) * (1.0 / 65536.0)) * (1.0 / TOP)


def whole(values):
    return jnp.round(values).astype(I32)


def join(first, second):
    return (first << 16) + second


def split(word):
    second = (word << 16) >> 16
    return (word - second) >> 16, second


def swap_bits(tiles, steps):
    tiles = list(tiles)
    keep = {s: (lanes_of(tiles[0].shape) & s) == 0 for s in steps}
    for bit, step in enumerate(steps):
        for one in range(len(tiles)):
            if one >> bit & 1:
                continue
            two = one | 1 << bit
            a, b = tiles[one], tiles[two]
            tiles[one] = jnp.where(keep[step], a, roll(b, step))
            tiles[two] = jnp.where(keep[step], roll(a, -step), b)
    return tiles


def compress(tiles, lane):
    out = []
    for t in range(9):
        out.append(jnp.where(lane < 96, tiles[t], roll(tiles[9 + t // 3], 96 - 32 * (t % 3))))
    return out


def expand(tiles, lane):
    out = list(tiles)
    for u in range(3):
        a, b, c = (roll(tiles[3 * u + p], 32 + 32 * p) for p in range(3))
        out.append(jnp.where(lane < 32, a, jnp.where(lane < 64, b, c)))
    return out


def pack_cubes(wide, lane):
    tiles = [wide[t * 8 : t * 8 + 8].astype(I32) for t in range(24)]
    words = []
    for c in range(3):
        for i in range(4):
            words.append(join(tiles[c * 8 + i], tiles[c * 8 + i + 4]))
    return compress(words, lane)


def open_cubes(tiles, lane):
    out = [None] * 24
    for t, word in enumerate(expand(tiles, lane)):
        at = t // 4 * 8 + t % 4
        out[at], out[at + 4] = split(word)
    return jnp.concatenate([t.astype(F32) for t in out], axis=0)


def pad(tile):
    return jnp.concatenate([tile, jnp.zeros((3, 128), I32)], axis=0)


def fold(tile, low, near):
    other = pltpu.roll(roll(tile, 64), 4, 0)
    return jnp.where(jnp.logical_or(low, jnp.logical_not(near)), tile, other)


def unfold(tile, near):
    return jnp.where(near, tile, pltpu.roll(roll(tile, 64), 4, 0))


def peak_of(values):
    while values.ndim > 2:
        values = jnp.max(values, axis=0)
    return jnp.max(jnp.max(values, axis=0, keepdims=True), axis=1, keepdims=True)


def column(row):
    shape = (row.shape[1], row.shape[1])
    diagonal = lax.broadcasted_iota(I32, shape, 0) == lax.broadcasted_iota(I32, shape, 1)
    return jnp.sum(jnp.where(diagonal, row, 0.0), axis=1, keepdims=True)


def mix(step, cols):
    ring, pair = step // cols, step % cols
    return ((6, 2, 4, 7, 3, 5, 1, 0).index(pair % 8), (2, 1, 3, 0).index(ring % 4), step)


def main_kernel(
    rows, columns, capacity,
    owner_hbm, brick_hbm, stiff_hbm, rest_hbm, pos_hbm, weight_hbm, velocity_hbm,
    fore_hbm, line_hbm, wide_hbm, unwide_hbm, back_hbm,
    last_ref, mark_ref, back_ref,
    owner_ref, brick_ref, stiff_ref, rest_ref, pos_ref, weight_ref, velocity_ref,
    fore_ref, line_ref, wide_ref, unwide_ref, noted,
    force, deep, cube, place, face_x, face_y, near_x, near_y, push, pushed, star, select,
    held, modes, arrived, reply, replied, ready,
    load_sems, face_sems, push_sems, mode_sems, reply_sems, last_sems,
):
    sources = (
        owner_hbm, brick_hbm, stiff_hbm, rest_hbm, pos_hbm, weight_hbm, velocity_hbm,
        fore_hbm, line_hbm, wide_hbm, unwide_hbm, back_hbm,
    )
    targets = (
        owner_ref, brick_ref, stiff_ref, rest_ref, pos_ref, weight_ref, velocity_ref,
        fore_ref, line_ref, wide_ref, unwide_ref, back_ref,
    )
    loads = []
    for number, (source, target) in enumerate(zip(sources, targets)):
        loads.append(pltpu.make_async_copy(source, target, load_sems.at[number]))
        loads[-1].start()
    row, col = lax.axis_index("row"), lax.axis_index("col")
    devices = rows * columns
    blocks = pos_ref.shape[1]
    size_x, size_y, size_z = velocity_ref.shape[1:]
    bricks_x = size_x // 8
    barrier = pltpu.get_barrier_semaphore()

    def flip(step):
        at, bit = 0, 1
        while bit < columns:
            own = lax.rem(col // bit, 2)
            at = at + bit * (1 - own if step & bit else own)
            bit *= 2
        return at

    def peer(step):
        to_row, to_col = lax.rem(row + step // columns, rows), flip(step % columns)
        return (to_row, to_col), to_row * columns + to_col

    greet = list(range(1, columns)) + list(range(columns, devices, columns))
    for step in greet:
        pl.semaphore_signal(barrier, inc=1, device_id=peer(step)[0], device_id_type=MESH)

    def remote(source, target, sems, step, device):
        return pltpu.make_async_remote_copy(
            source, target, sems.at[0, step], sems.at[1, step],
            device_id=device, device_id_type=MESH,
        )

    def send_all(source, target, sems, around):
        waits = []
        count = devices if around else columns
        me = row * columns + col if around else col
        for step in sorted(range(1, count), key=lambda n: mix(n, columns)):
            device, at = peer(step)
            at = at if around else device[1]
            copy = remote(source.at[at], target.at[me], sems, step, device)
            copy.start()
            opposite = (rows - step // columns) % rows * columns + step % columns
            origin_device, origin = peer(opposite)
            origin = origin if around else origin_device[1]
            arrival = remote(source.at[at], target.at[origin], sems, step, device)
            waits.append((copy, arrival))
        own = pltpu.make_async_copy(source.at[me], target.at[me], sems.at[0, 0])
        own.start()
        return waits, own

    def receive(sent):
        for _, arrival in sent[0]:
            arrival.wait_recv()
        sent[1].wait()

    def finish(sent):
        for copy, _ in sent[0]:
            copy.wait_send()

    lane8 = lanes_of((8, 128))
    near = lax.broadcasted_iota(I32, (8, 128), 0) < 4

    for load in loads[:4]:
        load.wait()
    owner_row = owner_ref[...].astype(F32)
    owner = column(owner_row)
    shape = (blocks, blocks)
    earlier = lax.broadcasted_iota(I32, shape, 1) < lax.broadcasted_iota(I32, shape, 0)
    rank = jnp.sum(
        jnp.where((owner == owner_row) & earlier, 1.0, 0.0), axis=1, keepdims=True
    )
    slot = jnp.broadcast_to(owner * 128.0 + rank * 8.0, (blocks, 128))
    brick = jnp.broadcast_to(column(brick_ref[...].astype(F32)) + 1.0, (blocks, 128))
    deep_shape = (blocks, 8, 128)
    inner = lax.broadcasted_iota(I32, deep_shape, 1).astype(F32)
    slot = (slot[:, None, :] + inner).reshape(blocks * 8, 128)
    brick = jnp.broadcast_to(brick[:, None, :], deep_shape).reshape(blocks * 8, 128)
    lane_f = lanes_of((blocks * 8, 128)).astype(F32)
    for at in range(columns):
        hit = slot == lane_f + 128.0 * at
        place[:, at * 128 : (at + 1) * 128] = jnp.where(hit, 1.0, 0.0).astype(BF16)
        named = jnp.sum(jnp.where(hit, brick, 0.0), axis=0, keepdims=True).astype(I32)
        noted[at] = jnp.broadcast_to(named, (8, 128))

    for load in loads[4:6]:
        load.wait()
    stiff = column(stiff_ref[...].astype(F32))
    rest = column(rest_ref[...].astype(F32))
    points = [pos_ref[c].astype(F32) for c in range(3)]
    segment = [pltpu.roll(p, 127, 1) - p for p in points]
    stretch = sum(part * part for part in segment) / rest
    pull = 0.5 * stiff * (stretch - 1.0)
    for c in range(3):
        tension = pull * segment[c]
        force[c] = tension - pltpu.roll(tension, 1, 1)

    def spread(index, carry):
        first = weight_ref[index, 0].astype(F32)
        second = weight_ref[index, 1].astype(F32)
        third = weight_ref[index, 2].astype(F32)
        high, low = parts((first[:, None, :] * third[None]).reshape(64, 128))
        both = jnp.concatenate([high, low], axis=0)
        deep[index] = both
        pushes = jnp.concatenate([force[c, pl.ds(index, 1), :] * second for c in range(3)], axis=0)
        upper = pushes.astype(BF16).astype(F32)
        left = jnp.concatenate([upper, pushes - upper], axis=0).astype(BF16)
        result = mul(left, both, NT)
        total = result[0:24] + result[24:48]
        total = total + pltpu.roll(total, 64, 1)
        cube[index] = total.reshape(3, 8, 128)
        return carry

    lax.fori_loop(0, blocks, spread, 0, unroll=16)

    low_half = lane8 < 64
    outs = [[None] * 2 for _ in range(24)]
    for c in range(3):
        for g in range(2):
            tiles = [
                jnp.where(low_half, cube[g * 16 + b, c], cube[g * 16 + 8 + b, c]) for b in range(8)
            ]
            for i, tile in enumerate(swap_bits(tiles, (8, 16, 32))):
                outs[c * 8 + i][g] = tile
    spreads = jnp.concatenate([jnp.concatenate(pair, axis=1) for pair in outs], axis=0)
    push_code = code_of(peak_of(jnp.abs(spreads)))
    high, low = parts(jnp.round(spreads * (1.0 / unit_of(push_code))))

    for load in loads[6:-1]:
        load.wait()
    value_code = code_of(peak_of(jnp.abs(velocity_ref[...].reshape(-1, 8, size_z))))
    scale = 1.0 / unit_of(value_code)
    half = size_x // 2
    for side, at in ((0, size_x - 1), (1, 0)):
        cells = whole(velocity_ref[:, at] * scale[None])
        face_x[side, 0:24] = join(cells[:, :, 0:128], cells[:, :, 128:256]).reshape(24, 128)
        face_x[side, 24:25] = jnp.broadcast_to(value_code, (1, 128))
    for side, at in ((0, size_y - 1), (1, 0)):
        cells = whole(velocity_ref[:, :, at, :] * scale[None])
        face_y[side, 0:24] = join(cells[:, 0:half], cells[:, half:]).reshape(24, size_z)
        face_y[side, 24:25] = jnp.broadcast_to(value_code, (1, size_z))

    pl.semaphore_wait(barrier, len(greet))
    faces = []
    for source, target, base, axis in ((face_x, near_x, 0, 0), (face_y, near_y, 2, 1)):
        for side in range(2):
            extent = (rows, columns)[axis]
            step = 1 if side == 0 else extent - 1
            if axis == 0:
                device = (lax.rem(row + step, rows), col)
            else:
                device = (row, lax.rem(col + step, columns))
            copy = remote(source.at[side], target.at[side], face_sems, base + side, device)
            copy.start()
            faces.append(copy)

    near_order = sorted(range(1, columns), key=lambda n: mix(n, columns))
    pushes, waiting = [], None
    for step in near_order + [0]:
        device, _ = peer(step)
        at = device[1]
        window = place[:, pl.ds(pl.multiple_of(at * 128, 128), 128)]
        tiles = pack_cubes(mul(high, window) + mul(low, window), lane8)
        target = push if step else pushed
        for t in range(9):
            target[at, t * 8 : t * 8 + 8] = tiles[t]
        target[at, 72:73] = jnp.where(lane8[0:1] < 96, noted[at, 0:1], push_code)
        if waiting is not None:
            waiting.start()
        if step:
            waiting = remote(push.at[at], pushed.at[col], push_sems, step, device)
            arrival = remote(push.at[at], pushed.at[at], push_sems, step, device)
            pushes.append((waiting, arrival))

    for copy in faces:
        copy.wait()
    value = velocity_ref[...]
    sides_x, sides_y = [], []
    for side in range(2):
        unit = unit_of(near_x[side, 24:25])[:, 0:1]
        one, two = split(near_x[side, 0:24])
        wide = jnp.concatenate([one.astype(F32), two.astype(F32)], axis=1) * unit
        sides_x.append(wide.reshape(3, 1, size_y, size_z))
        unit = unit_of(near_y[side, 24:25])[:, 0:1]
        one, two = (part.astype(F32) * unit for part in split(near_y[side, 0:24]))
        wide = [part.reshape(3, half, size_z) for part in (one, two)]
        sides_y.append(jnp.concatenate(wide, axis=1).reshape(3 * size_x, 1, size_z))
    ahead = jnp.concatenate([value[:, 1:], sides_x[1]], axis=1)
    behind = jnp.concatenate([sides_x[0], value[:, :-1]], axis=1)
    transport = value[0:1] * ((ahead - behind) * 0.5)
    flat = value.reshape(3 * size_x, size_y, size_z)
    sub = lax.broadcasted_iota(I32, flat.shape, 1)
    face_low, face_high = sides_y
    ahead = jnp.where(sub == size_y - 1, face_high, pltpu.roll(flat, size_y - 1, 1))
    behind = jnp.where(sub == 0, face_low, pltpu.roll(flat, 1, 1))
    transport += value[1:2] * ((ahead - behind) * 0.5).reshape(value.shape)
    ahead = pltpu.roll(flat, size_z - 1, 2)
    behind = pltpu.roll(flat, 1, 2)
    transport += value[2:3] * ((ahead - behind) * 0.5).reshape(value.shape)
    star[...] = value - DT_STEP * transport

    spot = lax.broadcasted_iota(I32, (bricks_x * size_z, 128), 0)
    inner = lanes_of((1, 128)) & 7
    origins = [0] + near_order
    for k, step in enumerate(origins):
        if step:
            pushes[k - 1][1].wait_recv()
        at = peer(step)[0][1]
        tiles = [pushed[at, t * 8 : t * 8 + 8] for t in range(9)]
        meta = pushed[at, 72:73]
        unit = unit_of(meta)[:, 127:128]
        wide = open_cubes(tiles, lane8).reshape(24, 8, 128) * unit[None]
        high, low = parts(wide.reshape(192, 128))
        held[0, :, k * 128 : (k + 1) * 128] = high
        held[1, :, k * 128 : (k + 1) * 128] = low
        mark = jnp.where((lanes_of((1, 128)) < 96) & (meta > 0), (meta - 1) * 8 + inner, -1)
        select[:, k * 128 : (k + 1) * 128] = jnp.where(spot == mark, 1.0, 0.0).astype(BF16)
    for brick_x in range(bricks_x):
        chosen = select[brick_x * size_z : (brick_x + 1) * size_z]
        field = mul(held[0], chosen, NT) + mul(held[1], chosen, NT)
        star[:, brick_x * 8 : (brick_x + 1) * 8] += DT_STEP * field.reshape(3, 8, 8, size_z)

    spectrum = mul3(parts(star[...].reshape(-1, size_z)), (fore_ref[0], fore_ref[1]))
    real = spectrum[:, 0:128].reshape(3 * size_x, 8, 128)
    imag = spectrum[:, 128:256].reshape(3 * size_x, 8, 128)
    peak = jnp.maximum(jnp.max(jnp.abs(real), axis=0), jnp.max(jnp.abs(imag), axis=0))
    mode_code = jnp.broadcast_to(code_of(jnp.max(peak, axis=0, keepdims=True)), (8, 128))
    scale = (1.0 / unit_of(mode_code))[None]
    words = join(whole(real * scale), whole(imag * scale))
    steps = (4, 8, 16, 32, 64)
    tiles = swap_bits([words[t] for t in range(32)], steps)
    for t in range(devices):
        modes[t, 0:8] = tiles[t]
    tiles = swap_bits([words[32 + t] for t in range(16)] + [mode_code] * 16, steps)
    for t in range(devices):
        modes[t, 8:13] = fold(tiles[t], low_half, near)[0:5]
    moved = send_all(modes, arrived, mode_sems, True)

    scale = 1.0 / unit_of(value_code)
    cells = []
    for brick_x in range(bricks_x):
        piece = velocity_ref[:, brick_x * 8 : (brick_x + 1) * 8].reshape(192, size_z)
        cells.append(parts(jnp.round(piece * scale)))
    for k, step in enumerate(origins):
        at = peer(step)[0][1]
        wide = None
        for brick_x in range(bricks_x):
            chosen = select[
                brick_x * size_z : (brick_x + 1) * size_z, k * 128 : (k + 1) * 128
            ]
            piece = mul(cells[brick_x][0], chosen) + mul(cells[brick_x][1], chosen)
            wide = piece if wide is None else wide + piece
        tiles = pack_cubes(wide, lane8)
        for t in range(9):
            reply[at, t * 8 : t * 8 + 8] = tiles[t]
        reply[at, 72:73] = jnp.broadcast_to(value_code, (1, 128))

    receive(moved)
    replies = send_all(reply, replied, reply_sems, False)
    here = row * columns + col
    first = here == 0
    upper = jnp.logical_not(low_half)
    lines = [[[] for _ in range(3)] for _ in range(4)]
    for at in range(columns):
        zero = swap_bits([arrived[r * columns + at, 0:8] for r in range(rows)], (1, 2))
        rest_tiles = swap_bits([pad(arrived[r * columns + at, 8:13]) for r in range(rows)], (1, 2))
        for mode in range(4):
            code = jnp.broadcast_to(rest_tiles[mode][4:5], (8, 128))
            unit = unit_of(jnp.where(low_half, roll(code, 64), code))
            real0, imag0 = (p.astype(F32) * unit for p in split(zero[mode]))
            real1, imag1 = (p.astype(F32) * unit for p in split(unfold(rest_tiles[mode], near)))
            lines[mode][0].append(jnp.where(low_half, real0, roll(imag0, 64)))
            lines[mode][1].append(jnp.where(low_half, roll(real0, 64), imag0))
            lines[mode][2].append(jnp.where(low_half, real1, roll(imag1, 64)))
    lines = [[jnp.concatenate(lines[mode][c], axis=0) for c in range(3)] for mode in range(4)]
    wide_y = columns * 8
    low_line = lanes_of((wide_y, 128)) < 64
    lines.append([jnp.where(low_line, roll(v, 64), 0.0) for v in lines[0]])
    lines[0] = [jnp.where(jnp.logical_and(first, jnp.logical_not(low_line)), 0.0, v) for v in lines[0]]
    line_table = (line_ref[0], line_ref[1])
    sign = jnp.where(low_line, 1.0, -1.0)
    lined = []
    for slot_at in range(5):
        both = mul3(line_table, parts(jnp.concatenate(lines[slot_at], axis=1)))
        for c in range(3):
            a = both[0:wide_y, c * 128 : (c + 1) * 128]
            b = both[wide_y:, c * 128 : (c + 1) * 128]
            lined.append(a + sign * roll(b, 64))
    full_x = rows * size_x
    index = lanes_of((wide_y, 128)) & (full_x - 1)
    line = lax.broadcasted_iota(I32, (wide_y, 128), 0)
    scale_x, scale_y, scale_z = (2.0 * np.pi / n for n in (full_x, wide_y, size_z))
    sig_x = jnp.where(index < full_x // 2, index, index - full_x).astype(F32) * scale_x
    sig_y = jnp.where(line < wide_y // 2, line, line - wide_y).astype(F32) * scale_y
    wave_x = jnp.where(index == full_x // 2, 0.0, sig_x)
    wave_y = jnp.where(line == wide_y // 2, 0.0, sig_y)
    backs = []
    for slot_at in range(5):
        spot_lines = jnp.concatenate(lined[slot_at * 3 : slot_at * 3 + 3], axis=0)
        values = mul3(parts(spot_lines), (wide_ref[0], wide_ref[1]))
        x, y, z = (values[c * wide_y : (c + 1) * wide_y] for c in range(3))
        if slot_at < 4:
            sig_z = (here * 4 + slot_at).astype(F32) * scale_z
            wave_z = sig_z
        else:
            sig_z, wave_z = F32(np.pi), F32(0.0)
        square = wave_x * wave_x + wave_y * wave_y + wave_z * wave_z
        full = sig_x * sig_x + sig_y * sig_y + sig_z * sig_z
        none = square == 0.0
        inverse_sq = jnp.where(none, 0.0, 1.0 / jnp.where(none, 1.0, square))
        damping = 1.0 / (1.0 + DT_STEP * VISCOSITY * full)
        normal = (wave_x * x + wave_y * y + wave_z * z) * inverse_sq
        result = jnp.concatenate(
            [
                (x - wave_x * normal) * damping,
                (y - wave_y * normal) * damping,
                (z - wave_z * normal) * damping,
            ],
            axis=0,
        )
        turned = mul3(parts(result), (unwide_ref[0], unwide_ref[1]))
        stacked = jnp.concatenate(
            [turned[c * wide_y : (c + 1) * wide_y] for c in range(3)], axis=1
        )
        both = mul3(line_table, parts(stacked))
        back = []
        for c in range(3):
            a = both[0:wide_y, c * 128 : (c + 1) * 128]
            b = both[wide_y:, c * 128 : (c + 1) * 128]
            back.append(a - sign * roll(b, 64))
        backs.append(back)
    top = jnp.logical_and(first, jnp.logical_not(low_line))
    backs[0] = [jnp.where(top, roll(backs[4][c], 64), backs[0][c]) for c in range(3)]
    zero_words, rest_words = [], []
    for mode in range(4):
        e = backs[mode]
        peak = jnp.maximum(jnp.maximum(jnp.abs(e[0]), jnp.abs(e[1])), jnp.abs(e[2]))
        code = code_of(peak_of(peak))
        scale = 1.0 / unit_of(code)
        e = [v * scale for v in e]
        real0 = whole(jnp.where(low_line, e[0], roll(e[1], 64)))
        imag0 = whole(jnp.where(low_line, roll(e[0], 64), e[1]))
        zero_words.append(join(real0, imag0))
        rest_words.append(jnp.where(low_line, join(whole(e[2]), whole(roll(e[2], 64))), code))
    for at in range(columns):
        span = slice(at * 8, at * 8 + 8)
        tiles = swap_bits([w[span] for w in zero_words], (1, 2))
        for r in range(rows):
            ready[r * columns + at, 0:8] = tiles[r]
        tiles = swap_bits([w[span] for w in rest_words], (1, 2))
        for r in range(rows):
            ready[r * columns + at, 8:13] = fold(tiles[r], low_half, near)[0:5]
    lasts = send_all(ready, last_ref, last_sems, True)

    receive(replies)
    for at in range(columns):
        tiles = [replied[at, t * 8 : t * 8 + 8] for t in range(9)]
        unit = unit_of(replied[at, 72:73])
        wide = open_cubes(tiles, lane8).reshape(24, 8, 128) * unit[None]
        high, low = parts(wide.reshape(192, 128))
        held[0, :, at * 128 : (at + 1) * 128] = high
        held[1, :, at * 128 : (at + 1) * 128] = low
    fetched = mul(held[0], place[...], NT) + mul(held[1], place[...], NT)
    for c in range(3):
        for g in range(2):
            tiles = [
                fetched[c * 64 + i * 8 : c * 64 + i * 8 + 8, g * 128 : (g + 1) * 128]
                for i in range(8)
            ]
            for b, tile in enumerate(swap_bits(tiles, (8, 16, 32))):
                cube[g * 8 + b, c] = tile

    low_rows = lanes_of((24, 128)) < 64

    def interpolate_pair(index, carry):
        block = index // 8 * 16 + lax.rem(index, 8)
        cells = cube[index].reshape(24, 128)
        apart = jnp.concatenate(
            [jnp.where(low_rows, cells, 0.0), jnp.where(low_rows, 0.0, cells)], axis=0
        )
        high, low = parts(apart)
        one, two = deep[block], deep[block + 8]
        upper = jnp.concatenate([one[0:64], two[0:64]], axis=0)
        lower = jnp.concatenate([one[64:128], two[64:128]], axis=0)
        summed = mul(high, upper) + mul(low, upper) + mul(high, lower)
        for half, at in ((0, block), (1, block + 8)):
            second = weight_ref[at, 1].astype(F32)
            piece = summed[half * 24 : half * 24 + 24].reshape(3, 8, 128) * second[None]
            piece = jnp.sum(piece, axis=1)
            for c in range(3):
                mark_ref[c, pl.ds(at, 1), :] = piece[c : c + 1]
        return carry

    lax.fori_loop(0, blocks // 2, interpolate_pair, 0, unroll=4)
    loads[-1].wait()
    receive(lasts)
    for copy, _ in pushes:
        copy.wait_send()
    for sent in (moved, replies, lasts):
        finish(sent)


def final_kernel(last_ref, back_ref, mark_ref, new_ref, out_ref):
    devices = last_ref.shape[0]
    steps = (4, 8, 16, 32, 64)
    words = swap_bits([last_ref[t, 0:8] for t in range(devices)], steps)
    low = lanes_of((8, 128)) < 64
    near = lax.broadcasted_iota(I32, (8, 128), 0) < 4
    rest = []
    for t in range(devices):
        tile = pad(last_ref[t, 8:13])
        code = jnp.broadcast_to(tile[4:5], (8, 128))
        rest.append(jnp.where(low, unfold(tile, near), code))
    rest = swap_bits(rest, steps)
    unit = unit_of(rest[16])
    words += rest[0:16]
    rows = []
    for word in words:
        real, imag = split(word)
        rows.append(jnp.concatenate([real.astype(F32) * unit, imag.astype(F32) * unit], axis=1))
    result = mul3(parts(jnp.concatenate(rows, axis=0)), (back_ref[0], back_ref[1]))
    new_ref[...] = result.reshape(new_ref.shape)
    out_ref[...] = mark_ref[...]


def local(velocity, positions, weights, stiffness, rest_sq, owner_column, brick_index):
    rows = lax.axis_size("row")
    columns = lax.axis_size("col")
    devices = rows * columns
    _, local_x, local_y, size_z = velocity.shape
    blocks = positions.shape[0]
    capacity = max(2, 3 * blocks // columns)
    fits = (
        local_x == 16 and local_y == 8 and size_z == 8 * devices and positions.shape[2] == 128
        and capacity == 12 and blocks == 32 and columns == 8 and rows == 4
    )
    if not fits:
        return general(
            velocity, positions, weights, stiffness, rest_sq, owner_column, brick_index
        )
    return fast(velocity, positions, weights, stiffness, rest_sq, owner_column, brick_index)


def fast(velocity, positions, weights, stiffness, rest_sq, owner_column, brick_index):
    rows = lax.axis_size("row")
    columns = lax.axis_size("col")
    devices = rows * columns
    _, local_x, local_y, size_z = velocity.shape
    blocks = positions.shape[0]
    capacity = max(2, 3 * blocks // columns)
    size_x, size_y = rows * local_x, columns * local_y
    fore, back, line, wide, unwide = build_tables(size_x, size_y, size_z, rows)
    vm = pl.BlockSpec(memory_space=VMEM)
    shape = jax.ShapeDtypeStruct
    cells = local_x // BRICK * size_z
    dma = pltpu.SemaphoreType.DMA
    operands = (
        owner_column.reshape(1, blocks), brick_index.reshape(1, blocks),
        stiffness.reshape(1, blocks), rest_sq.reshape(1, blocks),
        positions.transpose(1, 0, 2), weights, velocity, fore, line, wide, unwide,
    )
    last, marks, back = pl.pallas_call(
        partial(main_kernel, rows, columns, capacity),
        out_shape=[
            VMEM((devices, 13, 128), I32), VMEM((3, blocks, 128), F32), VMEM(back.shape, BF16),
        ],
        in_specs=[pl.BlockSpec(memory_space=pl.ANY)] * 12,
        out_specs=[vm, vm, vm],
        scratch_shapes=[VMEM(a.shape, a.dtype) for a in operands] + [
            VMEM((columns, 8, 128), I32),
            VMEM((3, blocks, 128), F32),
            VMEM((blocks, 128, 128), BF16),
            VMEM((blocks, 3, 8, 128), F32),
            VMEM((blocks * 8, columns * 128), BF16),
            VMEM((2, 25, 128), I32),
            VMEM((2, 25, size_z), I32),
            VMEM((2, 25, 128), I32),
            VMEM((2, 25, size_z), I32),
            VMEM((columns, 73, 128), I32),
            VMEM((columns, 73, 128), I32),
            VMEM((3, local_x, local_y, size_z), F32),
            VMEM((cells, columns * 128), BF16),
            VMEM((2, 192, columns * 128), BF16),
            VMEM((devices, 13, 128), I32),
            VMEM((devices, 13, 128), I32),
            VMEM((columns, 73, 128), I32),
            VMEM((columns, 73, 128), I32),
            VMEM((devices, 13, 128), I32),
            dma((12,)),
            dma((2, 4)),
            dma((2, columns)),
            dma((2, devices)),
            dma((2, columns)),
            dma((2, devices)),
        ],
        compiler_params=pltpu.CompilerParams(collective_id=1, has_side_effects=True),
        name="step",
    )(*operands, back)
    new_velocity, marks = pl.pallas_call(
        final_kernel,
        out_shape=[shape(velocity.shape, F32), shape((3, blocks, 128), F32)],
        in_specs=[vm, vm, vm],
        out_specs=[vm, vm],
        name="final",
    )(
        pltpu.with_memory_space_constraint(last, VMEM),
        pltpu.with_memory_space_constraint(back, VMEM),
        pltpu.with_memory_space_constraint(marks, VMEM),
    )
    return new_velocity, marks.transpose(1, 0, 2)


def solution(mesh):
    return jax.shard_map(
        local,
        mesh=mesh,
        in_specs=(
            P(None, "row", "col", None),
            P(("row", "col"), None, None),
            P(("row", "col"), None, None, None),
            P(("row", "col")),
            P(("row", "col")),
            P(("row", "col"), None),
            P(("row", "col")),
        ),
        out_specs=(P(None, "row", "col", None), P(("row", "col"), None, None)),
        check_vma=False,
    )
```

```python
from functools import partial

import numpy as np

import jax
import jax.numpy as jnp
from jax import lax
from jax.experimental import pallas as pl
from jax.experimental.pallas import tpu as pltpu
from jax.sharding import PartitionSpec as P

BRICK = 8


DT_STEP = 0.5
VISCOSITY = 0.1
PRECISE = lax.Precision.HIGHEST


def with_halo(block, sides, width):
    for axis, dim in sides:
        count = lax.axis_size(axis)
        forward = [(i, i + 1) for i in range(count - 1)]
        forward.append((count - 1, 0))
        backward = [(target, source) for source, target in forward]
        low = lax.ppermute(
            lax.slice_in_dim(block, block.shape[dim] - width, None, axis=dim), axis, forward
        )
        high = lax.ppermute(lax.slice_in_dim(block, 0, width, axis=dim), axis, backward)
        block = jnp.concatenate([low, block, high], axis=dim)
    return block


def to_bricks(values):
    components, size_x, size_y, size_z = values.shape
    blocks_view = values.reshape(
        components, size_x // BRICK, BRICK, size_y // BRICK, BRICK, size_z // BRICK, BRICK
    )
    blocks_view = blocks_view.transpose(1, 3, 5, 0, 2, 4, 6)
    return blocks_view.reshape(-1, components * BRICK * BRICK * BRICK)


def from_bricks(bricks, size_x, size_y, size_z):
    blocks_view = bricks.reshape(
        size_x // BRICK, size_y // BRICK, size_z // BRICK, 3, BRICK, BRICK, BRICK
    )
    blocks_view = blocks_view.transpose(3, 0, 4, 1, 5, 2, 6)
    return blocks_view.reshape(3, size_x, size_y, size_z)


def chain_force(positions_f, stiffness_f, rest_f):
    segment = jnp.roll(positions_f, -1, axis=2) - positions_f
    stretch = jnp.sum(segment * segment, axis=1, keepdims=True) / rest_f[:, None, None]
    tension = 0.5 * stiffness_f[:, None, None] * (stretch - 1.0) * segment
    return tension - jnp.roll(tension, 1, axis=2)


def interpolate(bricks_in, weights_f):
    cubes = bricks_in.reshape(-1, 3, BRICK, BRICK, BRICK)
    reduced = jnp.einsum("ncijk,nkm->ncijm", cubes, weights_f[:, 2], precision=PRECISE)
    reduced = jnp.einsum("ncijm,njm->ncim", reduced, weights_f[:, 1], precision=PRECISE)
    return jnp.einsum("ncim,nim->ncm", reduced, weights_f[:, 0], precision=PRECISE)


def spread(forces, weights_f):
    partial_sum = jnp.einsum("ncm,nim->ncim", forces, weights_f[:, 0], precision=PRECISE)
    partial_sum = jnp.einsum("ncim,njm->ncijm", partial_sum, weights_f[:, 1], precision=PRECISE)
    cubes = jnp.einsum("ncijm,nkm->ncijk", partial_sum, weights_f[:, 2], precision=PRECISE)
    return cubes.reshape(cubes.shape[0], -1)


def signed_modes(indices, length):
    return jnp.where(indices <= (length - 1) // 2, indices, indices - length)


def direction_modes(indices, length):
    return jnp.where(2 * indices == length, 0, signed_modes(indices, length))


def tables(length):
    indices = jnp.arange(length, dtype=jnp.int32)
    phases = indices[:, None] * indices[None, :] % length
    angles = 2.0 * jnp.pi / length * phases.astype(jnp.float32)
    return (jnp.cos(angles), jnp.sin(angles))


def forward(form, real_part, imag_part, length):
    cosine, sine = tables(length)
    product = partial(jnp.einsum, precision=PRECISE)
    out_real = product(form, real_part, cosine) + product(form, imag_part, sine)
    out_imag = product(form, imag_part, cosine) - product(form, real_part, sine)
    return (out_real, out_imag)


def backward(form, real_part, imag_part, length):
    cosine, sine = tables(length)
    product = partial(jnp.einsum, precision=PRECISE)
    out_real = product(form, real_part, cosine) - product(form, imag_part, sine)
    out_imag = product(form, imag_part, cosine) + product(form, real_part, sine)
    return (out_real / length, out_imag / length)


def col_transpose(values):
    return lax.all_to_all(values, "col", split_axis=4, concat_axis=3, tiled=True)


def row_transpose(values):
    return lax.all_to_all(values, "row", split_axis=4, concat_axis=2, tiled=True)


def wave_parts(indices, length):
    scale = 2.0 * jnp.pi / length
    direct = direction_modes(indices, length)
    signed = signed_modes(indices, length)
    return (scale * direct.astype(jnp.float32), scale * signed.astype(jnp.float32), direct == 0)


def general(velocity, positions, weights, stiffness, rest_sq, owner_column, brick_index):
    row_count = lax.axis_size("row")
    col_count = lax.axis_size("col")
    size_x = velocity.shape[1]
    size_y = velocity.shape[2]
    size_z = velocity.shape[3]
    block_count = positions.shape[0]
    capacity = max(2, 3 * block_count // col_count)
    total_slots = col_count * capacity
    owner_col = owner_column[:, 0]
    order_ids = jnp.arange(block_count, dtype=jnp.int32)
    earlier_same = (owner_col[None, :] == owner_col[:, None]) & (
        order_ids[None, :] < order_ids[:, None]
    )
    slot_index = owner_col * capacity + jnp.sum(earlier_same.astype(jnp.int32), axis=1)
    stored = to_bricks(velocity)
    brick_count = stored.shape[0]

    def place(values, fill):
        buffer = jnp.full((total_slots,) + values.shape[1:], fill, values.dtype)
        return buffer.at[slot_index].set(values).reshape((col_count, capacity) + values.shape[1:])

    weights_f = weights.astype(jnp.float32)
    forces = chain_force(
        positions.astype(jnp.float32), stiffness.astype(jnp.float32), rest_sq.astype(jnp.float32)
    )
    pushed = spread(forces, weights_f)
    send_force = place(pushed, 0.0)
    send_index = place(brick_index.astype(jnp.float32), 0.0)
    wanted = lax.all_to_all(send_index, "col", split_axis=0, concat_axis=0, tiled=True)
    pushes = lax.all_to_all(send_force, "col", split_axis=0, concat_axis=0, tiled=True)
    wanted_ids = wanted.astype(jnp.int32)
    reply = stored[wanted_ids]
    returned = lax.all_to_all(reply, "col", split_axis=0, concat_axis=0, tiled=True)
    returned, arrived_ids, arrived = (returned, wanted_ids, pushes)
    fetched = returned.reshape(total_slots, -1)[slot_index]
    marker_velocity = interpolate(fetched, weights_f)
    forcing = jax.ops.segment_sum(
        arrived.reshape(total_slots, -1), arrived_ids.reshape(-1), num_segments=brick_count
    )
    force_field = from_bricks(forcing, size_x, size_y, size_z)
    padded = with_halo(velocity, (("row", 1), ("col", 2)), 1)
    grad_x = (padded[:, 2:, 1:-1] - padded[:, :-2, 1:-1]) * 0.5
    grad_y = (padded[:, 1:-1, 2:] - padded[:, 1:-1, :-2]) * 0.5
    grad_z = (jnp.roll(velocity, -1, axis=3) - jnp.roll(velocity, 1, axis=3)) * 0.5
    transport = velocity[0] * grad_x + velocity[1] * grad_y + velocity[2] * grad_z
    star = velocity + DT_STEP * (force_field - transport)
    cos_z, sin_z = tables(size_z)
    half_z = size_z // 2
    col_here = lax.axis_index("col")
    cos_fore = cos_z[:, :half_z]
    sin_fore = sin_z[:, :half_z].at[:, 0].set(-cos_z[:, half_z])
    z_real = jnp.einsum("cxyz,zk->cxyk", star, cos_fore, precision=PRECISE)
    z_imag = -jnp.einsum("cxyz,zk->cxyk", star, sin_fore, precision=PRECISE)
    shuffled = col_transpose(jnp.stack([z_real, z_imag]))
    slab = shuffled.shape[4]
    first_slot = (col_here == 0) & (jnp.arange(slab, dtype=jnp.int32) == 0)
    highest = shuffled[1][..., 0:1] * (col_here == 0).astype(jnp.float32)
    lower_imag = jnp.where(first_slot, 0.0, shuffled[1])
    y_in_real = jnp.concatenate([shuffled[0], highest], axis=3)
    y_in_imag = jnp.concatenate([lower_imag, jnp.zeros_like(highest)], axis=3)
    z_index = jnp.concatenate(
        [col_here * slab + jnp.arange(slab, dtype=jnp.int32), jnp.full((1,), half_z, jnp.int32)]
    )
    y_real, y_imag = forward("cxyz,yk->cxzk", y_in_real, y_in_imag, y_in_real.shape[2])
    shuffled = row_transpose(jnp.stack([y_real, y_imag]))
    x_real, x_imag = forward("cxzy,xk->czyk", shuffled[0], shuffled[1], shuffled.shape[2])
    slab_y = x_real.shape[2]
    full_x = x_real.shape[3]
    full_y = slab_y * row_count
    y_index = lax.axis_index("row") * slab_y + jnp.arange(slab_y, dtype=jnp.int32)
    x_index = jnp.arange(full_x, dtype=jnp.int32)
    dir_z, sig_z, zero_z = wave_parts(z_index, size_z)
    dir_y, sig_y, zero_y = wave_parts(y_index, full_y)
    dir_x, sig_x, zero_x = wave_parts(x_index, full_x)
    wave_z = dir_z[:, None, None]
    wave_y = dir_y[None, :, None]
    wave_x = dir_x[None, None, :]
    no_direction = zero_z[:, None, None] & zero_y[None, :, None] & zero_x[None, None, :]
    wave_sq = wave_x * wave_x + wave_y * wave_y + wave_z * wave_z
    full_sq = sig_z[:, None, None] ** 2 + sig_y[None, :, None] ** 2 + sig_x[None, None, :] ** 2
    inverse_sq = jnp.where(no_direction, 0.0, 1.0 / jnp.where(no_direction, 1.0, wave_sq))
    damping = 1.0 / (1.0 + DT_STEP * VISCOSITY * full_sq)
    waves = jnp.stack(
        [
            jnp.broadcast_to(wave_x, wave_sq.shape),
            jnp.broadcast_to(wave_y, wave_sq.shape),
            jnp.broadcast_to(wave_z, wave_sq.shape),
        ]
    )
    normal_real = jnp.sum(waves * x_real, axis=0) * inverse_sq
    normal_imag = jnp.sum(waves * x_imag, axis=0) * inverse_sq
    p_real = (x_real - waves * normal_real) * damping
    p_imag = (x_imag - waves * normal_imag) * damping
    b_real, b_imag = backward("czyk,kx->cyzx", p_real, p_imag, full_x)
    shuffled = row_transpose(jnp.stack([b_real, b_imag]))
    b_real, b_imag = backward("cyzx,yk->cxzk", shuffled[0], shuffled[1], shuffled.shape[2])
    slab = b_real.shape[2] - 1
    first_slot = (col_here == 0) & (jnp.arange(slab, dtype=jnp.int32) == 0)
    highest = b_real[:, :, slab:, :]
    packed_imag = jnp.where(first_slot[None, None, :, None], highest, b_imag[:, :, :slab, :])
    shuffled = col_transpose(jnp.stack([b_real[:, :, :slab, :], packed_imag]))
    doubling = jnp.where(jnp.arange(half_z, dtype=jnp.int32) == 0, 1.0, 2.0)[:, None]
    cos_back = cos_z[:half_z] * doubling
    sin_back = (sin_z[:half_z] * doubling).at[0].set(-cos_z[half_z])
    new_velocity = (
        jnp.einsum("cxky,kz->cxyz", shuffled[0], cos_back, precision=PRECISE)
        - jnp.einsum("cxky,kz->cxyz", shuffled[1], sin_back, precision=PRECISE)
    ) / size_z
    return (new_velocity, marker_velocity)


VMEM = pltpu.VMEM
MESH = pl.DeviceIdType.MESH
F32 = jnp.float32
BF16 = jnp.bfloat16
I32 = jnp.int32
TOP = 32700.0
NT = ((1,), (1,))


def two_parts(table):
    table = np.asarray(table, np.float64)
    high = table.astype(jnp.bfloat16)
    low = (table - high.astype(np.float64)).astype(jnp.bfloat16)
    return np.stack([high, low])


def angle_of(length, left, right):
    return 2.0 * np.pi / length * (np.outer(left, right) % length)


def build_tables(size_x, size_y, size_z, rows):
    half_z = size_z // 2
    turn = angle_of(size_z, np.arange(size_z), np.arange(half_z))
    fore = np.concatenate([np.cos(turn), -np.sin(turn)], axis=1)
    back = np.concatenate([2.0 * np.cos(turn), -2.0 * np.sin(turn)], axis=1)
    alternate = np.where(np.arange(size_z) % 2 == 0, 1.0, -1.0)
    fore[:, half_z] = alternate
    back[:, 0], back[:, half_z] = 1.0, alternate
    back = back.T / (size_x * size_y * size_z)
    turn_y = angle_of(size_y, np.arange(size_y), np.arange(size_y))
    line = np.concatenate([np.cos(turn_y), np.sin(turn_y)], axis=0)
    lane = np.arange(size_x)
    place = (lane % rows) * (size_x // rows) + lane // rows
    turn_x = angle_of(size_x, place, np.arange(size_x))
    cosine, sine = np.cos(turn_x), np.sin(turn_x)
    wide = np.concatenate(
        [np.concatenate([cosine, -sine], axis=1), np.concatenate([sine, cosine], axis=1)], axis=0
    )
    return tuple(two_parts(t) for t in (fore, back, line, wide, wide.T))


def parts(values):
    high = values.astype(BF16)
    return high, (values - high.astype(F32)).astype(BF16)


def mul(left, right, dims=((1,), (0,))):
    return lax.dot_general(left, right, (dims, ((), ())), preferred_element_type=F32)


def mul3(left, right, dims=((1,), (0,))):
    return (
        mul(left[0], right[0], dims) + mul(left[1], right[0], dims) + mul(left[0], right[1], dims)
    )


def roll(values, shift):
    return pltpu.roll(values, shift % 128, values.ndim - 1)


def lanes_of(shape):
    return lax.broadcasted_iota(I32, shape, len(shape) - 1)


def code_of(peak):
    return jnp.floor(jnp.log2(jnp.maximum(peak, 1e-30)) * 65536.0).astype(I32) + 2


def unit_of(code):
    return jnp.exp2(code.astype(F32) * (1.0 / 65536.0)) * (1.0 / TOP)


def whole(values):
    return jnp.round(values).astype(I32)


def join(first, second):
    return (first << 16) + second


def split(word):
    second = (word << 16) >> 16
    return (word - second) >> 16, second


def swap_bits(tiles, steps):
    tiles = list(tiles)
    keep = {s: (lanes_of(tiles[0].shape) & s) == 0 for s in steps}
    for bit, step in enumerate(steps):
        for one in range(len(tiles)):
            if one >> bit & 1:
                continue
            two = one | 1 << bit
            a, b = tiles[one], tiles[two]
            tiles[one] = jnp.where(keep[step], a, roll(b, step))
            tiles[two] = jnp.where(keep[step], roll(a, -step), b)
    return tiles


def compress(tiles, lane):
    out = []
    for t in range(9):
        out.append(jnp.where(lane < 96, tiles[t], roll(tiles[9 + t // 3], 96 - 32 * (t % 3))))
    return out


def expand(tiles, lane):
    out = list(tiles)
    for u in range(3):
        a, b, c = (roll(tiles[3 * u + p], 32 + 32 * p) for p in range(3))
        out.append(jnp.where(lane < 32, a, jnp.where(lane < 64, b, c)))
    return out


def pack_cubes(wide, lane):
    tiles = [wide[t * 8 : t * 8 + 8].astype(I32) for t in range(24)]
    words = []
    for c in range(3):
        for i in range(4):
            words.append(join(tiles[c * 8 + i], tiles[c * 8 + i + 4]))
    return compress(words, lane)


def open_cubes(tiles, lane):
    out = [None] * 24
    for t, word in enumerate(expand(tiles, lane)):
        at = t // 4 * 8 + t % 4
        out[at], out[at + 4] = split(word)
    return jnp.concatenate([t.astype(F32) for t in out], axis=0)


def pad(tile):
    return jnp.concatenate([tile, jnp.zeros((3, 128), I32)], axis=0)


def fold(tile, low, near):
    other = pltpu.roll(roll(tile, 64), 4, 0)
    return jnp.where(jnp.logical_or(low, jnp.logical_not(near)), tile, other)


def unfold(tile, near):
    return jnp.where(near, tile, pltpu.roll(roll(tile, 64), 4, 0))


def peak_of(values):
    while values.ndim > 2:
        values = jnp.max(values, axis=0)
    return jnp.max(jnp.max(values, axis=0, keepdims=True), axis=1, keepdims=True)


def column(row):
    shape = (row.shape[1], row.shape[1])
    diagonal = lax.broadcasted_iota(I32, shape, 0) == lax.broadcasted_iota(I32, shape, 1)
    return jnp.sum(jnp.where(diagonal, row, 0.0), axis=1, keepdims=True)


def mix(step, cols):
    ring, pair = step // cols, step % cols
    return ((6, 2, 4, 7, 3, 5, 1, 0).index(pair % 8), (2, 1, 3, 0).index(ring % 4), step)


def main_kernel(
    rows, columns, capacity,
    owner_hbm, brick_hbm, stiff_hbm, rest_hbm, pos_hbm, weight_hbm, velocity_hbm,
    fore_hbm, line_hbm, wide_hbm, unwide_hbm, back_hbm,
    last_ref, mark_ref, back_ref,
    owner_ref, brick_ref, stiff_ref, rest_ref, pos_ref, weight_ref, velocity_ref,
    fore_ref, line_ref, wide_ref, unwide_ref, noted,
    force, deep, cube, place, face_x, face_y, near_x, near_y, push, pushed, star, select,
    held, modes, arrived, reply, replied, ready,
    load_sems, face_sems, push_sems, mode_sems, reply_sems, last_sems,
):
    sources = (
        owner_hbm, brick_hbm, stiff_hbm, rest_hbm, pos_hbm, weight_hbm, velocity_hbm,
        fore_hbm, line_hbm, wide_hbm, unwide_hbm, back_hbm,
    )
    targets = (
        owner_ref, brick_ref, stiff_ref, rest_ref, pos_ref, weight_ref, velocity_ref,
        fore_ref, line_ref, wide_ref, unwide_ref, back_ref,
    )
    loads = []
    for number, (source, target) in enumerate(zip(sources, targets)):
        loads.append(pltpu.make_async_copy(source, target, load_sems.at[number]))
        loads[-1].start()
    row, col = lax.axis_index("row"), lax.axis_index("col")
    devices = rows * columns
    blocks = pos_ref.shape[1]
    size_x, size_y, size_z = velocity_ref.shape[1:]
    bricks_x = size_x // 8
    barrier = pltpu.get_barrier_semaphore()

    def flip(step):
        at, bit = 0, 1
        while bit < columns:
            own = lax.rem(col // bit, 2)
            at = at + bit * (1 - own if step & bit else own)
            bit *= 2
        return at

    def peer(step):
        to_row, to_col = lax.rem(row + step // columns, rows), flip(step % columns)
        return (to_row, to_col), to_row * columns + to_col

    greet = list(range(1, columns)) + list(range(columns, devices, columns))
    for step in greet:
        pl.semaphore_signal(barrier, inc=1, device_id=peer(step)[0], device_id_type=MESH)

    def remote(source, target, sems, step, device):
        return pltpu.make_async_remote_copy(
            source, target, sems.at[0, step], sems.at[1, step],
            device_id=device, device_id_type=MESH,
        )

    def send_all(source, target, sems, around):
        waits = []
        count = devices if around else columns
        me = row * columns + col if around else col
        for step in sorted(range(1, count), key=lambda n: mix(n, columns)):
            device, at = peer(step)
            at = at if around else device[1]
            copy = remote(source.at[at], target.at[me], sems, step, device)
            copy.start()
            opposite = (rows - step // columns) % rows * columns + step % columns
            origin_device, origin = peer(opposite)
            origin = origin if around else origin_device[1]
            arrival = remote(source.at[at], target.at[origin], sems, step, device)
            waits.append((copy, arrival))
        own = pltpu.make_async_copy(source.at[me], target.at[me], sems.at[0, 0])
        own.start()
        return waits, own

    def receive(sent):
        for _, arrival in sent[0]:
            arrival.wait_recv()
        sent[1].wait()

    def finish(sent):
        for copy, _ in sent[0]:
            copy.wait_send()

    lane8 = lanes_of((8, 128))
    near = lax.broadcasted_iota(I32, (8, 128), 0) < 4

    for load in loads[:4]:
        load.wait()
    owner_row = owner_ref[...].astype(F32)
    owner = column(owner_row)
    shape = (blocks, blocks)
    earlier = lax.broadcasted_iota(I32, shape, 1) < lax.broadcasted_iota(I32, shape, 0)
    rank = jnp.sum(
        jnp.where((owner == owner_row) & earlier, 1.0, 0.0), axis=1, keepdims=True
    )
    slot = jnp.broadcast_to(owner * 128.0 + rank * 8.0, (blocks, 128))
    brick = jnp.broadcast_to(column(brick_ref[...].astype(F32)) + 1.0, (blocks, 128))
    deep_shape = (blocks, 8, 128)
    inner = lax.broadcasted_iota(I32, deep_shape, 1).astype(F32)
    lane_f = lanes_of((blocks, 128)).astype(F32)
    for at in range(columns):
        ahead = lane_f + 128.0 * at - slot
        named = jnp.where((ahead >= 0.0) & (ahead < 8.0), brick, 0.0)
        named = jnp.sum(named, axis=0, keepdims=True).astype(I32)
        noted[at] = jnp.broadcast_to(named, (8, 128))
    slot = (slot[:, None, :] + inner).reshape(blocks * 8, 128)
    lane_f = lanes_of((blocks * 8, 128)).astype(F32)
    for at in range(columns):
        hit = slot == lane_f + 128.0 * at
        place[:, at * 128 : (at + 1) * 128] = jnp.where(hit, 1.0, 0.0).astype(BF16)

    for load in loads[4:6]:
        load.wait()
    stiff = column(stiff_ref[...].astype(F32))
    rest = column(rest_ref[...].astype(F32))
    points = [pos_ref[c].astype(F32) for c in range(3)]
    segment = [pltpu.roll(p, 127, 1) - p for p in points]
    stretch = sum(part * part for part in segment) / rest
    pull = 0.5 * stiff * (stretch - 1.0)
    for c in range(3):
        tension = pull * segment[c]
        force[c] = tension - pltpu.roll(tension, 1, 1)

    def spread(index, carry):
        first = weight_ref[index, 0].astype(F32)
        second = weight_ref[index, 1].astype(F32)
        third = weight_ref[index, 2].astype(F32)
        high, low = parts((first[:, None, :] * third[None]).reshape(64, 128))
        both = jnp.concatenate([high, low], axis=0)
        deep[index] = both
        pushes = jnp.concatenate([force[c, pl.ds(index, 1), :] * second for c in range(3)], axis=0)
        upper = pushes.astype(BF16).astype(F32)
        left = jnp.concatenate([upper, pushes - upper], axis=0).astype(BF16)
        result = mul(left, both, NT)
        total = result[0:24] + result[24:48]
        total = total + pltpu.roll(total, 64, 1)
        cube[index] = total.reshape(3, 8, 128)
        return carry

    lax.fori_loop(0, blocks, spread, 0, unroll=32)

    low_half = lane8 < 64
    outs = [[None] * 2 for _ in range(24)]
    for c in range(3):
        for g in range(2):
            tiles = [
                jnp.where(low_half, cube[g * 16 + b, c], cube[g * 16 + 8 + b, c]) for b in range(8)
            ]
            for i, tile in enumerate(swap_bits(tiles, (8, 16, 32))):
                outs[c * 8 + i][g] = tile
    spreads = jnp.concatenate([jnp.concatenate(pair, axis=1) for pair in outs], axis=0)
    push_code = code_of(peak_of(jnp.abs(spreads)))
    high, low = parts(jnp.round(spreads * (1.0 / unit_of(push_code))))

    for load in loads[6:-1]:
        load.wait()
    value_code = code_of(peak_of(jnp.abs(velocity_ref[...].reshape(-1, 8, size_z))))
    scale = 1.0 / unit_of(value_code)
    half = size_x // 2
    for side, at in ((0, size_x - 1), (1, 0)):
        cells = whole(velocity_ref[:, at] * scale[None])
        face_x[side, 0:24] = join(cells[:, :, 0:128], cells[:, :, 128:256]).reshape(24, 128)
        face_x[side, 24:25] = jnp.broadcast_to(value_code, (1, 128))
    for side, at in ((0, size_y - 1), (1, 0)):
        cells = whole(velocity_ref[:, :, at, :] * scale[None])
        face_y[side, 0:24] = join(cells[:, 0:half], cells[:, half:]).reshape(24, size_z)
        face_y[side, 24:25] = jnp.broadcast_to(value_code, (1, size_z))

    pl.semaphore_wait(barrier, len(greet))
    faces = []
    for source, target, base, axis in ((face_x, near_x, 0, 0), (face_y, near_y, 2, 1)):
        for side in range(2):
            extent = (rows, columns)[axis]
            step = 1 if side == 0 else extent - 1
            if axis == 0:
                device = (lax.rem(row + step, rows), col)
            else:
                device = (row, lax.rem(col + step, columns))
            copy = remote(source.at[side], target.at[side], face_sems, base + side, device)
            copy.start()
            faces.append(copy)

    near_order = sorted(range(1, columns), key=lambda n: mix(n, columns))
    pushes, waiting = [], None
    for step in near_order + [0]:
        device, _ = peer(step)
        at = device[1]
        window = place[:, pl.ds(pl.multiple_of(at * 128, 128), 128)]
        tiles = pack_cubes(mul(high, window) + mul(low, window), lane8)
        target = push if step else pushed
        for t in range(9):
            target[at, t * 8 : t * 8 + 8] = tiles[t]
        target[at, 72:73] = jnp.where(lane8[0:1] < 96, noted[at, 0:1], push_code)
        if waiting is not None:
            waiting.start()
        if step:
            waiting = remote(push.at[at], pushed.at[col], push_sems, step, device)
            arrival = remote(push.at[at], pushed.at[at], push_sems, step, device)
            pushes.append((waiting, arrival))

    for copy in faces:
        copy.wait()
    value = velocity_ref[...]
    sides_x, sides_y = [], []
    for side in range(2):
        unit = unit_of(near_x[side, 24:25])[:, 0:1]
        one, two = split(near_x[side, 0:24])
        wide = jnp.concatenate([one.astype(F32), two.astype(F32)], axis=1) * unit
        sides_x.append(wide.reshape(3, 1, size_y, size_z))
        unit = unit_of(near_y[side, 24:25])[:, 0:1]
        one, two = (part.astype(F32) * unit for part in split(near_y[side, 0:24]))
        wide = [part.reshape(3, half, size_z) for part in (one, two)]
        sides_y.append(jnp.concatenate(wide, axis=1).reshape(3 * size_x, 1, size_z))
    ahead = jnp.concatenate([value[:, 1:], sides_x[1]], axis=1)
    behind = jnp.concatenate([sides_x[0], value[:, :-1]], axis=1)
    transport = value[0:1] * ((ahead - behind) * 0.5)
    flat = value.reshape(3 * size_x, size_y, size_z)
    sub = lax.broadcasted_iota(I32, flat.shape, 1)
    face_low, face_high = sides_y
    ahead = jnp.where(sub == size_y - 1, face_high, pltpu.roll(flat, size_y - 1, 1))
    behind = jnp.where(sub == 0, face_low, pltpu.roll(flat, 1, 1))
    transport += value[1:2] * ((ahead - behind) * 0.5).reshape(value.shape)
    ahead = pltpu.roll(flat, size_z - 1, 2)
    behind = pltpu.roll(flat, 1, 2)
    transport += value[2:3] * ((ahead - behind) * 0.5).reshape(value.shape)
    star[...] = value - DT_STEP * transport

    spot = lax.broadcasted_iota(I32, (bricks_x * size_z, 128), 0)
    inner = lanes_of((1, 128)) & 7
    origins = [0] + near_order
    for k, step in enumerate(origins):
        if step:
            pushes[k - 1][1].wait_recv()
        at = peer(step)[0][1]
        tiles = [pushed[at, t * 8 : t * 8 + 8] for t in range(9)]
        meta = pushed[at, 72:73]
        unit = unit_of(meta)[:, 127:128]
        wide = open_cubes(tiles, lane8).reshape(24, 8, 128) * unit[None]
        high, low = parts(wide.reshape(192, 128))
        held[0, :, k * 128 : (k + 1) * 128] = high
        held[1, :, k * 128 : (k + 1) * 128] = low
        mark = jnp.where((lanes_of((1, 128)) < 96) & (meta > 0), (meta - 1) * 8 + inner, -1)
        select[:, k * 128 : (k + 1) * 128] = jnp.where(spot == mark, 1.0, 0.0).astype(BF16)
        if k % 2 == 0:
            continue
        span = slice((k - 1) * 128, (k + 1) * 128)
        for brick_x in range(bricks_x):
            chosen = select[brick_x * size_z : (brick_x + 1) * size_z, span]
            field = mul(held[0, :, span], chosen, NT) + mul(held[1, :, span], chosen, NT)
            star[:, brick_x * 8 : (brick_x + 1) * 8] += DT_STEP * field.reshape(3, 8, 8, size_z)

    spectrum = mul3(parts(star[...].reshape(-1, size_z)), (fore_ref[0], fore_ref[1]))
    real = spectrum[:, 0:128].reshape(3 * size_x, 8, 128)
    imag = spectrum[:, 128:256].reshape(3 * size_x, 8, 128)
    peak = jnp.maximum(jnp.max(jnp.abs(real), axis=0), jnp.max(jnp.abs(imag), axis=0))
    mode_code = jnp.broadcast_to(code_of(jnp.max(peak, axis=0, keepdims=True)), (8, 128))
    scale = (1.0 / unit_of(mode_code))[None]
    words = join(whole(real * scale), whole(imag * scale))
    steps = (4, 8, 16, 32, 64)
    tiles = swap_bits([words[t] for t in range(32)], steps)
    for t in range(devices):
        modes[t, 0:8] = tiles[t]
    tiles = swap_bits([words[32 + t] for t in range(16)] + [mode_code] * 16, steps)
    for t in range(devices):
        modes[t, 8:13] = fold(tiles[t], low_half, near)[0:5]
    moved = send_all(modes, arrived, mode_sems, True)

    scale = 1.0 / unit_of(value_code)
    cells = []
    for brick_x in range(bricks_x):
        piece = velocity_ref[:, brick_x * 8 : (brick_x + 1) * 8].reshape(192, size_z)
        cells.append(parts(jnp.round(piece * scale)))
    for k, step in enumerate(origins):
        at = peer(step)[0][1]
        wide = None
        for brick_x in range(bricks_x):
            chosen = select[
                brick_x * size_z : (brick_x + 1) * size_z, k * 128 : (k + 1) * 128
            ]
            piece = mul(cells[brick_x][0], chosen) + mul(cells[brick_x][1], chosen)
            wide = piece if wide is None else wide + piece
        tiles = pack_cubes(wide, lane8)
        for t in range(9):
            reply[at, t * 8 : t * 8 + 8] = tiles[t]
        reply[at, 72:73] = jnp.broadcast_to(value_code, (1, 128))

    receive(moved)
    here = row * columns + col
    first = here == 0
    upper = jnp.logical_not(low_half)
    lines = [[[] for _ in range(3)] for _ in range(4)]
    for at in range(columns):
        zero = swap_bits([arrived[r * columns + at, 0:8] for r in range(rows)], (1, 2))
        rest_tiles = swap_bits([pad(arrived[r * columns + at, 8:13]) for r in range(rows)], (1, 2))
        for mode in range(4):
            code = jnp.broadcast_to(rest_tiles[mode][4:5], (8, 128))
            unit = unit_of(jnp.where(low_half, roll(code, 64), code))
            real0, imag0 = (p.astype(F32) * unit for p in split(zero[mode]))
            real1, imag1 = (p.astype(F32) * unit for p in split(unfold(rest_tiles[mode], near)))
            lines[mode][0].append(jnp.where(low_half, real0, roll(imag0, 64)))
            lines[mode][1].append(jnp.where(low_half, roll(real0, 64), imag0))
            lines[mode][2].append(jnp.where(low_half, real1, roll(imag1, 64)))
    lines = [[jnp.concatenate(lines[mode][c], axis=0) for c in range(3)] for mode in range(4)]
    wide_y = columns * 8
    low_line = lanes_of((wide_y, 128)) < 64
    lines.append([jnp.where(low_line, roll(v, 64), 0.0) for v in lines[0]])
    lines[0] = [jnp.where(jnp.logical_and(first, jnp.logical_not(low_line)), 0.0, v) for v in lines[0]]
    line_table = (line_ref[0], line_ref[1])
    sign = jnp.where(low_line, 1.0, -1.0)
    lined = []
    for slot_at in range(5):
        both = mul3(line_table, parts(jnp.concatenate(lines[slot_at], axis=1)))
        for c in range(3):
            a = both[0:wide_y, c * 128 : (c + 1) * 128]
            b = both[wide_y:, c * 128 : (c + 1) * 128]
            lined.append(a + sign * roll(b, 64))
    full_x = rows * size_x
    index = lanes_of((wide_y, 128)) & (full_x - 1)
    line = lax.broadcasted_iota(I32, (wide_y, 128), 0)
    scale_x, scale_y, scale_z = (2.0 * np.pi / n for n in (full_x, wide_y, size_z))
    sig_x = jnp.where(index < full_x // 2, index, index - full_x).astype(F32) * scale_x
    sig_y = jnp.where(line < wide_y // 2, line, line - wide_y).astype(F32) * scale_y
    wave_x = jnp.where(index == full_x // 2, 0.0, sig_x)
    wave_y = jnp.where(line == wide_y // 2, 0.0, sig_y)
    backs = []
    replies = send_all(reply, replied, reply_sems, False)
    for slot_at in range(5):
        spot_lines = jnp.concatenate(lined[slot_at * 3 : slot_at * 3 + 3], axis=0)
        values = mul3(parts(spot_lines), (wide_ref[0], wide_ref[1]))
        x, y, z = (values[c * wide_y : (c + 1) * wide_y] for c in range(3))
        if slot_at < 4:
            sig_z = (here * 4 + slot_at).astype(F32) * scale_z
            wave_z = sig_z
        else:
            sig_z, wave_z = F32(np.pi), F32(0.0)
        square = wave_x * wave_x + wave_y * wave_y + wave_z * wave_z
        full = sig_x * sig_x + sig_y * sig_y + sig_z * sig_z
        none = square == 0.0
        inverse_sq = jnp.where(none, 0.0, 1.0 / jnp.where(none, 1.0, square))
        damping = 1.0 / (1.0 + DT_STEP * VISCOSITY * full)
        normal = (wave_x * x + wave_y * y + wave_z * z) * inverse_sq
        result = jnp.concatenate(
            [
                (x - wave_x * normal) * damping,
                (y - wave_y * normal) * damping,
                (z - wave_z * normal) * damping,
            ],
            axis=0,
        )
        turned = mul3(parts(result), (unwide_ref[0], unwide_ref[1]))
        stacked = jnp.concatenate(
            [turned[c * wide_y : (c + 1) * wide_y] for c in range(3)], axis=1
        )
        both = mul3(line_table, parts(stacked))
        back = []
        for c in range(3):
            a = both[0:wide_y, c * 128 : (c + 1) * 128]
            b = both[wide_y:, c * 128 : (c + 1) * 128]
            back.append(a - sign * roll(b, 64))
        backs.append(back)
    top = jnp.logical_and(first, jnp.logical_not(low_line))
    backs[0] = [jnp.where(top, roll(backs[4][c], 64), backs[0][c]) for c in range(3)]
    zero_words, rest_words = [], []
    for mode in range(4):
        e = backs[mode]
        peak = jnp.maximum(jnp.maximum(jnp.abs(e[0]), jnp.abs(e[1])), jnp.abs(e[2]))
        code = code_of(peak_of(peak))
        scale = 1.0 / unit_of(code)
        e = [v * scale for v in e]
        real0 = whole(jnp.where(low_line, e[0], roll(e[1], 64)))
        imag0 = whole(jnp.where(low_line, roll(e[0], 64), e[1]))
        zero_words.append(join(real0, imag0))
        rest_words.append(jnp.where(low_line, join(whole(e[2]), whole(roll(e[2], 64))), code))
    for at in range(columns):
        span = slice(at * 8, at * 8 + 8)
        tiles = swap_bits([w[span] for w in zero_words], (1, 2))
        for r in range(rows):
            ready[r * columns + at, 0:8] = tiles[r]
        tiles = swap_bits([w[span] for w in rest_words], (1, 2))
        for r in range(rows):
            ready[r * columns + at, 8:13] = fold(tiles[r], low_half, near)[0:5]
    lasts = send_all(ready, last_ref, last_sems, True)

    receive(replies)
    for at in range(columns):
        tiles = [replied[at, t * 8 : t * 8 + 8] for t in range(9)]
        unit = unit_of(replied[at, 72:73])
        wide = open_cubes(tiles, lane8).reshape(24, 8, 128) * unit[None]
        high, low = parts(wide.reshape(192, 128))
        held[0, :, at * 128 : (at + 1) * 128] = high
        held[1, :, at * 128 : (at + 1) * 128] = low
    fetched = mul(held[0], place[...], NT) + mul(held[1], place[...], NT)
    for c in range(3):
        for g in range(2):
            tiles = [
                fetched[c * 64 + i * 8 : c * 64 + i * 8 + 8, g * 128 : (g + 1) * 128]
                for i in range(8)
            ]
            for b, tile in enumerate(swap_bits(tiles, (8, 16, 32))):
                cube[g * 8 + b, c] = tile

    low_rows = lanes_of((24, 128)) < 64

    def interpolate_pair(index, carry):
        block = index // 8 * 16 + lax.rem(index, 8)
        cells = cube[index].reshape(24, 128)
        apart = jnp.concatenate(
            [jnp.where(low_rows, cells, 0.0), jnp.where(low_rows, 0.0, cells)], axis=0
        )
        high, low = parts(apart)
        one, two = deep[block], deep[block + 8]
        upper = jnp.concatenate([one[0:64], two[0:64]], axis=0)
        lower = jnp.concatenate([one[64:128], two[64:128]], axis=0)
        summed = mul(high, upper) + mul(low, upper) + mul(high, lower)
        for half, at in ((0, block), (1, block + 8)):
            second = weight_ref[at, 1].astype(F32)
            piece = summed[half * 24 : half * 24 + 24].reshape(3, 8, 128) * second[None]
            piece = jnp.sum(piece, axis=1)
            for c in range(3):
                mark_ref[c, pl.ds(at, 1), :] = piece[c : c + 1]
        return carry

    lax.fori_loop(0, blocks // 2, interpolate_pair, 0, unroll=4)
    loads[-1].wait()
    receive(lasts)
    for copy, _ in pushes:
        copy.wait_send()
    for sent in (moved, replies, lasts):
        finish(sent)


def final_kernel(last_ref, back_ref, mark_ref, new_hbm, out_hbm, new_ref, sems):
    devices = last_ref.shape[0]
    copies = [pltpu.make_async_copy(mark_ref, out_hbm, sems.at[3])]
    copies[0].start()
    steps = (4, 8, 16, 32, 64)
    words = swap_bits([last_ref[t, 0:8] for t in range(devices)], steps)
    low = lanes_of((8, 128)) < 64
    near = lax.broadcasted_iota(I32, (8, 128), 0) < 4
    rest = []
    for t in range(devices):
        tile = pad(last_ref[t, 8:13])
        code = jnp.broadcast_to(tile[4:5], (8, 128))
        rest.append(jnp.where(low, unfold(tile, near), code))
    rest = swap_bits(rest, steps)
    unit = unit_of(rest[16])
    words += rest[0:16]
    rows = []
    for word in words:
        real, imag = split(word)
        rows.append(jnp.concatenate([real.astype(F32) * unit, imag.astype(F32) * unit], axis=1))
    count = len(rows) // 3
    for c in range(3):
        lines = jnp.concatenate(rows[c * count : (c + 1) * count], axis=0)
        result = mul3(parts(lines), (back_ref[0], back_ref[1]))
        new_ref[c] = result.reshape(new_ref.shape[1:])
        copies.append(pltpu.make_async_copy(new_ref.at[c], new_hbm.at[c], sems.at[c]))
        copies[-1].start()
    for copy in copies:
        copy.wait()


def local(velocity, positions, weights, stiffness, rest_sq, owner_column, brick_index):
    rows = lax.axis_size("row")
    columns = lax.axis_size("col")
    devices = rows * columns
    _, local_x, local_y, size_z = velocity.shape
    blocks = positions.shape[0]
    capacity = max(2, 3 * blocks // columns)
    fits = (
        local_x == 16 and local_y == 8 and size_z == 8 * devices and positions.shape[2] == 128
        and capacity == 12 and blocks == 32 and columns == 8 and rows == 4
    )
    if not fits:
        return general(
            velocity, positions, weights, stiffness, rest_sq, owner_column, brick_index
        )
    return fast(velocity, positions, weights, stiffness, rest_sq, owner_column, brick_index)


def fast(velocity, positions, weights, stiffness, rest_sq, owner_column, brick_index):
    rows = lax.axis_size("row")
    columns = lax.axis_size("col")
    devices = rows * columns
    _, local_x, local_y, size_z = velocity.shape
    blocks = positions.shape[0]
    capacity = max(2, 3 * blocks // columns)
    size_x, size_y = rows * local_x, columns * local_y
    fore, back, line, wide, unwide = build_tables(size_x, size_y, size_z, rows)
    vm = pl.BlockSpec(memory_space=VMEM)
    shape = jax.ShapeDtypeStruct
    cells = local_x // BRICK * size_z
    dma = pltpu.SemaphoreType.DMA
    operands = (
        owner_column.reshape(1, blocks), brick_index.reshape(1, blocks),
        stiffness.reshape(1, blocks), rest_sq.reshape(1, blocks),
        positions.transpose(1, 0, 2), weights, velocity, fore, line, wide, unwide,
    )
    last, marks, back = pl.pallas_call(
        partial(main_kernel, rows, columns, capacity),
        out_shape=[
            VMEM((devices, 13, 128), I32), VMEM((3, blocks, 128), F32), VMEM(back.shape, BF16),
        ],
        in_specs=[pl.BlockSpec(memory_space=pl.ANY)] * 12,
        out_specs=[vm, vm, vm],
        scratch_shapes=[VMEM(a.shape, a.dtype) for a in operands] + [
            VMEM((columns, 8, 128), I32),
            VMEM((3, blocks, 128), F32),
            VMEM((blocks, 128, 128), BF16),
            VMEM((blocks, 3, 8, 128), F32),
            VMEM((blocks * 8, columns * 128), BF16),
            VMEM((2, 25, 128), I32),
            VMEM((2, 25, size_z), I32),
            VMEM((2, 25, 128), I32),
            VMEM((2, 25, size_z), I32),
            VMEM((columns, 73, 128), I32),
            VMEM((columns, 73, 128), I32),
            VMEM((3, local_x, local_y, size_z), F32),
            VMEM((cells, columns * 128), BF16),
            VMEM((2, 192, columns * 128), BF16),
            VMEM((devices, 13, 128), I32),
            VMEM((devices, 13, 128), I32),
            VMEM((columns, 73, 128), I32),
            VMEM((columns, 73, 128), I32),
            VMEM((devices, 13, 128), I32),
            dma((12,)),
            dma((2, 4)),
            dma((2, columns)),
            dma((2, devices)),
            dma((2, columns)),
            dma((2, devices)),
        ],
        compiler_params=pltpu.CompilerParams(collective_id=1, has_side_effects=True),
        name="step",
    )(*operands, back)
    new_velocity, marks = pl.pallas_call(
        final_kernel,
        out_shape=[shape(velocity.shape, F32), shape((3, blocks, 128), F32)],
        in_specs=[vm, vm, vm],
        out_specs=[pl.BlockSpec(memory_space=pl.ANY)] * 2,
        scratch_shapes=[VMEM(velocity.shape, F32), dma((4,))],
        name="final",
    )(
        pltpu.with_memory_space_constraint(last, VMEM),
        pltpu.with_memory_space_constraint(back, VMEM),
        pltpu.with_memory_space_constraint(marks, VMEM),
    )
    return new_velocity, marks.transpose(1, 0, 2)


def solution(mesh):
    return jax.shard_map(
        local,
        mesh=mesh,
        in_specs=(
            P(None, "row", "col", None),
            P(("row", "col"), None, None),
            P(("row", "col"), None, None, None),
            P(("row", "col")),
            P(("row", "col")),
            P(("row", "col"), None),
            P(("row", "col")),
        ),
        out_specs=(P(None, "row", "col", None), P(("row", "col"), None, None)),
        check_vma=False,
    )
```

```python
from functools import partial

import numpy as np

import jax
import jax.numpy as jnp
from jax import lax
from jax.experimental import pallas as pl
from jax.experimental.pallas import tpu as pltpu
from jax.sharding import PartitionSpec as P

BRICK = 8


DT_STEP = 0.5
VISCOSITY = 0.1
PRECISE = lax.Precision.HIGHEST


def with_halo(block, sides, width):
    for axis, dim in sides:
        count = lax.axis_size(axis)
        forward = [(i, i + 1) for i in range(count - 1)]
        forward.append((count - 1, 0))
        backward = [(target, source) for source, target in forward]
        low = lax.ppermute(
            lax.slice_in_dim(block, block.shape[dim] - width, None, axis=dim), axis, forward
        )
        high = lax.ppermute(lax.slice_in_dim(block, 0, width, axis=dim), axis, backward)
        block = jnp.concatenate([low, block, high], axis=dim)
    return block


def to_bricks(values):
    components, size_x, size_y, size_z = values.shape
    blocks_view = values.reshape(
        components, size_x // BRICK, BRICK, size_y // BRICK, BRICK, size_z // BRICK, BRICK
    )
    blocks_view = blocks_view.transpose(1, 3, 5, 0, 2, 4, 6)
    return blocks_view.reshape(-1, components * BRICK * BRICK * BRICK)


def from_bricks(bricks, size_x, size_y, size_z):
    blocks_view = bricks.reshape(
        size_x // BRICK, size_y // BRICK, size_z // BRICK, 3, BRICK, BRICK, BRICK
    )
    blocks_view = blocks_view.transpose(3, 0, 4, 1, 5, 2, 6)
    return blocks_view.reshape(3, size_x, size_y, size_z)


def chain_force(positions_f, stiffness_f, rest_f):
    segment = jnp.roll(positions_f, -1, axis=2) - positions_f
    stretch = jnp.sum(segment * segment, axis=1, keepdims=True) / rest_f[:, None, None]
    tension = 0.5 * stiffness_f[:, None, None] * (stretch - 1.0) * segment
    return tension - jnp.roll(tension, 1, axis=2)


def interpolate(bricks_in, weights_f):
    cubes = bricks_in.reshape(-1, 3, BRICK, BRICK, BRICK)
    reduced = jnp.einsum("ncijk,nkm->ncijm", cubes, weights_f[:, 2], precision=PRECISE)
    reduced = jnp.einsum("ncijm,njm->ncim", reduced, weights_f[:, 1], precision=PRECISE)
    return jnp.einsum("ncim,nim->ncm", reduced, weights_f[:, 0], precision=PRECISE)


def spread(forces, weights_f):
    partial_sum = jnp.einsum("ncm,nim->ncim", forces, weights_f[:, 0], precision=PRECISE)
    partial_sum = jnp.einsum("ncim,njm->ncijm", partial_sum, weights_f[:, 1], precision=PRECISE)
    cubes = jnp.einsum("ncijm,nkm->ncijk", partial_sum, weights_f[:, 2], precision=PRECISE)
    return cubes.reshape(cubes.shape[0], -1)


def signed_modes(indices, length):
    return jnp.where(indices <= (length - 1) // 2, indices, indices - length)


def direction_modes(indices, length):
    return jnp.where(2 * indices == length, 0, signed_modes(indices, length))


def tables(length):
    indices = jnp.arange(length, dtype=jnp.int32)
    phases = indices[:, None] * indices[None, :] % length
    angles = 2.0 * jnp.pi / length * phases.astype(jnp.float32)
    return (jnp.cos(angles), jnp.sin(angles))


def forward(form, real_part, imag_part, length):
    cosine, sine = tables(length)
    product = partial(jnp.einsum, precision=PRECISE)
    out_real = product(form, real_part, cosine) + product(form, imag_part, sine)
    out_imag = product(form, imag_part, cosine) - product(form, real_part, sine)
    return (out_real, out_imag)


def backward(form, real_part, imag_part, length):
    cosine, sine = tables(length)
    product = partial(jnp.einsum, precision=PRECISE)
    out_real = product(form, real_part, cosine) - product(form, imag_part, sine)
    out_imag = product(form, imag_part, cosine) + product(form, real_part, sine)
    return (out_real / length, out_imag / length)


def col_transpose(values):
    return lax.all_to_all(values, "col", split_axis=4, concat_axis=3, tiled=True)


def row_transpose(values):
    return lax.all_to_all(values, "row", split_axis=4, concat_axis=2, tiled=True)


def wave_parts(indices, length):
    scale = 2.0 * jnp.pi / length
    direct = direction_modes(indices, length)
    signed = signed_modes(indices, length)
    return (scale * direct.astype(jnp.float32), scale * signed.astype(jnp.float32), direct == 0)


def general(velocity, positions, weights, stiffness, rest_sq, owner_column, brick_index):
    row_count = lax.axis_size("row")
    col_count = lax.axis_size("col")
    size_x = velocity.shape[1]
    size_y = velocity.shape[2]
    size_z = velocity.shape[3]
    block_count = positions.shape[0]
    capacity = max(2, 3 * block_count // col_count)
    total_slots = col_count * capacity
    owner_col = owner_column[:, 0]
    order_ids = jnp.arange(block_count, dtype=jnp.int32)
    earlier_same = (owner_col[None, :] == owner_col[:, None]) & (
        order_ids[None, :] < order_ids[:, None]
    )
    slot_index = owner_col * capacity + jnp.sum(earlier_same.astype(jnp.int32), axis=1)
    stored = to_bricks(velocity)
    brick_count = stored.shape[0]

    def place(values, fill):
        buffer = jnp.full((total_slots,) + values.shape[1:], fill, values.dtype)
        return buffer.at[slot_index].set(values).reshape((col_count, capacity) + values.shape[1:])

    weights_f = weights.astype(jnp.float32)
    forces = chain_force(
        positions.astype(jnp.float32), stiffness.astype(jnp.float32), rest_sq.astype(jnp.float32)
    )
    pushed = spread(forces, weights_f)
    send_force = place(pushed, 0.0)
    send_index = place(brick_index.astype(jnp.float32), 0.0)
    wanted = lax.all_to_all(send_index, "col", split_axis=0, concat_axis=0, tiled=True)
    pushes = lax.all_to_all(send_force, "col", split_axis=0, concat_axis=0, tiled=True)
    wanted_ids = wanted.astype(jnp.int32)
    reply = stored[wanted_ids]
    returned = lax.all_to_all(reply, "col", split_axis=0, concat_axis=0, tiled=True)
    returned, arrived_ids, arrived = (returned, wanted_ids, pushes)
    fetched = returned.reshape(total_slots, -1)[slot_index]
    marker_velocity = interpolate(fetched, weights_f)
    forcing = jax.ops.segment_sum(
        arrived.reshape(total_slots, -1), arrived_ids.reshape(-1), num_segments=brick_count
    )
    force_field = from_bricks(forcing, size_x, size_y, size_z)
    padded = with_halo(velocity, (("row", 1), ("col", 2)), 1)
    grad_x = (padded[:, 2:, 1:-1] - padded[:, :-2, 1:-1]) * 0.5
    grad_y = (padded[:, 1:-1, 2:] - padded[:, 1:-1, :-2]) * 0.5
    grad_z = (jnp.roll(velocity, -1, axis=3) - jnp.roll(velocity, 1, axis=3)) * 0.5
    transport = velocity[0] * grad_x + velocity[1] * grad_y + velocity[2] * grad_z
    star = velocity + DT_STEP * (force_field - transport)
    cos_z, sin_z = tables(size_z)
    half_z = size_z // 2
    col_here = lax.axis_index("col")
    cos_fore = cos_z[:, :half_z]
    sin_fore = sin_z[:, :half_z].at[:, 0].set(-cos_z[:, half_z])
    z_real = jnp.einsum("cxyz,zk->cxyk", star, cos_fore, precision=PRECISE)
    z_imag = -jnp.einsum("cxyz,zk->cxyk", star, sin_fore, precision=PRECISE)
    shuffled = col_transpose(jnp.stack([z_real, z_imag]))
    slab = shuffled.shape[4]
    first_slot = (col_here == 0) & (jnp.arange(slab, dtype=jnp.int32) == 0)
    highest = shuffled[1][..., 0:1] * (col_here == 0).astype(jnp.float32)
    lower_imag = jnp.where(first_slot, 0.0, shuffled[1])
    y_in_real = jnp.concatenate([shuffled[0], highest], axis=3)
    y_in_imag = jnp.concatenate([lower_imag, jnp.zeros_like(highest)], axis=3)
    z_index = jnp.concatenate(
        [col_here * slab + jnp.arange(slab, dtype=jnp.int32), jnp.full((1,), half_z, jnp.int32)]
    )
    y_real, y_imag = forward("cxyz,yk->cxzk", y_in_real, y_in_imag, y_in_real.shape[2])
    shuffled = row_transpose(jnp.stack([y_real, y_imag]))
    x_real, x_imag = forward("cxzy,xk->czyk", shuffled[0], shuffled[1], shuffled.shape[2])
    slab_y = x_real.shape[2]
    full_x = x_real.shape[3]
    full_y = slab_y * row_count
    y_index = lax.axis_index("row") * slab_y + jnp.arange(slab_y, dtype=jnp.int32)
    x_index = jnp.arange(full_x, dtype=jnp.int32)
    dir_z, sig_z, zero_z = wave_parts(z_index, size_z)
    dir_y, sig_y, zero_y = wave_parts(y_index, full_y)
    dir_x, sig_x, zero_x = wave_parts(x_index, full_x)
    wave_z = dir_z[:, None, None]
    wave_y = dir_y[None, :, None]
    wave_x = dir_x[None, None, :]
    no_direction = zero_z[:, None, None] & zero_y[None, :, None] & zero_x[None, None, :]
    wave_sq = wave_x * wave_x + wave_y * wave_y + wave_z * wave_z
    full_sq = sig_z[:, None, None] ** 2 + sig_y[None, :, None] ** 2 + sig_x[None, None, :] ** 2
    inverse_sq = jnp.where(no_direction, 0.0, 1.0 / jnp.where(no_direction, 1.0, wave_sq))
    damping = 1.0 / (1.0 + DT_STEP * VISCOSITY * full_sq)
    waves = jnp.stack(
        [
            jnp.broadcast_to(wave_x, wave_sq.shape),
            jnp.broadcast_to(wave_y, wave_sq.shape),
            jnp.broadcast_to(wave_z, wave_sq.shape),
        ]
    )
    normal_real = jnp.sum(waves * x_real, axis=0) * inverse_sq
    normal_imag = jnp.sum(waves * x_imag, axis=0) * inverse_sq
    p_real = (x_real - waves * normal_real) * damping
    p_imag = (x_imag - waves * normal_imag) * damping
    b_real, b_imag = backward("czyk,kx->cyzx", p_real, p_imag, full_x)
    shuffled = row_transpose(jnp.stack([b_real, b_imag]))
    b_real, b_imag = backward("cyzx,yk->cxzk", shuffled[0], shuffled[1], shuffled.shape[2])
    slab = b_real.shape[2] - 1
    first_slot = (col_here == 0) & (jnp.arange(slab, dtype=jnp.int32) == 0)
    highest = b_real[:, :, slab:, :]
    packed_imag = jnp.where(first_slot[None, None, :, None], highest, b_imag[:, :, :slab, :])
    shuffled = col_transpose(jnp.stack([b_real[:, :, :slab, :], packed_imag]))
    doubling = jnp.where(jnp.arange(half_z, dtype=jnp.int32) == 0, 1.0, 2.0)[:, None]
    cos_back = cos_z[:half_z] * doubling
    sin_back = (sin_z[:half_z] * doubling).at[0].set(-cos_z[half_z])
    new_velocity = (
        jnp.einsum("cxky,kz->cxyz", shuffled[0], cos_back, precision=PRECISE)
        - jnp.einsum("cxky,kz->cxyz", shuffled[1], sin_back, precision=PRECISE)
    ) / size_z
    return (new_velocity, marker_velocity)


VMEM = pltpu.VMEM
MESH = pl.DeviceIdType.MESH
F32 = jnp.float32
BF16 = jnp.bfloat16
I32 = jnp.int32
TOP = 32700.0
NT = ((1,), (1,))


def two_parts(table):
    table = np.asarray(table, np.float64)
    high = table.astype(jnp.bfloat16)
    low = (table - high.astype(np.float64)).astype(jnp.bfloat16)
    return np.stack([high, low])


def angle_of(length, left, right):
    return 2.0 * np.pi / length * (np.outer(left, right) % length)


def build_tables(size_x, size_y, size_z, rows):
    half_z = size_z // 2
    turn = angle_of(size_z, np.arange(size_z), np.arange(half_z))
    fore = np.concatenate([np.cos(turn), -np.sin(turn)], axis=1)
    back = np.concatenate([2.0 * np.cos(turn), -2.0 * np.sin(turn)], axis=1)
    alternate = np.where(np.arange(size_z) % 2 == 0, 1.0, -1.0)
    fore[:, half_z] = alternate
    back[:, 0], back[:, half_z] = 1.0, alternate
    back = back.T / (size_x * size_y * size_z)
    turn_y = angle_of(size_y, np.arange(size_y), np.arange(size_y))
    line = np.concatenate([np.cos(turn_y), np.sin(turn_y)], axis=0)
    lane = np.arange(size_x)
    place = (lane % rows) * (size_x // rows) + lane // rows
    turn_x = angle_of(size_x, place, np.arange(size_x))
    cosine, sine = np.cos(turn_x), np.sin(turn_x)
    wide = np.concatenate(
        [np.concatenate([cosine, -sine], axis=1), np.concatenate([sine, cosine], axis=1)], axis=0
    )
    return tuple(two_parts(t) for t in (fore, back, line, wide, wide.T))


def parts(values):
    high = values.astype(BF16)
    return high, (values - high.astype(F32)).astype(BF16)


def mul(left, right, dims=((1,), (0,))):
    return lax.dot_general(left, right, (dims, ((), ())), preferred_element_type=F32)


def mul3(left, right, dims=((1,), (0,))):
    return (
        mul(left[0], right[0], dims) + mul(left[1], right[0], dims) + mul(left[0], right[1], dims)
    )


def roll(values, shift):
    return pltpu.roll(values, shift % 128, values.ndim - 1)


def lanes_of(shape):
    return lax.broadcasted_iota(I32, shape, len(shape) - 1)


def code_of(peak):
    return jnp.floor(jnp.log2(jnp.maximum(peak, 1e-30)) * 65536.0).astype(I32) + 2


def unit_of(code):
    return jnp.exp2(code.astype(F32) * (1.0 / 65536.0)) * (1.0 / TOP)


def whole(values):
    return jnp.round(values).astype(I32)


def join(first, second):
    return (first << 16) + second


def split(word):
    second = (word << 16) >> 16
    return (word - second) >> 16, second


def swap_bits(tiles, steps):
    tiles = list(tiles)
    keep = {s: (lanes_of(tiles[0].shape) & s) == 0 for s in steps}
    for bit, step in enumerate(steps):
        for one in range(len(tiles)):
            if one >> bit & 1:
                continue
            two = one | 1 << bit
            a, b = tiles[one], tiles[two]
            tiles[one] = jnp.where(keep[step], a, roll(b, step))
            tiles[two] = jnp.where(keep[step], roll(a, -step), b)
    return tiles


def compress(tiles, lane):
    out = []
    for t in range(9):
        out.append(jnp.where(lane < 96, tiles[t], roll(tiles[9 + t // 3], 96 - 32 * (t % 3))))
    return out


def expand(tiles, lane):
    out = list(tiles)
    for u in range(3):
        a, b, c = (roll(tiles[3 * u + p], 32 + 32 * p) for p in range(3))
        out.append(jnp.where(lane < 32, a, jnp.where(lane < 64, b, c)))
    return out


def pack_cubes(wide, lane):
    tiles = [wide[t * 8 : t * 8 + 8].astype(I32) for t in range(24)]
    words = []
    for c in range(3):
        for i in range(4):
            words.append(join(tiles[c * 8 + i], tiles[c * 8 + i + 4]))
    return compress(words, lane)


def open_cubes(tiles, lane):
    out = [None] * 24
    for t, word in enumerate(expand(tiles, lane)):
        at = t // 4 * 8 + t % 4
        out[at], out[at + 4] = split(word)
    return jnp.concatenate([t.astype(F32) for t in out], axis=0)


def pad(tile):
    return jnp.concatenate([tile, jnp.zeros((3, 128), I32)], axis=0)


def fold(tile, low, near):
    other = pltpu.roll(roll(tile, 64), 4, 0)
    return jnp.where(jnp.logical_or(low, jnp.logical_not(near)), tile, other)


def unfold(tile, near):
    return jnp.where(near, tile, pltpu.roll(roll(tile, 64), 4, 0))


def peak_of(values):
    while values.ndim > 2:
        values = jnp.max(values, axis=0)
    return jnp.max(jnp.max(values, axis=0, keepdims=True), axis=1, keepdims=True)


def column(row):
    shape = (row.shape[1], row.shape[1])
    diagonal = lax.broadcasted_iota(I32, shape, 0) == lax.broadcasted_iota(I32, shape, 1)
    return jnp.sum(jnp.where(diagonal, row, 0.0), axis=1, keepdims=True)


def mix(step, cols):
    ring, pair = step // cols, step % cols
    return ((6, 2, 4, 7, 3, 5, 1, 0).index(pair % 8), (2, 1, 3, 0).index(ring % 4), step)


def main_kernel(
    rows, columns, capacity,
    owner_hbm, brick_hbm, stiff_hbm, rest_hbm, pos_hbm, weight_hbm, velocity_hbm,
    fore_hbm, line_hbm, wide_hbm, unwide_hbm, back_hbm,
    last_ref, mark_ref, back_ref,
    owner_ref, brick_ref, stiff_ref, rest_ref, pos_ref, weight_ref, velocity_ref,
    fore_ref, line_ref, wide_ref, unwide_ref, noted,
    force, deep, cube, place, face_x, face_y, near_x, near_y, push, pushed, star, select,
    held, modes, arrived, reply, replied, ready,
    load_sems, face_sems, push_sems, mode_sems, reply_sems, last_sems,
):
    sources = (
        owner_hbm, brick_hbm, stiff_hbm, rest_hbm, pos_hbm, weight_hbm, velocity_hbm,
        fore_hbm, line_hbm, wide_hbm, unwide_hbm, back_hbm,
    )
    targets = (
        owner_ref, brick_ref, stiff_ref, rest_ref, pos_ref, weight_ref, velocity_ref,
        fore_ref, line_ref, wide_ref, unwide_ref, back_ref,
    )
    loads = []
    for number, (source, target) in enumerate(zip(sources, targets)):
        loads.append(pltpu.make_async_copy(source, target, load_sems.at[number]))
        loads[-1].start()
    row, col = lax.axis_index("row"), lax.axis_index("col")
    devices = rows * columns
    blocks = pos_ref.shape[1]
    size_x, size_y, size_z = velocity_ref.shape[1:]
    bricks_x = size_x // 8
    barrier = pltpu.get_barrier_semaphore()

    def flip(step):
        at, bit = 0, 1
        while bit < columns:
            own = lax.rem(col // bit, 2)
            at = at + bit * (1 - own if step & bit else own)
            bit *= 2
        return at

    def peer(step):
        to_row, to_col = lax.rem(row + step // columns, rows), flip(step % columns)
        return (to_row, to_col), to_row * columns + to_col

    greet = list(range(1, columns)) + list(range(columns, devices, columns))
    for step in greet:
        pl.semaphore_signal(barrier, inc=1, device_id=peer(step)[0], device_id_type=MESH)

    def remote(source, target, sems, step, device):
        return pltpu.make_async_remote_copy(
            source, target, sems.at[0, step], sems.at[1, step],
            device_id=device, device_id_type=MESH,
        )

    def send_all(source, target, sems, around):
        waits = []
        count = devices if around else columns
        me = row * columns + col if around else col
        for step in sorted(range(1, count), key=lambda n: mix(n, columns)):
            device, at = peer(step)
            at = at if around else device[1]
            copy = remote(source.at[at], target.at[me], sems, step, device)
            copy.start()
            opposite = (rows - step // columns) % rows * columns + step % columns
            origin_device, origin = peer(opposite)
            origin = origin if around else origin_device[1]
            arrival = remote(source.at[at], target.at[origin], sems, step, device)
            waits.append((copy, arrival))
        own = pltpu.make_async_copy(source.at[me], target.at[me], sems.at[0, 0])
        own.start()
        return waits, own

    def receive(sent):
        for _, arrival in sent[0]:
            arrival.wait_recv()
        sent[1].wait()

    def finish(sent):
        for copy, _ in sent[0]:
            copy.wait_send()

    lane8 = lanes_of((8, 128))
    near = lax.broadcasted_iota(I32, (8, 128), 0) < 4

    for load in loads[:4]:
        load.wait()
    owner_row = owner_ref[...].astype(F32)
    owner = column(owner_row)
    shape = (blocks, blocks)
    earlier = lax.broadcasted_iota(I32, shape, 1) < lax.broadcasted_iota(I32, shape, 0)
    rank = jnp.sum(
        jnp.where((owner == owner_row) & earlier, 1.0, 0.0), axis=1, keepdims=True
    )
    slot = jnp.broadcast_to(owner * 128.0 + rank * 8.0, (blocks, 128))
    brick = jnp.broadcast_to(column(brick_ref[...].astype(F32)) + 1.0, (blocks, 128))
    deep_shape = (blocks, 8, 128)
    inner = lax.broadcasted_iota(I32, deep_shape, 1).astype(F32)
    lane_f = lanes_of((blocks, 128)).astype(F32)
    for at in range(columns):
        ahead = lane_f + 128.0 * at - slot
        named = jnp.where((ahead >= 0.0) & (ahead < 8.0), brick, 0.0)
        named = jnp.sum(named, axis=0, keepdims=True).astype(I32)
        noted[at] = jnp.broadcast_to(named, (8, 128))
    slot = (slot[:, None, :] + inner).reshape(blocks * 8, 128)
    lane_f = lanes_of((blocks * 8, 128)).astype(F32)
    for at in range(columns):
        hit = slot == lane_f + 128.0 * at
        place[:, at * 128 : (at + 1) * 128] = jnp.where(hit, 1.0, 0.0).astype(BF16)

    for load in loads[4:6]:
        load.wait()
    stiff = column(stiff_ref[...].astype(F32))
    rest = column(rest_ref[...].astype(F32))
    points = [pos_ref[c].astype(F32) for c in range(3)]
    segment = [pltpu.roll(p, 127, 1) - p for p in points]
    stretch = sum(part * part for part in segment) / rest
    pull = 0.5 * stiff * (stretch - 1.0)
    for c in range(3):
        tension = pull * segment[c]
        force[c] = tension - pltpu.roll(tension, 1, 1)

    def spread(index, carry):
        first = weight_ref[index, 0].astype(F32)
        second = weight_ref[index, 1].astype(F32)
        third = weight_ref[index, 2].astype(F32)
        high, low = parts((first[:, None, :] * third[None]).reshape(64, 128))
        both = jnp.concatenate([high, low], axis=0)
        deep[index] = both
        pushes = jnp.concatenate([force[c, pl.ds(index, 1), :] * second for c in range(3)], axis=0)
        upper = pushes.astype(BF16).astype(F32)
        left = jnp.concatenate([upper, pushes - upper], axis=0).astype(BF16)
        result = mul(left, both, NT)
        total = result[0:24] + result[24:48]
        total = total + pltpu.roll(total, 64, 1)
        cube[index] = total.reshape(3, 8, 128)
        return carry

    lax.fori_loop(0, blocks, spread, 0, unroll=32)

    low_half = lane8 < 64
    outs = [[None] * 2 for _ in range(24)]
    for c in range(3):
        for g in range(2):
            tiles = [
                jnp.where(low_half, cube[g * 16 + b, c], cube[g * 16 + 8 + b, c]) for b in range(8)
            ]
            for i, tile in enumerate(swap_bits(tiles, (8, 16, 32))):
                outs[c * 8 + i][g] = tile
    spreads = jnp.concatenate([jnp.concatenate(pair, axis=1) for pair in outs], axis=0)
    push_code = code_of(peak_of(jnp.abs(spreads)))
    high, low = parts(jnp.round(spreads * (1.0 / unit_of(push_code))))

    for load in loads[6:-1]:
        load.wait()
    value_code = code_of(peak_of(jnp.abs(velocity_ref[...].reshape(-1, 8, size_z))))
    scale = 1.0 / unit_of(value_code)
    half = size_x // 2
    for side, at in ((0, size_x - 1), (1, 0)):
        cells = whole(velocity_ref[:, at] * scale[None])
        face_x[side, 0:24] = join(cells[:, :, 0:128], cells[:, :, 128:256]).reshape(24, 128)
        face_x[side, 24:25] = jnp.broadcast_to(value_code, (1, 128))
    for side, at in ((0, size_y - 1), (1, 0)):
        cells = whole(velocity_ref[:, :, at, :] * scale[None])
        face_y[side, 0:24] = join(cells[:, 0:half], cells[:, half:]).reshape(24, size_z)
        face_y[side, 24:25] = jnp.broadcast_to(value_code, (1, size_z))

    pl.semaphore_wait(barrier, len(greet))
    faces = []
    for source, target, base, axis in ((face_x, near_x, 0, 0), (face_y, near_y, 2, 1)):
        for side in range(2):
            extent = (rows, columns)[axis]
            step = 1 if side == 0 else extent - 1
            if axis == 0:
                device = (lax.rem(row + step, rows), col)
            else:
                device = (row, lax.rem(col + step, columns))
            copy = remote(source.at[side], target.at[side], face_sems, base + side, device)
            copy.start()
            faces.append(copy)

    near_order = sorted(range(1, columns), key=lambda n: mix(n, columns))
    pushes, waiting = [], None
    for step in near_order + [0]:
        device, _ = peer(step)
        at = device[1]
        window = place[:, pl.ds(pl.multiple_of(at * 128, 128), 128)]
        tiles = pack_cubes(mul(high, window) + mul(low, window), lane8)
        target = push if step else pushed
        for t in range(9):
            target[at, t * 8 : t * 8 + 8] = tiles[t]
        target[at, 72:73] = jnp.where(lane8[0:1] < 96, noted[at, 0:1], push_code)
        if waiting is not None:
            waiting.start()
        if step:
            waiting = remote(push.at[at], pushed.at[col], push_sems, step, device)
            arrival = remote(push.at[at], pushed.at[at], push_sems, step, device)
            pushes.append((waiting, arrival))

    for copy in faces:
        copy.wait()
    value = velocity_ref[...]
    sides_x, sides_y = [], []
    for side in range(2):
        unit = unit_of(near_x[side, 24:25])[:, 0:1]
        one, two = split(near_x[side, 0:24])
        wide = jnp.concatenate([one.astype(F32), two.astype(F32)], axis=1) * unit
        sides_x.append(wide.reshape(3, 1, size_y, size_z))
        unit = unit_of(near_y[side, 24:25])[:, 0:1]
        one, two = (part.astype(F32) * unit for part in split(near_y[side, 0:24]))
        wide = [part.reshape(3, half, size_z) for part in (one, two)]
        sides_y.append(jnp.concatenate(wide, axis=1).reshape(3 * size_x, 1, size_z))
    ahead = jnp.concatenate([value[:, 1:], sides_x[1]], axis=1)
    behind = jnp.concatenate([sides_x[0], value[:, :-1]], axis=1)
    transport = value[0:1] * ((ahead - behind) * 0.5)
    flat = value.reshape(3 * size_x, size_y, size_z)
    sub = lax.broadcasted_iota(I32, flat.shape, 1)
    face_low, face_high = sides_y
    ahead = jnp.where(sub == size_y - 1, face_high, pltpu.roll(flat, size_y - 1, 1))
    behind = jnp.where(sub == 0, face_low, pltpu.roll(flat, 1, 1))
    transport += value[1:2] * ((ahead - behind) * 0.5).reshape(value.shape)
    ahead = pltpu.roll(flat, size_z - 1, 2)
    behind = pltpu.roll(flat, 1, 2)
    transport += value[2:3] * ((ahead - behind) * 0.5).reshape(value.shape)
    star[...] = value - DT_STEP * transport

    spot = lax.broadcasted_iota(I32, (bricks_x * size_z, 128), 0)
    inner = lanes_of((1, 128)) & 7
    origins = [0] + near_order
    for k, step in enumerate(origins):
        if step:
            pushes[k - 1][1].wait_recv()
        at = peer(step)[0][1]
        tiles = [pushed[at, t * 8 : t * 8 + 8] for t in range(9)]
        meta = pushed[at, 72:73]
        unit = unit_of(meta)[:, 127:128]
        wide = open_cubes(tiles, lane8).reshape(24, 8, 128) * unit[None]
        high, low = parts(wide.reshape(192, 128))
        held[0, :, k * 128 : (k + 1) * 128] = high
        held[1, :, k * 128 : (k + 1) * 128] = low
        mark = jnp.where((lanes_of((1, 128)) < 96) & (meta > 0), (meta - 1) * 8 + inner, -1)
        select[:, k * 128 : (k + 1) * 128] = jnp.where(spot == mark, 1.0, 0.0).astype(BF16)
        if k % 2 == 0:
            continue
        span = slice((k - 1) * 128, (k + 1) * 128)
        chosen = select[:, span]
        field = mul(held[0, :, span], chosen, NT) + mul(held[1, :, span], chosen, NT)
        for brick_x in range(bricks_x):
            piece = field[:, brick_x * size_z : (brick_x + 1) * size_z].reshape(3, 8, 8, size_z)
            star[:, brick_x * 8 : (brick_x + 1) * 8] += DT_STEP * piece

    spectrum = mul3(parts(star[...].reshape(-1, size_z)), (fore_ref[0], fore_ref[1]))
    real = spectrum[:, 0:128].reshape(3 * size_x, 8, 128)
    imag = spectrum[:, 128:256].reshape(3 * size_x, 8, 128)
    peak = jnp.maximum(jnp.max(jnp.abs(real), axis=0), jnp.max(jnp.abs(imag), axis=0))
    mode_code = jnp.broadcast_to(code_of(jnp.max(peak, axis=0, keepdims=True)), (8, 128))
    scale = (1.0 / unit_of(mode_code))[None]
    words = join(whole(real * scale), whole(imag * scale))
    steps = (4, 8, 16, 32, 64)
    tiles = swap_bits([words[t] for t in range(32)], steps)
    for t in range(devices):
        modes[t, 0:8] = tiles[t]
    tiles = swap_bits([words[32 + t] for t in range(16)] + [mode_code] * 16, steps)
    for t in range(devices):
        modes[t, 8:13] = fold(tiles[t], low_half, near)[0:5]
    moved = send_all(modes, arrived, mode_sems, True)

    scale = 1.0 / unit_of(value_code)
    cells = []
    for brick_x in range(bricks_x):
        piece = velocity_ref[:, brick_x * 8 : (brick_x + 1) * 8].reshape(192, size_z)
        cells.append(parts(jnp.round(piece * scale)))
    for k, step in enumerate(origins):
        at = peer(step)[0][1]
        wide = None
        for brick_x in range(bricks_x):
            chosen = select[
                brick_x * size_z : (brick_x + 1) * size_z, k * 128 : (k + 1) * 128
            ]
            piece = mul(cells[brick_x][0], chosen) + mul(cells[brick_x][1], chosen)
            wide = piece if wide is None else wide + piece
        tiles = pack_cubes(wide, lane8)
        for t in range(9):
            reply[at, t * 8 : t * 8 + 8] = tiles[t]
        reply[at, 72:73] = jnp.broadcast_to(value_code, (1, 128))

    receive(moved)
    here = row * columns + col
    first = here == 0
    upper = jnp.logical_not(low_half)
    lines = [[[] for _ in range(3)] for _ in range(4)]
    for at in range(columns):
        zero = swap_bits([arrived[r * columns + at, 0:8] for r in range(rows)], (1, 2))
        rest_tiles = swap_bits([pad(arrived[r * columns + at, 8:13]) for r in range(rows)], (1, 2))
        for mode in range(4):
            code = jnp.broadcast_to(rest_tiles[mode][4:5], (8, 128))
            unit = unit_of(jnp.where(low_half, roll(code, 64), code))
            real0, imag0 = (p.astype(F32) * unit for p in split(zero[mode]))
            real1, imag1 = (p.astype(F32) * unit for p in split(unfold(rest_tiles[mode], near)))
            lines[mode][0].append(jnp.where(low_half, real0, roll(imag0, 64)))
            lines[mode][1].append(jnp.where(low_half, roll(real0, 64), imag0))
            lines[mode][2].append(jnp.where(low_half, real1, roll(imag1, 64)))
    lines = [[jnp.concatenate(lines[mode][c], axis=0) for c in range(3)] for mode in range(4)]
    wide_y = columns * 8
    low_line = lanes_of((wide_y, 128)) < 64
    lines.append([jnp.where(low_line, roll(v, 64), 0.0) for v in lines[0]])
    lines[0] = [jnp.where(jnp.logical_and(first, jnp.logical_not(low_line)), 0.0, v) for v in lines[0]]
    line_table = (line_ref[0], line_ref[1])
    sign = jnp.where(low_line, 1.0, -1.0)
    lined = []
    for slot_at in range(5):
        both = mul3(line_table, parts(jnp.concatenate(lines[slot_at], axis=1)))
        for c in range(3):
            a = both[0:wide_y, c * 128 : (c + 1) * 128]
            b = both[wide_y:, c * 128 : (c + 1) * 128]
            lined.append(a + sign * roll(b, 64))
    full_x = rows * size_x
    index = lanes_of((wide_y, 128)) & (full_x - 1)
    line = lax.broadcasted_iota(I32, (wide_y, 128), 0)
    scale_x, scale_y, scale_z = (2.0 * np.pi / n for n in (full_x, wide_y, size_z))
    sig_x = jnp.where(index < full_x // 2, index, index - full_x).astype(F32) * scale_x
    sig_y = jnp.where(line < wide_y // 2, line, line - wide_y).astype(F32) * scale_y
    wave_x = jnp.where(index == full_x // 2, 0.0, sig_x)
    wave_y = jnp.where(line == wide_y // 2, 0.0, sig_y)
    backs = []
    replies = send_all(reply, replied, reply_sems, False)
    for slot_at in range(5):
        spot_lines = jnp.concatenate(lined[slot_at * 3 : slot_at * 3 + 3], axis=0)
        values = mul3(parts(spot_lines), (wide_ref[0], wide_ref[1]))
        x, y, z = (values[c * wide_y : (c + 1) * wide_y] for c in range(3))
        if slot_at < 4:
            sig_z = (here * 4 + slot_at).astype(F32) * scale_z
            wave_z = sig_z
        else:
            sig_z, wave_z = F32(np.pi), F32(0.0)
        square = wave_x * wave_x + wave_y * wave_y + wave_z * wave_z
        full = sig_x * sig_x + sig_y * sig_y + sig_z * sig_z
        none = square == 0.0
        inverse_sq = jnp.where(none, 0.0, 1.0 / jnp.where(none, 1.0, square))
        damping = 1.0 / (1.0 + DT_STEP * VISCOSITY * full)
        normal = (wave_x * x + wave_y * y + wave_z * z) * inverse_sq
        result = jnp.concatenate(
            [
                (x - wave_x * normal) * damping,
                (y - wave_y * normal) * damping,
                (z - wave_z * normal) * damping,
            ],
            axis=0,
        )
        turned = mul3(parts(result), (unwide_ref[0], unwide_ref[1]))
        stacked = jnp.concatenate(
            [turned[c * wide_y : (c + 1) * wide_y] for c in range(3)], axis=1
        )
        both = mul3(line_table, parts(stacked))
        back = []
        for c in range(3):
            a = both[0:wide_y, c * 128 : (c + 1) * 128]
            b = both[wide_y:, c * 128 : (c + 1) * 128]
            back.append(a - sign * roll(b, 64))
        backs.append(back)
    top = jnp.logical_and(first, jnp.logical_not(low_line))
    backs[0] = [jnp.where(top, roll(backs[4][c], 64), backs[0][c]) for c in range(3)]
    zero_words, rest_words = [], []
    for mode in range(4):
        e = backs[mode]
        peak = jnp.maximum(jnp.maximum(jnp.abs(e[0]), jnp.abs(e[1])), jnp.abs(e[2]))
        code = code_of(peak_of(peak))
        scale = 1.0 / unit_of(code)
        e = [v * scale for v in e]
        real0 = whole(jnp.where(low_line, e[0], roll(e[1], 64)))
        imag0 = whole(jnp.where(low_line, roll(e[0], 64), e[1]))
        zero_words.append(join(real0, imag0))
        rest_words.append(jnp.where(low_line, join(whole(e[2]), whole(roll(e[2], 64))), code))
    for at in range(columns):
        span = slice(at * 8, at * 8 + 8)
        tiles = swap_bits([w[span] for w in zero_words], (1, 2))
        for r in range(rows):
            ready[r * columns + at, 0:8] = tiles[r]
        tiles = swap_bits([w[span] for w in rest_words], (1, 2))
        for r in range(rows):
            ready[r * columns + at, 8:13] = fold(tiles[r], low_half, near)[0:5]
    lasts = send_all(ready, last_ref, last_sems, True)

    receive(replies)
    for at in range(columns):
        tiles = [replied[at, t * 8 : t * 8 + 8] for t in range(9)]
        unit = unit_of(replied[at, 72:73])
        wide = open_cubes(tiles, lane8).reshape(24, 8, 128) * unit[None]
        high, low = parts(wide.reshape(192, 128))
        held[0, :, at * 128 : (at + 1) * 128] = high
        held[1, :, at * 128 : (at + 1) * 128] = low
    fetched = mul(held[0], place[...], NT) + mul(held[1], place[...], NT)
    for c in range(3):
        for g in range(2):
            tiles = [
                fetched[c * 64 + i * 8 : c * 64 + i * 8 + 8, g * 128 : (g + 1) * 128]
                for i in range(8)
            ]
            for b, tile in enumerate(swap_bits(tiles, (8, 16, 32))):
                cube[g * 8 + b, c] = tile

    low_rows = lanes_of((24, 128)) < 64

    def interpolate_pair(index, carry):
        block = index // 8 * 16 + lax.rem(index, 8)
        cells = cube[index].reshape(24, 128)
        apart = jnp.concatenate(
            [jnp.where(low_rows, cells, 0.0), jnp.where(low_rows, 0.0, cells)], axis=0
        )
        high, low = parts(apart)
        one, two = deep[block], deep[block + 8]
        upper = jnp.concatenate([one[0:64], two[0:64]], axis=0)
        lower = jnp.concatenate([one[64:128], two[64:128]], axis=0)
        summed = mul(high, upper) + mul(low, upper) + mul(high, lower)
        for half, at in ((0, block), (1, block + 8)):
            second = weight_ref[at, 1].astype(F32)
            piece = summed[half * 24 : half * 24 + 24].reshape(3, 8, 128) * second[None]
            piece = jnp.sum(piece, axis=1)
            for c in range(3):
                mark_ref[c, pl.ds(at, 1), :] = piece[c : c + 1]
        return carry

    lax.fori_loop(0, blocks // 2, interpolate_pair, 0, unroll=4)
    loads[-1].wait()
    receive(lasts)
    for copy, _ in pushes:
        copy.wait_send()
    for sent in (moved, replies, lasts):
        finish(sent)


def final_kernel(last_ref, back_ref, mark_ref, new_hbm, out_hbm, new_ref, sems):
    devices = last_ref.shape[0]
    copies = [pltpu.make_async_copy(mark_ref, out_hbm, sems.at[3])]
    copies[0].start()
    steps = (4, 8, 16, 32, 64)
    words = swap_bits([last_ref[t, 0:8] for t in range(devices)], steps)
    low = lanes_of((8, 128)) < 64
    near = lax.broadcasted_iota(I32, (8, 128), 0) < 4
    rest = []
    for t in range(devices):
        tile = pad(last_ref[t, 8:13])
        code = jnp.broadcast_to(tile[4:5], (8, 128))
        rest.append(jnp.where(low, unfold(tile, near), code))
    rest = swap_bits(rest, steps)
    unit = unit_of(rest[16])
    words += rest[0:16]
    rows = []
    for word in words:
        real, imag = split(word)
        rows.append(jnp.concatenate([real.astype(F32) * unit, imag.astype(F32) * unit], axis=1))
    count = len(rows) // 3
    for c in range(3):
        lines = jnp.concatenate(rows[c * count : (c + 1) * count], axis=0)
        result = mul3(parts(lines), (back_ref[0], back_ref[1]))
        new_ref[c] = result.reshape(new_ref.shape[1:])
        copies.append(pltpu.make_async_copy(new_ref.at[c], new_hbm.at[c], sems.at[c]))
        copies[-1].start()
    for copy in copies:
        copy.wait()


def local(velocity, positions, weights, stiffness, rest_sq, owner_column, brick_index):
    rows = lax.axis_size("row")
    columns = lax.axis_size("col")
    devices = rows * columns
    _, local_x, local_y, size_z = velocity.shape
    blocks = positions.shape[0]
    capacity = max(2, 3 * blocks // columns)
    fits = (
        local_x == 16 and local_y == 8 and size_z == 8 * devices and positions.shape[2] == 128
        and capacity == 12 and blocks == 32 and columns == 8 and rows == 4
    )
    if not fits:
        return general(
            velocity, positions, weights, stiffness, rest_sq, owner_column, brick_index
        )
    return fast(velocity, positions, weights, stiffness, rest_sq, owner_column, brick_index)


def fast(velocity, positions, weights, stiffness, rest_sq, owner_column, brick_index):
    rows = lax.axis_size("row")
    columns = lax.axis_size("col")
    devices = rows * columns
    _, local_x, local_y, size_z = velocity.shape
    blocks = positions.shape[0]
    capacity = max(2, 3 * blocks // columns)
    size_x, size_y = rows * local_x, columns * local_y
    fore, back, line, wide, unwide = build_tables(size_x, size_y, size_z, rows)
    vm = pl.BlockSpec(memory_space=VMEM)
    shape = jax.ShapeDtypeStruct
    cells = local_x // BRICK * size_z
    dma = pltpu.SemaphoreType.DMA
    operands = (
        owner_column.reshape(1, blocks), brick_index.reshape(1, blocks),
        stiffness.reshape(1, blocks), rest_sq.reshape(1, blocks),
        positions.transpose(1, 0, 2), weights, velocity, fore, line, wide, unwide,
    )
    last, marks, back = pl.pallas_call(
        partial(main_kernel, rows, columns, capacity),
        out_shape=[
            VMEM((devices, 13, 128), I32), VMEM((3, blocks, 128), F32), VMEM(back.shape, BF16),
        ],
        in_specs=[pl.BlockSpec(memory_space=pl.ANY)] * 12,
        out_specs=[vm, vm, vm],
        scratch_shapes=[VMEM(a.shape, a.dtype) for a in operands] + [
            VMEM((columns, 8, 128), I32),
            VMEM((3, blocks, 128), F32),
            VMEM((blocks, 128, 128), BF16),
            VMEM((blocks, 3, 8, 128), F32),
            VMEM((blocks * 8, columns * 128), BF16),
            VMEM((2, 25, 128), I32),
            VMEM((2, 25, size_z), I32),
            VMEM((2, 25, 128), I32),
            VMEM((2, 25, size_z), I32),
            VMEM((columns, 73, 128), I32),
            VMEM((columns, 73, 128), I32),
            VMEM((3, local_x, local_y, size_z), F32),
            VMEM((cells, columns * 128), BF16),
            VMEM((2, 192, columns * 128), BF16),
            VMEM((devices, 13, 128), I32),
            VMEM((devices, 13, 128), I32),
            VMEM((columns, 73, 128), I32),
            VMEM((columns, 73, 128), I32),
            VMEM((devices, 13, 128), I32),
            dma((12,)),
            dma((2, 4)),
            dma((2, columns)),
            dma((2, devices)),
            dma((2, columns)),
            dma((2, devices)),
        ],
        compiler_params=pltpu.CompilerParams(collective_id=1, has_side_effects=True),
        name="step",
    )(*operands, back)
    new_velocity, marks = pl.pallas_call(
        final_kernel,
        out_shape=[shape(velocity.shape, F32), shape((3, blocks, 128), F32)],
        in_specs=[vm, vm, vm],
        out_specs=[pl.BlockSpec(memory_space=pl.ANY)] * 2,
        scratch_shapes=[VMEM(velocity.shape, F32), dma((4,))],
        name="final",
    )(
        pltpu.with_memory_space_constraint(last, VMEM),
        pltpu.with_memory_space_constraint(back, VMEM),
        pltpu.with_memory_space_constraint(marks, VMEM),
    )
    return new_velocity, marks.transpose(1, 0, 2)


def solution(mesh):
    return jax.shard_map(
        local,
        mesh=mesh,
        in_specs=(
            P(None, "row", "col", None),
            P(("row", "col"), None, None),
            P(("row", "col"), None, None, None),
            P(("row", "col")),
            P(("row", "col")),
            P(("row", "col"), None),
            P(("row", "col")),
        ),
        out_specs=(P(None, "row", "col", None), P(("row", "col"), None, None)),
        check_vma=False,
    )
```
